32 devices in a mesh: px: 4 (over z), py: 4 (over y, x), pz: 2 (over core).
Axes of the slice: x: 2, y: 2, z: 4, core: 2. Of those that a mesh axis runs over, the one named last changes fastest.
Arguments:
- right_side: float32 [16, 64, 256], P('px', 'py', 'pz'), may hold values from -160 to 160
- start_guess: float32 [16, 64, 256], P('px', 'py', 'pz'), may hold values from -4 to 4
- conductivity: float32 [16, 64, 256], P('px', 'py', 'pz'), may hold values from 0.05 to 0.4
- recycled: float32 [16, 16, 64, 256], P(None, 'px', 'py', 'pz'), may hold values from -6 to 6
Outputs:
- solution: float32 [16, 64, 256], P('px', 'py', 'pz')
- residual: float32 [16, 64, 256], P('px', 'py', 'pz')
- hessenberg: float32 [9, 8], replicated
The draws below stay inside these ranges and needn't reach their ends.
All inputs are finite; a program needn't handle non-finite values.
Results may differ from the reference program's by a relative error of at most 0.03.
Values sent between devices are 32-bit elements; how exact they have to be, the bound alone decides.
A program may use at most 128 MiB of HBM per device.

```python
import math
import jax
import jax.numpy as jnp
from jax import lax

K = 16
STEPS = 8
NX = 16
NY = 64
NZ = 256


def recycled_fields(key):
    base_key = jax.random.fold_in(key, 11)
    return jnp.clip(jax.random.normal(base_key, (K, NX, NY, NZ), jnp.float32), -6.0, 6.0)


def draw_recycled(key, part):
    return recycled_fields(key)


def draw_right_side(key, part):
    fields = recycled_fields(key)
    weights = 0.5 * jnp.clip(jax.random.normal(jax.random.fold_in(key, 12), (K,), jnp.float32), -3.0, 3.0)
    noise_part = jnp.clip(jax.random.normal(jax.random.fold_in(key, 13), (NX, NY, NZ), jnp.float32), -6.0, 6.0)
    combined = noise_part + jnp.tensordot(weights, fields, axes=1)
    return combined


def level_of(rng, extent, pieces, low, largest):
    def one(dim, parts):
        heights = jax.random.uniform(jax.random.fold_in(jax.random.fold_in(rng, 6), dim), (parts,), jnp.float32, low / len(pieces), largest / len(pieces))
        return jnp.repeat(jnp.exp(heights), extent[dim] // parts).reshape((-1,) + (1,) * (len(extent) - dim - 1))

    loudness = one(*pieces[0])
    for cut in pieces[1:]:
        loudness = loudness * one(*cut)
    return loudness


def bell_draw(stream_key, dims, deviation, reach, pieces=(), kind=jnp.bfloat16):
    entries = deviation * jax.random.normal(stream_key, dims, jnp.float32)
    if pieces:
        entries = entries * level_of(stream_key, dims, pieces, -0.22, 0.18)
    return jnp.clip(entries, -reach, reach).astype(kind)


def setup_inputs(seed: int = 0) -> dict:
    key_of = jax.random.split(jax.random.key(seed), 5)
    right_side = draw_right_side(jax.random.fold_in(key_of[4], 71), 0)
    start_guess = bell_draw(key_of[1], (NX, NY, NZ), 0.3, 4.0, ((0, 4), (1, 4), (2, 2)), jnp.float32)
    conductivity = jnp.clip(jnp.exp(math.log(0.4) - 2.0794415 * jax.random.uniform(key_of[2], (NX, NY, NZ), jnp.float32) ** level_of(key_of[2], (NX, NY, NZ), ((0, 4), (1, 4), (2, 2)), -0.2, 0.2)), 0.05, 0.4)
    recycled = draw_recycled(jax.random.fold_in(key_of[4], 71), 0)
    return dict(right_side=right_side, start_guess=start_guess, conductivity=conductivity, recycled=recycled)


highest = lax.Precision.HIGHEST
edge_weight = 0.25 ** (1.0 / 3.0)
middle_weight = 2.0 * edge_weight
shift_value = 0.4

def stencil_sum(padded):
    along_z = edge_weight * (padded[..., :-2] + padded[..., 2:]) + middle_weight * padded[..., 1:-1]
    along_y = edge_weight * (along_z[..., :-2, :] + along_z[..., 2:, :]) + middle_weight * along_z[..., 1:-1, :]
    along_x = edge_weight * (along_y[..., :-2, :, :] + along_y[..., 2:, :, :]) + middle_weight * along_y[..., 1:-1, :, :]
    return along_x - 2.0 * padded[..., 1:-1, 1:-1, 1:-1]

def pad_cells(field_in):
    return jnp.pad(field_in, ((1, 1), (1, 1), (1, 1)))

def operate(field_in, conductivity, diagonal):
    near_sum = stencil_sum(pad_cells(field_in))
    far_sum = stencil_sum(pad_cells(conductivity * field_in))
    return diagonal * field_in - 0.5 * conductivity * near_sum - 0.5 * far_sum

def cholesky_low(gram):
    order = gram.shape[0]
    rows_idx = jnp.arange(order)
    factor = jnp.zeros((order, order), jnp.float32)
    for column in range(order):
        known = factor[:, :column]
        partial_sum = lax.optimization_barrier(jnp.sum(known * known[column][None, :], axis=1))
        pivot = jnp.sqrt(gram[column, column] - partial_sum[column])
        values = (gram[:, column] - partial_sum) / pivot
        values = jnp.where(rows_idx > column, values, 0.0)
        factor = factor.at[:, column].set(values).at[column, column].set(pivot)
    return factor

def lower_inverse(factor):
    order = factor.shape[0]
    inverse = jnp.zeros((order, order), jnp.float32)
    for row in range(order):
        unit_row = jnp.zeros((order,), jnp.float32).at[row].set(1.0)
        partial_value = lax.optimization_barrier(jnp.sum(factor[row, :row][:, None] * inverse[:row], axis=0))
        inverse = inverse.at[row].set((unit_row - partial_value) / factor[row, row])
    return inverse

def back_solve(upper_tri, target):
    order = upper_tri.shape[0]
    result = jnp.zeros((order,), jnp.float32)
    for row in range(order - 1, -1, -1):
        partial_value = jnp.sum(upper_tri[row, row + 1:] * result[row + 1:])
        result = result.at[row].set((target[row] - partial_value) / upper_tri[row, row])
    return result

def least_squares(hessenberg, beta_norm):
    upper_tri = hessenberg
    target = jnp.zeros((STEPS + 1,), jnp.float32).at[0].set(beta_norm)
    for column in range(STEPS):
        top_entry = upper_tri[column, column]
        low_entry = upper_tri[column + 1, column]
        radius = jnp.sqrt(top_entry * top_entry + low_entry * low_entry)
        cosine = top_entry / radius
        sine_val = low_entry / radius
        row_top = cosine * upper_tri[column] + sine_val * upper_tri[column + 1]
        row_low = cosine * upper_tri[column + 1] - sine_val * upper_tri[column]
        upper_tri = upper_tri.at[column].set(row_top).at[column + 1].set(row_low)
        goal_top = cosine * target[column] + sine_val * target[column + 1]
        goal_low = cosine * target[column + 1] - sine_val * target[column]
        target = target.at[column].set(goal_top).at[column + 1].set(goal_low)
    return back_solve(upper_tri[:STEPS], target[:STEPS])

def reference(right_side, start_guess, conductivity, recycled):
    diagonal = shift_value + 7.0 * conductivity + 0.5 * stencil_sum(pad_cells(conductivity))
    images_c = lax.map(lambda single_field: operate(single_field, conductivity, diagonal), recycled)
    flat_images = images_c.reshape(K, -1)
    first_residual = (right_side - operate(start_guess, conductivity, diagonal)).reshape(-1)
    gram = jnp.dot(flat_images, flat_images.T, precision=highest)
    factor_low = cholesky_low(gram)
    inverse = lower_inverse(factor_low)
    basis_c = jnp.dot(inverse, flat_images, precision=highest)
    projected = jnp.dot(basis_c, first_residual, precision=highest)
    recycle_flat = recycled.reshape(K, -1)
    solution = start_guess.reshape(-1) + jnp.dot(jnp.dot(inverse.T, projected, precision=highest), recycle_flat, precision=highest)
    residual = first_residual - jnp.dot(projected, basis_c, precision=highest)
    beta_norm = jnp.sqrt(jnp.dot(residual, residual, precision=highest))
    krylov = [residual / beta_norm]
    coupling = jnp.zeros((K, STEPS), jnp.float32)
    hessenberg = jnp.zeros((STEPS + 1, STEPS), jnp.float32)
    for column in range(STEPS):
        vector_new = operate(krylov[column].reshape(NX, NY, NZ), conductivity, diagonal).reshape(-1)
        known_basis = jnp.stack(krylov)
        coeff_c = jnp.dot(basis_c, vector_new, precision=highest)
        coeff_v = jnp.dot(known_basis, vector_new, precision=highest)
        vector_new = vector_new - jnp.dot(coeff_c, basis_c, precision=highest) - jnp.dot(coeff_v, known_basis, precision=highest)
        norm_new = jnp.sqrt(jnp.dot(vector_new, vector_new, precision=highest))
        coupling = coupling.at[:, column].set(coeff_c)
        hessenberg = hessenberg.at[:column + 1, column].set(coeff_v)
        hessenberg = hessenberg.at[column + 1, column].set(norm_new)
        krylov.append(vector_new / norm_new)
    coeffs = least_squares(hessenberg, beta_norm)
    basis_all = jnp.stack(krylov)
    recycle_coeffs = jnp.dot(inverse.T, jnp.dot(coupling, coeffs, precision=highest), precision=highest)
    solution = solution + jnp.dot(coeffs, basis_all[:STEPS], precision=highest) - jnp.dot(recycle_coeffs, recycle_flat, precision=highest)
    residual = residual - jnp.dot(jnp.dot(hessenberg, coeffs, precision=highest), basis_all, precision=highest)
    return (solution.reshape(NX, NY, NZ), residual.reshape(NX, NY, NZ), hessenberg)
```

```python
import functools
import itertools

import jax
import jax.numpy as jnp
from jax import lax
from jax.experimental import pallas as pl
from jax.experimental.pallas import tpu as pltpu
from jax.sharding import PartitionSpec as P

STEPS = 8
MESH = pl.DeviceIdType.MESH
AXES = ("px", "py", "pz")
TWO = (("py", "pz"), ("px",))
ONE = (("px", "py", "pz"),)
CHUNK = 8
GF = 4

edge_weight = 0.25 ** (1.0 / 3.0)
middle_weight = 2.0 * edge_weight
shift_value = 0.4

DIRS = [d for d in itertools.product((-1, 0, 1), repeat=3) if d != (0, 0, 0)]


def sem_counts(sizes):
    dirs = [d for d in DIRS if all(s == 0 or n > 1 for n, s in zip(sizes, d))]
    flat = sum(d[2] == 0 for d in dirs)
    tall = len(dirs) - flat
    return flat, tall // 2 if sizes[2] == 2 else tall


def kernel(
    sizes, groups,
    rhs, guess, cond, rec,
    sol_out, res_out, hes_out,
    src, img, bface, bedge, pack, pface, pedge,
    bx, by, bc,
    zm, zx, zy, zc,
    mx, my, mc,
    wbuf, wface, wedge,
    fields, kext, diag, temp, zext,
    gpart, gred1, gred2, sred1, sred2,
    mat, hcols, scale, coef, ecoef,
    hsend, hrecv, rsend, rrecv,
):
    nsz = dict(zip(AXES, sizes))
    me = {a: lax.axis_index(a) for a in AXES}
    K, X, Y, Z = rec.shape
    NF = K + 2
    C0 = K
    NC = (NF + CHUNK - 1) // CHUNK
    f32 = jnp.float32
    lane3 = lax.broadcasted_iota(jnp.int32, (X + 2, Y + 8, Z), 2)
    lane2 = lax.broadcasted_iota(jnp.int32, (32, Z), 1)
    row2 = lax.broadcasted_iota(jnp.int32, (32, Z), 0)

    def exists(d):
        ok = None
        for a, s in zip(AXES, d):
            if s == 0:
                continue
            here = (me[a] < nsz[a] - 1) if s > 0 else (me[a] > 0)
            ok = here if ok is None else jnp.logical_and(ok, here)
        return ok

    def possible(d):
        return all(s == 0 or nsz[a] > 1 for a, s in zip(AXES, d))

    flat = [d for d in DIRS if possible(d) and d[2] == 0]
    tall = [d for d in DIRS if possible(d) and d[2] != 0]
    dirs = flat + tall
    NFLAT, NTALL = sem_counts(sizes)

    def sem_index(chunk, d):
        if d[2] == 0:
            return chunk * NFLAT + flat.index(d)
        twin = (d[0], d[1], 1) if nsz["pz"] == 2 else d
        return NC * NFLAT + tall.index(twin) % NTALL

    def target(d):
        return tuple(me[a] + s for a, s in zip(AXES, d))

    def group_info(group):
        n = 1
        rank = 0
        for a in group:
            n *= nsz[a]
            rank = rank * nsz[a] + me[a]
        return n, rank

    def member(group, r):
        co = dict(me)
        for a in reversed(group):
            co[a] = lax.rem(r, nsz[a])
            r = lax.div(r, nsz[a])
        return tuple(co[a] for a in AXES)

    def copies(sends, recvs, batch, chunk, zones):
        out = []
        for dx, dy, dz in dirs:
            if (dz != 0) not in zones:
                continue
            main, face, edge = sends(dz)
            rm, rx, ry, rc = recvs(-dz)
            hx, hy = int(dx > 0), int(dy > 0)
            if dx == 0 and dy == 0:
                s, t = main, rm
            elif dy == 0:
                s, t = main.at[:, X - 1 if hx else 0], rx.at[1 - hx]
            elif dx == 0:
                s, t = face.at[hy], ry.at[1 - hy]
            else:
                s, t = edge.at[hx, hy], rc.at[1 - hx, 1 - hy]
            d = (dx, dy, dz)
            out.append((d, pltpu.make_async_remote_copy(
                src_ref=s, dst_ref=t,
                send_sem=hsend.at[sem_index(chunk, d)], recv_sem=hrecv.at[batch, sem_index(chunk, d)],
                device_id=target(d), device_id_type=MESH,
            )))
        return out

    def start_halo(cs):
        for d, c in cs:
            pl.when(exists(d))(c.start)

    def wait_recv(cs):
        for d, c in cs:
            pl.when(exists(tuple(-s for s in d)))(c.wait_recv)

    def wait_send(cs):
        for d, c in cs:
            pl.when(exists(d))(c.wait_send)

    def batch_copies(b, c):
        f0, f1 = c * CHUNK, min((c + 1) * CHUNK, NF)
        fs, es = pl.ds(f0, f1 - f0), pl.ds(f0, CHUNK)
        rows = pl.ds(f0 * X, min(CHUNK * X, bface.shape[2] - f0 * X))

        def sends(dz):
            if dz == 0:
                body = (src if b == 0 else img).at[fs]
                return body, bface.at[b, :, rows], bedge.at[b, :, :, es]
            h = int(dz > 0)
            return pack.at[b, h], pface.at[b, h], pedge.at[b, h]

        def recvs(z):
            if z == 0:
                return None, bx.at[b, :, fs], by.at[b, :, rows], bc.at[b, :, :, es]
            h = int(z > 0)
            return zm.at[b, h], zx.at[b, h], zy.at[b, h], zc.at[b, h]

        return copies(sends, recvs, b, c % NC, (c == NC,))

    def step_copies(par):
        def sends(dz):
            return wbuf.at[par], wface.at[par], wedge.at[par]

        def recvs(z):
            if z == 0:
                return None, mx.at[par], my.at[par], mc.at[par]
            h = int(z > 0)
            return zm.at[2 + par, h], zx.at[2 + par, h], zy.at[2 + par, h], zc.at[2 + par, h]

        return copies(sends, recvs, par, 0, (False, True))

    def pack_faces(val, face, edge, row, erow):
        for h, y in ((0, 0), (1, Y - 1)):
            for x in range(X):
                face[h, pl.ds(row + x, 1), :] = val[x, y : y + 1, :]
            edge[0, h, pl.ds(erow, 1), :] = val[0, y : y + 1, :]
            edge[1, h, pl.ds(erow, 1), :] = val[X - 1, y : y + 1, :]

    def assemble(dst, main, rx, ry, rc, f, row, erow):
        dst[1 : X + 1, 0:Y, :] = main
        dst[0, 0:Y, :] = rx[0, f]
        dst[X + 1, 0:Y, :] = rx[1, f]
        for h, y in ((1, Y), (0, Y + 7)):
            for x in range(X):
                dst[1 + x, y : y + 1, :] = ry[h, pl.ds(row + x, 1), :]
            dst[0, y : y + 1, :] = rc[0, h, pl.ds(erow, 1), :]
            dst[X + 1, y : y + 1, :] = rc[1, h, pl.ds(erow, 1), :]

    def assemble_zones(slot):
        for h in range(2):
            assemble(zext.at[h], zm[slot, h, 0], zx.at[slot, h], zy.at[slot, h], zc.at[slot, h], 0, 0, 0)

    def zone_field(f):
        low = pltpu.roll(zext[0], lax.rem(2 * Z - 1 - f, Z), 2)
        high = pltpu.roll(zext[1], lax.rem(Z - f, Z), 2)
        return jnp.where(lane3 == Z - 1, low, jnp.where(lane3 == 0, high, 0.0))

    def pack_lanes(get, count, b):
        lane = lax.broadcasted_iota(jnp.int32, (X, Y, Z), 2)
        low = jnp.zeros((X, Y, Z), f32)
        high = jnp.zeros((X, Y, Z), f32)
        for f in range(count):
            v = get(f)
            low = jnp.where(lane == f, pltpu.roll(v, f, 2) if f else v, low)
            high = jnp.where(lane == f, pltpu.roll(v, (f + 1) % Z, 2), high)
        for h, v in ((0, low), (1, high)):
            pack[b, h, 0] = v
            pack_faces(v, pface.at[b, h], pedge.at[b, h], 0, 0)

    def stencil(e, b):
        left = pltpu.roll(jnp.where(lane3 == Z - 1, b, e), 1, 2)
        right = pltpu.roll(jnp.where(lane3 == 0, b, e), Z - 1, 2)
        az = edge_weight * (left + right) + middle_weight * e
        ay = edge_weight * (pltpu.roll(az, 1, 1) + pltpu.roll(az, Y + 7, 1)) + middle_weight * az
        ay = ay[:, :Y]
        ax = edge_weight * (ay[:X] + ay[2:]) + middle_weight * ay[1 : X + 1]
        return ax - 2.0 * e[1 : X + 1, :Y]

    def apply(e, b):
        k = kext[0]
        near = stencil(e, b)
        far = stencil(k * e, kext[1] * b)
        return diag[...] * e[1 : X + 1, :Y] - 0.5 * k[1 : X + 1, :Y] * near - 0.5 * far

    def tile_sum(v):
        v = jnp.sum(v.reshape(X * Y // 8, 8, Z), axis=0)
        return jnp.sum(v, axis=0, keepdims=True)

    def all_reduce(value, groups, bufs, slot, between):
        total = value
        for g, group in enumerate(groups):
            n, rank = group_info(group)
            buf = bufs[g]
            buf[rank] = total
            for k in sorted(range(1, n), key=lambda k: -min(k, n - k)):
                pltpu.make_async_remote_copy(
                    src_ref=buf.at[rank], dst_ref=buf.at[rank],
                    send_sem=rsend.at[slot, g], recv_sem=rrecv.at[slot, g],
                    device_id=member(group, lax.rem(rank + k, n)), device_id_type=MESH,
                ).start()
            if g == len(groups) - 1:
                between()
            others = pltpu.make_async_remote_copy(
                src_ref=buf.at[pl.ds(0, n - 1)], dst_ref=buf.at[pl.ds(0, n - 1)],
                send_sem=rsend.at[slot, g], recv_sem=rrecv.at[slot, g],
                device_id=member(group, lax.rem(rank + 1, n)), device_id_type=MESH,
            )
            others.wait_recv()
            parts = [buf[r] for r in range(n)]
            while len(parts) > 1:
                parts = [sum(parts[r : r + 2][1:], parts[r]) for r in range(0, len(parts), 2)]
            total = parts[0]
            others.wait_send()
        return total

    def clear_all(refs):
        for ref in refs:
            def clear(i, carry, ref=ref):
                ref[i] = jnp.zeros(ref.shape[1:], f32)
                return carry

            lax.fori_loop(0, ref.shape[0], clear, 0)

    clear_all((bx, by, bc, zm, zx, zy, zc, mx, my, mc))
    barrier = pltpu.get_barrier_semaphore()
    count = jnp.int32(0)
    for group in ONE:
        n, rank = group_info(group)
        for k in range(1, n):
            pl.semaphore_signal(
                barrier, inc=1, device_id=member(group, lax.rem(rank + k, n)), device_id_type=MESH
            )
        count = count + (n - 1)

    clear_all((wface, wedge, bface, bedge, pface, pedge))

    def load_field(f, carry):
        v = rec[f]
        src[f] = v
        pack_faces(v, bface.at[0], bedge.at[0], f * X, f)
        return carry

    lax.fori_loop(0, K, load_field, 0)
    for f, ref in ((K, guess), (K + 1, cond)):
        v = ref[...]
        src[f] = v
        pack_faces(v, bface.at[0], bedge.at[0], f * X, f)
    pack_lanes(lambda f: src[f], NF, 0)
    pl.semaphore_wait(barrier, count)

    first = [batch_copies(0, c) for c in range(NC + 1)]
    second = [batch_copies(1, c) for c in range(NC + 1)]
    order = [NC - 1] + list(range(NC - 1))
    for c in [NC] + order:
        start_halo(first[c])
    clear_all((fields, kext, zext))
    temp[...] = jnp.zeros(temp.shape, f32)
    img[NF - 1] = jnp.zeros((X, Y, Z), f32)
    wait_recv(first[NC])
    assemble_zones(0)

    def image(f, carry):
        assemble(temp, src[f], bx.at[0], by.at[0], bc.at[0], f, f * X, f)
        v = apply(temp[...], zone_field(f))
        img[f] = v
        pack_faces(v, bface.at[1], bedge.at[1], f * X, f)
        return carry

    for c in order:
        wait_recv(first[c])
        if c == NC - 1:
            assemble(kext.at[0], src[K + 1], bx.at[0], by.at[0], bc.at[0], K + 1, (K + 1) * X, K + 1)
            kext[1] = zone_field(K + 1)
            k_all = kext[0]
            diag[...] = shift_value + 7.0 * k_all[1 : X + 1, :Y] + 0.5 * stencil(k_all, kext[1])
            lax.fori_loop(c * CHUNK, K + 1, image, 0)
            v = rhs[...] - img[K]
            img[K] = v
            pack_faces(v, bface.at[1], bedge.at[1], K * X, K)
        else:
            lax.fori_loop(c * CHUNK, (c + 1) * CHUNK, image, 0, unroll=2)
        wait_send(first[c])
        start_halo(second[c])
    pack_lanes(lambda f: img[f], K + 1, 1)
    wait_send(first[NC])
    start_halo(second[NC])

    GR = gpart.shape[1]
    GW = Z // (GR // GF)
    assert K + 1 <= GW

    def gram_part(a, carry):
        va = img[a]
        rows = [tile_sum(img[b] * va) for b in range(K + 1)]
        rows.append(jnp.zeros((GR - K - 1, Z), f32))
        gpart[a] = jnp.concatenate(rows, axis=0)
        return carry

    lax.fori_loop(0, K + 1, gram_part, 0, unroll=2)
    lane_g = lax.broadcasted_iota(jnp.int32, (GR, Z), 1)
    gram = jnp.zeros((GR, Z), f32)
    for a in range(K + 1):
        gram = jnp.where(lane_g == a, jnp.sum(gpart[a], axis=1, keepdims=True), gram)
    def extend_all():
        for c in second:
            wait_recv(c)
        assemble_zones(1)

        def extend(f, carry):
            assemble(fields.at[f, 0], img[f], bx.at[1], by.at[1], bc.at[1], f, f * X, f)
            fields[f, 1] = zone_field(f)
            return carry

        lax.fori_loop(0, K + 1, extend, 0, unroll=4)

    part = gram[:GF]
    for q in range(1, GR // GF):
        part = part + pltpu.roll(gram[GF * q : GF * q + GF], q * GW, 1)
    part = all_reduce(part, groups, (gred1, gred2), 2, extend_all)
    gram = [part] + [pltpu.roll(part, Z - q * GW, 1) for q in range(1, GR // GF)]
    gram = jnp.concatenate(gram, axis=0)

    lane_k = lax.broadcasted_iota(jnp.int32, (K, Z), 1)
    row_k = lax.broadcasted_iota(jnp.int32, (K, Z), 0)
    a_mat = jnp.where(lane_k < K, gram[:K], 0.0)
    for k in range(K):
        prow = a_mat[k : k + 1, :]
        pcol = a_mat[:, k : k + 1]
        inv_p = 1.0 / a_mat[k : k + 1, k : k + 1]
        prow_s = jnp.where(lax.broadcasted_iota(jnp.int32, (1, Z), 1) == k, 1.0, prow) * inv_p
        base = jnp.where(lane_k == k, 0.0, a_mat)
        a_mat = jnp.where(row_k == k, jnp.broadcast_to(prow_s, (K, Z)), base - pcol * prow_s)
    mat[...] = jnp.where(lane2 == row2, 1.0, 0.0)
    mat[0:K, :] = a_mat
    grow = jnp.where(lax.broadcasted_iota(jnp.int32, (1, Z), 1) < K, gram[K : K + 1, :], 0.0)
    ecoef[...] = jnp.broadcast_to(jnp.sum(a_mat * grow, axis=1, keepdims=True), (K, Z))

    def begin(p, carry):
        z, x = lax.div(p, X + 2), lax.rem(p, X + 2)
        v = fields[C0, z, x]
        for a in range(K):
            v = v - ecoef[a : a + 1, :] * fields[a, z, x]
        fields[C0, z, x] = v
        return carry

    lax.fori_loop(0, 2 * (X + 2), begin, 0)
    for c in second:
        wait_send(c)
    hcols[...] = jnp.zeros((32, Z), f32)
    scale[...] = jnp.where(row2 < K, 1.0, 0.0)

    def step(j, carry):
        par = lax.rem(j, 2)
        u = fields[C0 + j, 0]
        w = apply(u, fields[C0 + j, 1])
        wbuf[par, 0] = w
        pack_faces(w, wface.at[par], wedge.at[par], 0, 0)
        cs = step_copies(par)

        @pl.when(j < STEPS - 1)
        def _():
            start_halo(cs)

        rows = [tile_sum(fields[f, 0, 1 : X + 1, 0:Y, :] * w) for f in range(K + STEPS)]
        ui = u[1 : X + 1, :Y]
        rows.append(tile_sum(w * w))
        rows.append(tile_sum(ui * ui))
        rows.append(jnp.zeros((32 - K - STEPS - 2, Z), f32))
        sums = jnp.sum(jnp.concatenate(rows, axis=0), axis=1, keepdims=True)
        part = jnp.sum(jnp.where(lane2 == row2, sums, 0.0), axis=0, keepdims=True)
        def extend_w():
            @pl.when(j < STEPS - 1)
            def _():
                wait_recv(cs)
                slot = 2 + par
                assemble(temp, wbuf[par, 0], mx.at[par], my.at[par], mc.at[par], 0, 0, 0)
                fields[C0 + 1 + j, 0] = temp[...]
                assemble_zones(slot)
                fields[C0 + 1 + j, 1] = jnp.where(
                    lane3 == Z - 1, zext[0], jnp.where(lane3 == 0, zext[1], 0.0)
                )

            @pl.when(j == STEPS - 1)
            def _():
                fields[C0 + STEPS, 0, 1 : X + 1, 0:Y, :] = wbuf[par, 0]

        total = all_reduce(part, groups, (sred1.at[par], sred2.at[par]), par, extend_w)
        c = jnp.broadcast_to(jnp.sum(mat[...] * total, axis=1, keepdims=True), (32, Z))
        uu = c[K + STEPS + 1 : K + STEPS + 2, :]
        sc = jnp.where(row2 == C0 + j, 1.0 / uu, scale[...])
        scale[...] = sc
        hcols[...] = jnp.where(lane2 == j, c, hcols[...])
        inv_n = 1.0 / jnp.sqrt(uu)
        coef[...] = jnp.where(
            row2 < K + STEPS, c * sc * inv_n, jnp.where(row2 == 30, inv_n, total)
        )

        def update(p, carry):
            z, x = lax.div(p, X + 2), lax.rem(p, X + 2)
            v = coef[30:31, :] * fields[C0 + 1 + j, z, x]
            v2 = jnp.zeros_like(v)
            for a in range(0, K + STEPS, 2):
                v = v - coef[a : a + 1, :] * fields[a, z, x]
                v2 = v2 - coef[a + 1 : a + 2, :] * fields[a + 1, z, x]
            fields[C0 + 1 + j, z, x] = v + v2
            return carry

        lax.fori_loop(0, 2 * (X + 2), update, 0, unroll=4)

        @pl.when(j < STEPS - 1)
        def _():
            wait_send(cs)

        return carry

    lax.fori_loop(0, STEPS, step, 0)

    lane8 = lane2[:8]
    row8 = row2[:8]
    hc = hcols[...]
    inv_n2 = scale[C0 : C0 + STEPS, :]
    inv_col = jnp.sqrt(inv_n2)
    n_col = 1.0 / inv_col
    inv_row = jnp.sum(jnp.where(lane8 == row8, inv_col, 0.0), axis=0, keepdims=True)
    last_c = jnp.sum(jnp.where(lane2 == STEPS - 1, hc, 0.0), axis=1, keepdims=True)
    raw = jnp.broadcast_to(coef[31:32, :], (32, Z))
    raw_col = jnp.sum(jnp.where(lane2 == row2, raw, 0.0), axis=1, keepdims=True)
    terms = jnp.where(row2[:, :1] < K + STEPS, raw_col * last_c * scale[:, :1], 0.0)
    used = jnp.sum(terms, axis=0, keepdims=True)
    last_sq = (raw_col[K + STEPS : K + STEPS + 1] - used) * inv_n2[STEPS - 1 : STEPS, :1]
    last_n = jnp.sqrt(last_sq)
    upper = hc[C0 : C0 + STEPS] * inv_col * inv_row
    upper = jnp.where(lane8 < STEPS, upper, 0.0)
    upper = jnp.where(lane8 == row8 - 1, n_col, upper)
    lane1 = lane2[:1]
    bottom = jnp.where(lane1 == STEPS - 1, last_n, 0.0)
    hes = jnp.concatenate([upper, bottom], axis=0)
    lane_t, row_t = lane2[: STEPS + 1], row2[: STEPS + 1]
    for col in range(STEPS):
        picked = jnp.where(lane_t == row_t, hes[:, col : col + 1], 0.0)
        hes_out[col : col + 1, :] = jnp.sum(picked, axis=0, keepdims=True)[:, : STEPS + 1]

    rows = [hes[i : i + 1] for i in range(STEPS + 1)]
    rows[0] = jnp.where(lane1 == STEPS, n_col[0:1], rows[0])
    for i in range(STEPS):
        top, low = rows[i][:, i : i + 1], rows[i + 1][:, i : i + 1]
        inv_r = 1.0 / jnp.sqrt(top * top + low * low)
        cs_, sn = top * inv_r, low * inv_r
        rows[i], rows[i + 1] = cs_ * rows[i] + sn * rows[i + 1], cs_ * rows[i + 1] - sn * rows[i]
    ysol = jnp.zeros((1, Z), f32)
    for i in range(STEPS - 1, -1, -1):
        known = jnp.sum(jnp.where(lane1 > i, rows[i] * ysol, 0.0), axis=1, keepdims=True)
        yi = (rows[i][:, STEPS : STEPS + 1] - known) / rows[i][:, i : i + 1]
        ysol = jnp.where(lane1 == i, yi, ysol)

    rcoef = ecoef[:, :1] - jnp.sum(hc[:K] * (ysol * inv_row), axis=1, keepdims=True)
    ycol = jnp.sum(jnp.where(lane8 == row8, ysol * inv_row, 0.0), axis=1, keepdims=True)
    hy8 = jnp.sum(upper * ysol, axis=1, keepdims=True) * inv_col[:, :1]
    hy9 = jnp.sum(bottom * ysol, axis=1, keepdims=True) / last_n
    out = guess[...]
    for a in range(K):
        out = out + rcoef[a : a + 1, :] * rec[a]
    res = fields[C0, 0, 1 : X + 1, 0:Y, :]
    for i in range(STEPS):
        ui = fields[C0 + i, 0, 1 : X + 1, 0:Y, :]
        out = out + ycol[i : i + 1, :] * ui
        res = res - hy8[i : i + 1, :] * ui
    res = res - hy9 * fields[C0 + STEPS, 0, 1 : X + 1, 0:Y, :]
    sol_out[...] = out
    res_out[...] = res


def deliver(sol, res, hes, sol_out, res_out, hes_out):
    sol_out[...] = sol[...]
    res_out[...] = res[...]
    hes_out[...] = hes[...]


def round_up(n, m):
    return (n + m - 1) // m * m


def solution(mesh):
    sizes = tuple(mesh.shape[a] for a in AXES)

    def body(right_side, start_guess, conductivity, recycled):
        K, X, Y, Z = recycled.shape
        NF = K + 2
        FR, ER, XR = round_up(NF * X, 8), round_up(NF, 8), round_up(X, 8)
        def count(group):
            n = 1
            for a in group:
                n *= mesh.shape[a]
            return n

        groups = ONE if count(AXES) <= 64 else TWO
        n_step = [count(g) for g in groups]
        nflat, ntall = sem_counts(sizes)
        nsem = (NF + CHUNK - 1) // CHUNK * nflat + ntall
        GR = round_up(K + 1, 8)
        V = lambda *s: pltpu.VMEM(s, jnp.float32)
        vm = pl.BlockSpec(memory_space=pltpu.VMEM)
        shape = jax.ShapeDtypeStruct((X, Y, Z), jnp.float32)
        sol, res, hes = pl.pallas_call(
            functools.partial(kernel, sizes, groups),
            out_shape=(shape, shape, jax.ShapeDtypeStruct((STEPS, STEPS + 1), jnp.float32)),
            in_specs=[vm] * 4,
            out_specs=(vm, vm, vm),
            scratch_shapes=[
                V(NF, X, Y, Z), V(NF, X, Y, Z),
                V(2, 2, FR, Z), V(2, 2, 2, ER, Z),
                V(2, 2, 1, X, Y, Z), V(2, 2, 2, XR, Z), V(2, 2, 2, 2, 1, Z),
                V(2, 2, NF, Y, Z), V(2, 2, FR, Z), V(2, 2, 2, ER, Z),
                V(4, 2, 1, X, Y, Z), V(4, 2, 2, 1, Y, Z), V(4, 2, 2, XR, Z), V(4, 2, 2, 2, 1, Z),
                V(2, 2, 1, Y, Z), V(2, 2, XR, Z), V(2, 2, 2, 1, Z),
                V(2, 1, X, Y, Z), V(2, 2, XR, Z), V(2, 2, 2, 1, Z),
                V(K + STEPS + 1, 2, X + 2, Y + 8, Z), V(2, X + 2, Y + 8, Z), V(X, Y, Z),
                V(X + 2, Y + 8, Z), V(2, X + 2, Y + 8, Z),
                V(K + 1, GR, Z), V(n_step[0], GF, Z), V(n_step[-1], GF, Z),
                V(2, n_step[0], 1, Z), V(2, n_step[-1], 1, Z),
                V(32, Z), V(32, Z), V(32, Z), V(32, Z), V(K, Z),
                pltpu.SemaphoreType.DMA((nsem,)), pltpu.SemaphoreType.DMA((2, nsem)),
                pltpu.SemaphoreType.DMA((3, len(groups))), pltpu.SemaphoreType.DMA((3, len(groups))),
            ],
            compiler_params=pltpu.CompilerParams(collective_id=0, has_side_effects=True),
        )(right_side, start_guess, conductivity, recycled)
        sol, res, hes = pl.pallas_call(
            deliver,
            out_shape=(shape, shape, jax.ShapeDtypeStruct(hes.shape, hes.dtype)),
            in_specs=[vm] * 3,
            out_specs=(vm,) * 3,
        )(sol, res, hes)
        return sol, res, hes.T

    return jax.shard_map(
        body,
        mesh=mesh,
        in_specs=(P(*AXES), P(*AXES), P(*AXES), P(None, *AXES)),
        out_specs=(P(*AXES), P(*AXES), P()),
        check_vma=False,
    )
```

```python
import functools
import itertools

import jax
import jax.numpy as jnp
from jax import lax
from jax.experimental import pallas as pl
from jax.experimental.pallas import tpu as pltpu
from jax.sharding import PartitionSpec as P

STEPS = 8
MESH = pl.DeviceIdType.MESH
AXES = ("px", "py", "pz")
TWO = (("py", "pz"), ("px",))
ONE = (("px", "py", "pz"),)
CHUNK = 8
GF = 4
DEEP = 3
PAIR = 2
VROWS = 24

shift_value = 0.4
SHIFT = 2.8

DIRS = [d for d in itertools.product((-1, 0, 1), repeat=3) if d != (0, 0, 0)]


def sem_counts(sizes):
    dirs = [d for d in DIRS if all(s == 0 or n > 1 for n, s in zip(sizes, d))]
    flat = sum(d[2] == 0 for d in dirs)
    tall = len(dirs) - flat
    return flat, tall // 2 if sizes[2] == 2 else tall


def shell_cells(s):
    return [(i, j) for i in range(1, s + 1) for j in range(1, s + 1) if max(i, j) == s]


def square_cells(d):
    return [(i, j) for i in range(1, d + 1) for j in range(1, d + 1)]


def kernel(
    sizes, groups,
    rhs, guess, cond, rec,
    sol_out, res_out, hes_out,
    src, img, awf,
    aface, aedge, ax, ay, ac,
    bface1, bedge1, bx1, by1, bc1,
    bface2, bedge2, bx2, by2, bc2,
    bface3, bedge3, bx3, by3, bc3,
    pack0, pface0, pedge0, zm0, zx0, zy0, zc0,
    pack1, pface1, pedge1, zm1, zx1, zy1, zc1,
    wbuf, wface, wedge, mx, my, mc, zm2, zx2, zy2, zc2,
    fields, kext, dext, temp, zext, pe,
    gpart, npart, gred1, gred2, nred1, nred2, sred1, sred2,
    mat, na, gmat, n2mat, hcols, nsq, coefa, coefb, ecoef,
    hsend, hrecv, rsend, rrecv,
):
    nsz = dict(zip(AXES, sizes))
    me = {a: lax.axis_index(a) for a in AXES}
    K, X, Y, Z = rec.shape
    NF = K + 2
    C0 = K
    XE, YE = X + 2 * DEEP, Y + 8
    NC = (NF + CHUNK - 1) // CHUNK
    f32 = jnp.float32
    lane_p = lax.broadcasted_iota(jnp.int32, (YE, Z), 1)
    lane2 = lax.broadcasted_iota(jnp.int32, (32, Z), 1)
    row2 = lax.broadcasted_iota(jnp.int32, (32, Z), 0)
    row1 = row2[:, :1]
    lane1 = lane2[:1]

    def exists(d):
        ok = None
        for a, s in zip(AXES, d):
            if s == 0:
                continue
            here = (me[a] < nsz[a] - 1) if s > 0 else (me[a] > 0)
            ok = here if ok is None else jnp.logical_and(ok, here)
        return ok

    def possible(d):
        return all(s == 0 or nsz[a] > 1 for a, s in zip(AXES, d))

    flat = [d for d in DIRS if possible(d) and d[2] == 0]
    tall = [d for d in DIRS if possible(d) and d[2] != 0]
    dirs = flat + tall
    NFLAT, NTALL = sem_counts(sizes)

    def sem_index(chunk, d):
        if d[2] == 0:
            return NTALL + chunk * NFLAT + flat.index(d)
        twin = (d[0], d[1], 1) if nsz["pz"] == 2 else d
        return tall.index(twin) % NTALL

    def target(d):
        return tuple(me[a] + s for a, s in zip(AXES, d))

    def group_info(group):
        n = 1
        rank = 0
        for a in group:
            n *= nsz[a]
            rank = rank * nsz[a] + me[a]
        return n, rank

    def member(group, r):
        co = dict(me)
        for a in reversed(group):
            co[a] = lax.rem(r, nsz[a])
            r = lax.div(r, nsz[a])
        return tuple(co[a] for a in AXES)

    def copies(sends, recvs, batch, chunk, zones):
        out = []
        for dx, dy, dz in dirs:
            if (dz != 0) not in zones:
                continue
            main, xsl, face, edge = sends(dz)
            rm, rx, ry, rc = recvs(-dz)
            hx, hy = int(dx > 0), int(dy > 0)
            if dx == 0 and dy == 0:
                s, t = main, rm
            elif dy == 0:
                s, t = main.at[:, xsl[hx]], rx.at[1 - hx]
            elif dx == 0:
                s, t = face.at[hy], ry.at[1 - hy]
            else:
                s, t = edge.at[hx, hy], rc.at[1 - hx, 1 - hy]
            d = (dx, dy, dz)
            out.append((d, pltpu.make_async_remote_copy(
                src_ref=s, dst_ref=t,
                send_sem=hsend.at[sem_index(chunk, d)], recv_sem=hrecv.at[batch, sem_index(chunk, d)],
                device_id=target(d), device_id_type=MESH,
            )))
        return out

    def start_halo(cs):
        for d, c in cs:
            pl.when(exists(d))(c.start)

    def wait_recv(cs):
        for d, c in cs:
            pl.when(exists(tuple(-s for s in d)))(c.wait_recv)

    def wait_send(cs):
        for d, c in cs:
            pl.when(exists(d))(c.wait_send)

    def ends(d):
        return pl.ds(0, d), pl.ds(X - d, d)

    def batch_copies(b, c):
        f0, f1 = c * CHUNK, min((c + 1) * CHUNK, NF)
        fs, es = pl.ds(f0, f1 - f0), pl.ds(f0, CHUNK)
        depth = DEEP if b else 1
        wholes = (img, bface1, bedge1, bx1, by1, bc1) if b else (src, aface, aedge, ax, ay, ac)
        lanes = (
            (pack1, pface1, pedge1, zm1, zx1, zy1, zc1) if b
            else (pack0, pface0, pedge0, zm0, zx0, zy0, zc0)
        )
        rows = pl.ds(f0 * X, min(CHUNK * X, aface.shape[1] - f0 * X))

        def sends(dz):
            if dz == 0:
                main, face, edge = wholes[:3]
                return main.at[fs], ends(1), face.at[:, rows], edge.at[:, :, es]
            h = int(dz > 0)
            return lanes[0].at[h], ends(depth), lanes[1].at[h], lanes[2].at[h]

        def recvs(z):
            if z == 0:
                rx, ry, rc = wholes[3:]
                return None, rx.at[:, fs], ry.at[:, rows], rc.at[:, :, es]
            h = int(z > 0)
            return tuple(r.at[h] for r in lanes[3:])

        return copies(sends, recvs, b, c % NC, (c == NC,))

    def shell_copies(s):
        face, edge, rx, ry, rc = (
            (bface2, bedge2, bx2, by2, bc2) if s == 2 else (bface3, bedge3, bx3, by3, bc3)
        )
        planes = pl.ds(s - 1, 1), pl.ds(X - s, 1)
        return copies(
            lambda dz: (img, planes, face, edge), lambda z: (None, rx, ry, rc),
            0, NC + s - 2, (False,),
        )

    def pair_copies(par):
        def sends(dz):
            return wbuf.at[par], ends(PAIR), wface.at[par], wedge.at[par]

        def recvs(z):
            if z == 0:
                return None, mx.at[par], my.at[par], mc.at[par]
            h = int(z > 0)
            return zm2.at[par, h], zx2.at[par, h], zy2.at[par, h], zc2.at[par, h]

        return copies(sends, recvs, par, 0, (False, True))

    def pack_edges(row_of, face, edge, frow, erow, depths, cells):
        for n, i in enumerate(depths):
            for x in range(X):
                at = pl.ds(frow + n * X + x, 1)
                face[0, at, :] = row_of(x, i - 1)
                face[1, at, :] = row_of(x, Y - i)
        for n, (i, j) in enumerate(cells):
            for hx, hy in itertools.product((0, 1), repeat=2):
                edge[hx, hy, pl.ds(erow + n, 1), :] = row_of(
                    X - i if hx else i - 1, Y - j if hy else j - 1
                )

    def value_rows(val):
        return lambda x, y: val[x, y : y + 1, :]

    def ref_rows(ref, f):
        return lambda x, y: ref[f, x, y : y + 1, :]

    def place_edges(dst, ry, rc, frow, erow, depths, cells):
        for n, i in enumerate(depths):
            for x in range(X):
                at = pl.ds(frow + n * X + x, 1)
                dst[DEEP + x, Y + i - 1 : Y + i, :] = ry[1, at, :]
                dst[DEEP + x, YE - i : YE - i + 1, :] = ry[0, at, :]
        for n, (i, j) in enumerate(cells):
            for hx, hy in itertools.product((0, 1), repeat=2):
                x = DEEP + X + i - 1 if hx else DEEP - i
                y = Y + j - 1 if hy else YE - j
                dst[x, y : y + 1, :] = rc[hx, hy, pl.ds(erow + n, 1), :]

    def place_shell(dst, rx, ry, rc, f, s):
        cells = shell_cells(s)
        dst[DEEP - s, 0:Y, :] = rx[0, f, 0]
        dst[DEEP + X + s - 1, 0:Y, :] = rx[1, f, 0]
        place_edges(dst, ry, rc, f * X, f * len(cells), (s,), cells)

    def place_all(dst, main, rx, ry, rc, f, depth):
        cells = square_cells(depth)
        dst[DEEP : DEEP + X, 0:Y, :] = main[f]
        dst[DEEP - depth : DEEP, 0:Y, :] = rx[0, f]
        dst[DEEP + X : DEEP + X + depth, 0:Y, :] = rx[1, f]
        place_edges(
            dst, ry, rc, f * X * depth, f * len(cells), tuple(range(1, depth + 1)), cells
        )

    def zone_plane(f, x, depth):
        low = pltpu.roll(zext[0, x], lax.rem(2 * Z - depth - depth * f, Z), 1)
        high = pltpu.roll(zext[1, x], lax.rem(Z - depth * f, Z), 1)
        return jnp.where(lane_p >= Z - depth, low, jnp.where(lane_p < depth, high, 0.0))

    def pack_lanes(get, count, depth, pack, pface, pedge):
        lane = lax.broadcasted_iota(jnp.int32, (X, Y, Z), 2)
        low = jnp.zeros((X, Y, Z), f32)
        high = jnp.zeros((X, Y, Z), f32)
        for f in range(count):
            v = get(f)
            here = jnp.logical_and(lane >= depth * f, lane < depth * (f + 1))
            low = jnp.where(here, pltpu.roll(v, depth * f, 2) if f else v, low)
            high = jnp.where(here, pltpu.roll(v, (depth * (f + 1)) % Z, 2), high)
        for h, v in ((0, low), (1, high)):
            pack[h, 0] = v
            pack_edges(
                value_rows(v), pface.at[h], pedge.at[h], 0, 0,
                tuple(range(1, depth + 1)), square_cells(depth),
            )

    def sum_zy(e, b):
        left = pltpu.roll(jnp.where(lane_p == Z - 1, b, e), 1, 1)
        right = pltpu.roll(jnp.where(lane_p == 0, b, e), Z - 1, 1)
        t = (left + right) + (e + e)
        return (pltpu.roll(t, 1, 0) + pltpu.roll(t, YE - 1, 0)) + (t + t)

    def apply(get, zone, lo, hi, rows, use):
        sums = {}
        for x in range(lo - 1, hi + 1):
            e, b = get(zone, x), get(1 - zone, x)
            k, kb = kext[zone, x], kext[1 - zone, x]
            sums[x] = (e[:rows], k[:rows], sum_zy(e, b)[:rows], sum_zy(k * e, kb * b)[:rows])
            if x > lo:
                e0, k0, s0, t0 = sums[x - 1]
                near = (sums[x - 2][2] + sums[x][2]) + (s0 + s0)
                far = (sums[x - 2][3] + sums[x][3]) + (t0 + t0)
                use(x - 1, dext[zone, x - 1, :rows] * e0 - k0 * near - far, k0)

    def make_diag(shift):
        for z in range(2):
            sums = [sum_zy(kext[z, x], kext[1 - z, x]) for x in range(XE)]
            for x in range(1, XE - 1):
                total = (sums[x - 1] + sums[x + 1]) + (sums[x] + sums[x])
                dext[z, x] = (shift_value - shift) + 64.0 * kext[z, x] + total

    def tile_sum(v):
        v = jnp.sum(v.reshape(X * Y // 8, 8, Z), axis=0)
        return jnp.sum(v, axis=0, keepdims=True)

    def reduce_start(value, bufs, slot, g):
        group = groups[g]
        n, rank = group_info(group)
        buf = bufs[g]
        buf[rank] = value
        for k in sorted(range(1, n), key=lambda k: -min(k, n - k)):
            pltpu.make_async_remote_copy(
                src_ref=buf.at[rank], dst_ref=buf.at[rank],
                send_sem=rsend.at[slot, g], recv_sem=rrecv.at[slot, g],
                device_id=member(group, lax.rem(rank + k, n)), device_id_type=MESH,
            ).start()

    def reduce_end(bufs, slot, g):
        group = groups[g]
        n, rank = group_info(group)
        buf = bufs[g]
        others = pltpu.make_async_remote_copy(
            src_ref=buf.at[pl.ds(0, n - 1)], dst_ref=buf.at[pl.ds(0, n - 1)],
            send_sem=rsend.at[slot, g], recv_sem=rrecv.at[slot, g],
            device_id=member(group, lax.rem(rank + 1, n)), device_id_type=MESH,
        )
        others.wait_recv()
        parts = [buf[r] for r in range(n)]
        while len(parts) > 1:
            parts = [sum(parts[r : r + 2][1:], parts[r]) for r in range(0, len(parts), 2)]
        others.wait_send()
        return parts[0]

    def reduce_rest(bufs, slot):
        total = reduce_end(bufs, slot, 0)
        for g in range(1, len(groups)):
            reduce_start(total, bufs, slot, g)
            total = reduce_end(bufs, slot, g)
        return total

    def clear_all(refs):
        for ref in refs:
            def clear(i, carry, ref=ref):
                ref[i] = jnp.zeros(ref.shape[1:], f32)
                return carry

            lax.fori_loop(0, ref.shape[0], clear, 0)

    clear_all((ax, ay, ac, bx1, by1, bc1, bx2, by2, bc2, bx3, by3, bc3))
    clear_all((zm0, zx0, zy0, zc0, zm1, zx1, zy1, zc1, mx, my, mc, zm2, zx2, zy2, zc2))
    barrier = pltpu.get_barrier_semaphore()
    count = jnp.int32(0)
    for group in ONE:
        n, rank = group_info(group)
        for k in range(1, n):
            pl.semaphore_signal(
                barrier, inc=1, device_id=member(group, lax.rem(rank + k, n)), device_id_type=MESH
            )
        count = count + (n - 1)

    clear_all((wface, wedge, aface, aedge, bface1, bedge1, bface2, bedge2, bface3, bedge3))
    clear_all((pface0, pedge0, pface1, pedge1))

    near_cells = shell_cells(1)

    def load_field(f, carry):
        v = rec[f]
        src[f] = v
        pack_edges(value_rows(v), aface, aedge, f * X, f, (1,), near_cells)
        return carry

    lax.fori_loop(0, K, load_field, 0)
    for f, v in ((K, guess[...]), (K + 1, 0.125 * cond[...])):
        src[f] = v
        pack_edges(value_rows(v), aface, aedge, f * X, f, (1,), near_cells)
    pack_lanes(lambda f: src[f], NF, 1, pack0, pface0, pedge0)
    pl.semaphore_wait(barrier, count)

    first = [batch_copies(0, c) for c in range(NC + 1)]
    second = [batch_copies(1, c) for c in range(NC + 1)]
    order = [NC - 1] + list(range(NC - 1))
    for c in [NC] + order:
        start_halo(first[c])
    clear_all((fields, kext, dext, zext, pe))
    temp[...] = jnp.zeros(temp.shape, f32)
    img[NF - 1] = src[NF - 1]
    pack_edges(
        ref_rows(src, NF - 1), bface1, bedge1, (NF - 1) * X, NF - 1, (1,), near_cells
    )
    wait_recv(first[NC])
    for h in range(2):
        place_all(zext.at[h], zm0.at[h], zx0.at[h], zy0.at[h], zc0.at[h], 0, 1)

    def image(f, carry):
        dst = temp.at[0]
        dst[DEEP : DEEP + X, 0:Y, :] = src[f]
        place_shell(dst, ax, ay, ac, f, 1)
        for x in range(DEEP - 1, DEEP + X + 1):
            temp[1, x] = zone_plane(f, x, 1)

        def use(x, v, k):
            img[f, x - DEEP] = v

        apply(lambda z, x: temp[z, x], 0, DEEP, DEEP + X, Y, use)
        pack_edges(ref_rows(img, f), bface1, bedge1, f * X, f, (1,), near_cells)
        return carry

    for c in order:
        wait_recv(first[c])
        if c == NC - 1:
            kext[0, DEEP : DEEP + X, 0:Y, :] = src[K + 1]
            place_shell(kext.at[0], ax, ay, ac, K + 1, 1)
            for x in range(DEEP - 1, DEEP + X + 1):
                kext[1, x] = zone_plane(K + 1, x, 1)
            make_diag(0.0)
            lax.fori_loop(c * CHUNK, K + 1, image, 0)
            img[K] = rhs[...] - img[K]
            pack_edges(ref_rows(img, K), bface1, bedge1, K * X, K, (1,), near_cells)
        else:
            lax.fori_loop(c * CHUNK, (c + 1) * CHUNK, image, 0)
        wait_send(first[c])
        start_halo(second[c])
    pack_lanes(lambda f: img[f], NF, DEEP, pack1, pface1, pedge1)
    wait_send(first[NC])
    start_halo(second[NC])

    GR = gpart.shape[1]
    GW = Z // (GR // GF)
    assert K + 1 <= GW and DEEP * NF <= Z

    def gram_part(a, carry):
        va = img[a]
        rows = [tile_sum(img[b] * va) for b in range(K + 1)]
        rows.append(jnp.zeros((GR - K - 1, Z), f32))
        gpart[a] = jnp.concatenate(rows, axis=0)
        return carry

    lax.fori_loop(0, K + 1, gram_part, 0, unroll=2)
    lane_g = lax.broadcasted_iota(jnp.int32, (GR, Z), 1)
    gram = jnp.zeros((GR, Z), f32)
    for a in range(K + 1):
        gram = jnp.where(lane_g == a, jnp.sum(gpart[a], axis=1, keepdims=True), gram)
    part = gram[:GF]
    for q in range(1, GR // GF):
        part = part + pltpu.roll(gram[GF * q : GF * q + GF], q * GW, 1)
    reduce_start(part, (gred1, gred2), 2, 0)

    shells = {2: shell_copies(2), 3: shell_copies(3)}
    for s, face, edge in ((2, bface2, bedge2), (3, bface3, bedge3)):
        cells = shell_cells(s)

        def pack_shell(f, carry, s=s, face=face, edge=edge, cells=cells):
            pack_edges(ref_rows(img, f), face, edge, f * X, f * len(cells), (s,), cells)
            return carry

        lax.fori_loop(0, NF, pack_shell, 0)
        start_halo(shells[s])

    for c in second:
        wait_recv(c)
    for h in range(2):
        place_all(zext.at[h], zm1.at[h], zx1.at[h], zy1.at[h], zc1.at[h], 0, DEEP)

    def inner(f, carry):
        fields[f, 0, DEEP : DEEP + X, 0:Y, :] = img[f]
        place_shell(fields.at[f, 0], bx1, by1, bc1, f, 1)
        for x in range(XE):
            fields[f, 1, x] = zone_plane(f, x, DEEP)
        return carry

    lax.fori_loop(0, K + 1, inner, 0)
    for x in range(XE):
        kext[1, x] = zone_plane(K + 1, x, DEEP)
    make_diag(SHIFT)

    def second_image(f, carry):
        def use(x, v, k):
            awf[f, x - DEEP] = v

        apply(lambda z, x: fields[f, z, x], 0, DEEP, DEEP + X, Y, use)
        return carry

    lax.fori_loop(0, K, second_image, 0)

    def cross_part(a, carry):
        va, vb = img[a], awf[a]
        rows = []
        for b in range(K):
            vw = awf[b]
            rows.append((tile_sum(vw * va), tile_sum(vw * vb)))
        npart[a] = jnp.concatenate([r[0] for r in rows] + [r[1] for r in rows], axis=0)
        return carry

    lax.fori_loop(0, K, cross_part, 0)
    cross = jnp.zeros((2 * K, Z), f32)
    lane_n = lax.broadcasted_iota(jnp.int32, (2 * K, Z), 1)
    for a in range(K):
        cross = jnp.where(lane_n == a, jnp.sum(npart[a], axis=1, keepdims=True), cross)
    NW = Z // (2 * K // GF)
    assert K <= NW
    part = cross[:GF]
    for q in range(1, 2 * K // GF):
        part = part + pltpu.roll(cross[GF * q : GF * q + GF], q * NW, 1)
    reduce_start(part, (nred1, nred2), 3, 0)

    def outer(s, rx, ry, rc):
        wait_recv(shells[s])

        def place(f, carry):
            place_shell(fields.at[f, 0], rx, ry, rc, f, s)
            return carry

        lax.fori_loop(0, K + 1, place, 0)
        place_shell(kext.at[0], rx, ry, rc, K + 1, s)
        make_diag(SHIFT)

    outer(2, bx2, by2, bc2)

    part = reduce_rest((gred1, gred2), 2)
    gram = [part] + [pltpu.roll(part, Z - q * GW, 1) for q in range(1, GR // GF)]
    gram = jnp.concatenate(gram, axis=0)

    lane_k = lax.broadcasted_iota(jnp.int32, (K, Z), 1)
    row_k = lax.broadcasted_iota(jnp.int32, (K, Z), 0)
    a_mat = jnp.where(lane_k < K, gram[:K], 0.0)
    gmat[...] = a_mat
    for k in range(K):
        prow = a_mat[k : k + 1, :]
        pcol = a_mat[:, k : k + 1]
        inv_p = 1.0 / a_mat[k : k + 1, k : k + 1]
        prow_s = jnp.where(lane1 == k, 1.0, prow) * inv_p
        base = jnp.where(lane_k == k, 0.0, a_mat)
        a_mat = jnp.where(row_k == k, jnp.broadcast_to(prow_s, (K, Z)), base - pcol * prow_s)
    mat[...] = jnp.where(
        row2 < VROWS, jnp.where(lane2 == row2, 1.0, 0.0),
        jnp.where(lane2 == row2 + VROWS, 1.0, 0.0),
    )
    mat[0:K, :] = a_mat
    grow = jnp.where(lane1 < K, gram[K : K + 1, :], 0.0)
    ecoef[...] = jnp.broadcast_to(jnp.sum(a_mat * grow, axis=1, keepdims=True), (K, Z))

    def begin(p, carry):
        z, x = lax.rem(p, 2), DEEP - PAIR + lax.div(p, 2)
        v = fields[C0, z, x]
        for a in range(K):
            v = v - ecoef[a : a + 1, :] * fields[a, z, x]
        fields[C0, z, x] = v
        return carry

    lax.fori_loop(0, 2 * (X + 2 * PAIR), begin, 0)
    for c in second:
        wait_send(c)
    hcols[...] = jnp.zeros((32, Z), f32)
    nsq[...] = jnp.ones((32, Z), f32)

    def col_sum(v):
        return jnp.sum(v, axis=0, keepdims=True)

    def lane_sum(v):
        return jnp.sum(v, axis=1, keepdims=True)

    def finish_cross():
        part = reduce_rest((nred1, nred2), 3)
        both = [part] + [pltpu.roll(part, Z - q * NW, 1) for q in range(1, 2 * K // GF)]
        both = jnp.where(lane_n < K, jnp.concatenate(both, axis=0), 0.0)
        na[...] = both[:K]
        n2mat[...] = both[K:]

    def record(j, c1, c2, t1, q1, q2, uu, ww):
        old = hcols[...]
        q_lane = col_sum(jnp.where((lane2 == row2 - K) & (lane2 < j), c1, 0.0))
        c3 = c2 - q1 * c1 - lane_sum(old * q_lane)
        c3 = jnp.where(row1 < VROWS, c3, 0.0)
        e_lane = col_sum(jnp.where((lane2 == row2) & (row2 < K), c3, 0.0))
        ge = lane_sum(gmat[...] * e_lane)
        now = jnp.where(row1 == K + j + 1, 1.0, c1)
        then = jnp.where(row1 == K + j + 1, q2, jnp.where(row1 == K + j + 2, 1.0, c3))
        hcols[...] = jnp.where(lane2 == j, now, jnp.where(lane2 == j + 1, then, old))
        nv = na[...]
        nv = jnp.where(lane_k == K + j, t1[:K], jnp.where(lane_k == K + j + 1, ge, nv))
        na[...] = nv
        new = jnp.where(row2 == K + j, uu, jnp.where(row2 == K + j + 1, ww, nsq[...]))
        nsq[...] = new
        fresh = jnp.logical_and(lane2 == row2, (row2 == K + j) | (row2 == K + j + 1))
        mat[...] = jnp.where(fresh, 1.0 / new, mat[...])

    pending = []
    last_sq = None
    for j in range(0, STEPS, 2):
        last = j == STEPS - 2
        par = (j // 2) % 2
        u = fields.at[C0 + j]
        p1r, p2r = pe.at[0], pe.at[1]

        for zone in range(2):
            def use(x, v, k, zone=zone):
                p1r[zone, x] = jnp.where(k > 0.0, v, 0.0)

            apply(lambda z, x: u[z, x], zone, DEEP - 1, DEEP + X + 1, YE, use)

        def use(x, v, k):
            wbuf[par, 1, x - DEEP] = v

        apply(lambda z, x: p1r[z, x], 0, DEEP, DEEP + X, Y, use)
        p1 = p1r[0, DEEP : DEEP + X, 0:Y, :]
        p2 = wbuf[par, 1]
        wbuf[par, 0] = p1
        if not last:
            for n, v in ((0, p1), (1, p2)):
                cells = square_cells(PAIR)
                pack_edges(
                    value_rows(v), wface.at[par], wedge.at[par], n * X * PAIR,
                    n * len(cells), tuple(range(1, PAIR + 1)), cells,
                )

        rows1, rows2 = [], []
        for f in range(K + j + 1):
            v = fields[f, 0, DEEP : DEEP + X, 0:Y, :]
            rows1.append(tile_sum(v * p1))
            rows2.append(tile_sum(v * p2))
        fill = [jnp.zeros((VROWS - K - j - 1, Z), f32)] if K + j + 1 < VROWS else []
        rows = rows1 + fill + rows2 + fill
        uin = u[0, DEEP : DEEP + X, 0:Y, :]
        rows += [tile_sum(p1 * p1), tile_sum(p1 * p2), tile_sum(p2 * p2), tile_sum(uin * uin)]
        rows.append(jnp.zeros((4, Z), f32))
        if last:
            rows += [tile_sum(awf[a] * p2) for a in range(K)]
        R = 2 * VROWS + 8 + (K if last else 0)
        lane_r = lax.broadcasted_iota(jnp.int32, (R, Z), 1)
        row_r = lax.broadcasted_iota(jnp.int32, (R, Z), 0)
        sums = lane_sum(jnp.concatenate(rows, axis=0))
        part = col_sum(jnp.where(lane_r == row_r, sums, 0.0))
        bufs = (sred1.at[par], sred2.at[par])
        reduce_start(part, bufs, par, 0)
        if not last:
            cs = pair_copies(par)
            if j == 0:
                for s in shells:
                    wait_send(shells[s])
            start_halo(cs)
        if j == 0:
            outer(3, bx3, by3, bc3)
            finish_cross()
        for p in pending:
            record(*p)
        if not last:
            wait_recv(cs)
            for n in range(2):
                place_all(pe.at[n, 0], wbuf.at[par], mx.at[par], my.at[par], mc.at[par], n, PAIR)
                for h in range(2):
                    place_all(
                        zext.at[h], zm2.at[par, h], zx2.at[par, h], zy2.at[par, h],
                        zc2.at[par, h], n, PAIR,
                    )
                for x in range(DEEP - PAIR, DEEP + X + PAIR):
                    pe[n, 1, x] = jnp.where(
                        lane_p >= Z - PAIR, zext[0, x],
                        jnp.where(lane_p < PAIR, zext[1, x], 0.0),
                    )
        else:
            pe[1, 0, DEEP : DEEP + X, 0:Y, :] = p2
        total = reduce_rest(bufs, par)

        m = mat[...]
        c1 = lane_sum(m * total)
        p11, p12, p22, uu = (c1[VROWS + n : VROWS + n + 1] for n in range(4))
        inv_uu = 1.0 / uu
        c1 = jnp.where(row1 == K + j, c1 * inv_uu, jnp.where(row1 < VROWS, c1, 0.0))
        t1 = lane_sum(jnp.where((lane2 == row2) & (row2 < VROWS), total, 0.0))
        t2 = lane_sum(jnp.where((lane2 == row2 + VROWS) & (row2 < K), total, 0.0))
        nv = jnp.where(lane_k == K + j, t1[:K], na[...])
        low = col_sum(nv * c1[:K])
        diff = pltpu.roll(total, Z - VROWS, 1) - low
        c2 = lane_sum(m * diff)
        c2 = jnp.where(row1 == K + j, c2 * inv_uu, jnp.where(row1 < VROWS, c2, 0.0))
        ww = p11 - col_sum(t1 * c1)
        q1 = c1[K + j : K + j + 1]
        a2e = col_sum(t2 * c1)
        q2 = (p12 - col_sum(t1 * c2) - a2e) / ww - q1
        s = q1 + q2
        cc = c2 - s * c1
        coefa[...] = jnp.broadcast_to(c1, (32, Z))
        coefb[...] = jnp.broadcast_to(jnp.where(row1 == VROWS, s, cc), (32, Z))
        pending = [(j, c1, c2, t1, q1, q2, uu, ww)]
        if last:
            a3 = lane_sum(jnp.where(lane2 == row2 + 2 * VROWS + 8, total, 0.0))[:K]
            e1 = c1[:K]
            e_lane = col_sum(jnp.where(lane_k == row_k, e1, 0.0))
            n2e = lane_sum(n2mat[...] * e_lane)
            d_col = lane_sum(jnp.where((lane2 == row2) & (row2 < VROWS), diff, 0.0))
            last_sq = (
                p22 - s * p12 + s * a2e - col_sum(e1 * (2.0 * a3 - n2e)) - col_sum(cc * d_col)
            )

        p_lo, p_n = (DEEP - 1, X + 2) if last else (0, XE)

        def combine(p, carry, j=j, p_lo=p_lo):
            z, x = lax.rem(p, 2), p_lo + lax.div(p, 2)
            t = jnp.zeros((YE, Z), f32)
            g = jnp.zeros((YE, Z), f32)
            for a in range(K):
                w = fields[a, z, x]
                t = t + coefa[a : a + 1, :] * w
                g = g + coefb[a : a + 1, :] * w
            temp[z, x] = t
            v1 = pe[0, z, x]
            g = pe[1, z, x] - coefb[VROWS : VROWS + 1, :] * v1 - g
            v1 = v1 - t
            for a in range(K, K + j + 1):
                w = fields[a, z, x]
                v1 = v1 - coefa[a : a + 1, :] * w
                g = g - coefb[a : a + 1, :] * w
            fields[C0 + j + 1, z, x] = v1
            fields[C0 + j + 2, z, x] = g
            return carry

        lax.fori_loop(0, 2 * p_n, combine, 0)
        w2 = fields.at[C0 + j + 2]
        if last:
            def use(x, v, k):
                w2[0, x, 0:Y, :] = w2[0, x, 0:Y, :] - v

            apply(lambda z, x: temp[z, x], 0, DEEP, DEEP + X, Y, use)
        else:
            for zone in range(2):
                def use(x, v, k, zone=zone):
                    w2[zone, x] = w2[zone, x] - jnp.where(k > 0.0, v, 0.0)

                apply(
                    lambda z, x: temp[z, x], zone, DEEP - PAIR, DEEP + X + PAIR, YE, use
                )
            wait_send(cs)

    for p in pending:
        record(*p)

    lane8 = lane2[:8]
    row8 = row2[:8]
    hc = hcols[...]
    n2_col = nsq[C0 : C0 + STEPS, :]
    n_col = jnp.sqrt(n2_col)
    inv_col = 1.0 / n_col
    inv_row = col_sum(jnp.where(lane8 == row8, inv_col, 0.0))
    last_n = jnp.sqrt(last_sq)
    upper = hc[C0 : C0 + STEPS] * n_col * inv_row
    upper = jnp.where(lane8 < STEPS, upper, 0.0)
    upper = jnp.where(lane8 == row8, upper + SHIFT, upper)
    bottom = jnp.where(lane1 == STEPS - 1, last_n * inv_row, 0.0)
    hes = jnp.concatenate([upper, bottom], axis=0)
    lane_t, row_t = lane2[: STEPS + 1], row2[: STEPS + 1]
    for col in range(STEPS):
        picked = jnp.where(lane_t == row_t, hes[:, col : col + 1], 0.0)
        hes_out[col : col + 1, :] = jnp.sum(picked, axis=0, keepdims=True)[:, : STEPS + 1]

    rows = [hes[i : i + 1] for i in range(STEPS + 1)]
    rows[0] = jnp.where(lane1 == STEPS, n_col[0:1], rows[0])
    for i in range(STEPS):
        top, low = rows[i][:, i : i + 1], rows[i + 1][:, i : i + 1]
        inv_r = 1.0 / jnp.sqrt(top * top + low * low)
        cs_, sn = top * inv_r, low * inv_r
        rows[i], rows[i + 1] = cs_ * rows[i] + sn * rows[i + 1], cs_ * rows[i + 1] - sn * rows[i]
    ysol = jnp.zeros((1, Z), f32)
    for i in range(STEPS - 1, -1, -1):
        known = jnp.sum(jnp.where(lane1 > i, rows[i] * ysol, 0.0), axis=1, keepdims=True)
        yi = (rows[i][:, STEPS : STEPS + 1] - known) / rows[i][:, i : i + 1]
        ysol = jnp.where(lane1 == i, yi, ysol)

    rcoef = ecoef[:, :1] - jnp.sum(hc[:K] * (ysol * inv_row), axis=1, keepdims=True)
    ycol = jnp.sum(jnp.where(lane8 == row8, ysol * inv_row, 0.0), axis=1, keepdims=True)
    hy8 = jnp.sum(upper * ysol, axis=1, keepdims=True) * inv_col[:, :1]
    hy9 = jnp.sum(bottom * ysol, axis=1, keepdims=True) / last_n
    out = guess[...]
    for a in range(K):
        out = out + rcoef[a : a + 1, :] * rec[a]
    res = fields[C0, 0, DEEP : DEEP + X, 0:Y, :]
    for i in range(STEPS):
        ui = fields[C0 + i, 0, DEEP : DEEP + X, 0:Y, :]
        out = out + ycol[i : i + 1, :] * ui
        res = res - hy8[i : i + 1, :] * ui
    res = res - hy9 * fields[C0 + STEPS, 0, DEEP : DEEP + X, 0:Y, :]
    sol_out[...] = out
    res_out[...] = res


def deliver(sol, res, hes, sol_out, res_out, hes_out):
    sol_out[...] = sol[...]
    res_out[...] = res[...]
    hes_out[...] = hes[...]


def round_up(n, m):
    return (n + m - 1) // m * m


def solution(mesh):
    sizes = tuple(mesh.shape[a] for a in AXES)

    def body(right_side, start_guess, conductivity, recycled):
        K, X, Y, Z = recycled.shape
        NF = K + 2
        FR, ER = round_up(NF * X, 8), round_up(NF, 8)
        assert X >= DEEP and Y % 8 == 0 and K + STEPS <= VROWS

        def count(group):
            n = 1
            for a in group:
                n *= mesh.shape[a]
            return n

        groups = ONE if count(AXES) <= 64 else TWO
        n_step = [count(g) for g in groups]
        nflat, ntall = sem_counts(sizes)
        chunks = (NF + CHUNK - 1) // CHUNK
        nsem = ntall + (chunks + 2) * nflat
        GR = round_up(K + 1, 8)
        XE, YE = X + 2 * DEEP, Y + 8
        V = lambda *s: pltpu.VMEM(s, jnp.float32)
        vm = pl.BlockSpec(memory_space=pltpu.VMEM)
        shape = jax.ShapeDtypeStruct((X, Y, Z), jnp.float32)

        def halo(s):
            cells = 2 * s - 1
            return [
                V(2, FR, Z), V(2, 2, ER * cells, Z),
                V(2, NF, 1, Y, Z), V(2, FR, Z), V(2, 2, ER * cells, Z),
            ]

        def lanes(d):
            rows, cells = round_up(X * d, 8), d * d
            return [
                V(2, 1, X, Y, Z), V(2, 2, rows, Z), V(2, 2, 2, cells, Z),
                V(2, 1, X, Y, Z), V(2, 2, 1, d, Y, Z), V(2, 2, rows, Z), V(2, 2, 2, cells, Z),
            ]

        prow, pcell = round_up(2 * X * PAIR, 8), 2 * PAIR * PAIR
        sol, res, hes = pl.pallas_call(
            functools.partial(kernel, sizes, groups),
            out_shape=(shape, shape, jax.ShapeDtypeStruct((STEPS, STEPS + 1), jnp.float32)),
            in_specs=[vm] * 4,
            out_specs=(vm, vm, vm),
            scratch_shapes=[
                V(NF, X, Y, Z), V(NF, X, Y, Z), V(K, X, Y, Z),
                *halo(1), *halo(1), *halo(2), *halo(3), *lanes(1), *lanes(DEEP),
                V(2, 2, X, Y, Z), V(2, 2, prow, Z), V(2, 2, 2, pcell, Z),
                V(2, 2, 2, PAIR, Y, Z), V(2, 2, prow, Z), V(2, 2, 2, pcell, Z),
                V(2, 2, 2, X, Y, Z), V(2, 2, 2, 2, PAIR, Y, Z),
                V(2, 2, 2, prow, Z), V(2, 2, 2, 2, pcell, Z),
                V(K + STEPS + 1, 2, XE, YE, Z), V(2, XE, YE, Z), V(2, XE, YE, Z),
                V(2, XE, YE, Z), V(2, XE, YE, Z), V(2, 2, XE, YE, Z),
                V(K + 1, GR, Z), V(K, 2 * K, Z),
                V(n_step[0], GF, Z), V(n_step[-1], GF, Z), V(n_step[0], GF, Z), V(n_step[-1], GF, Z),
                V(2, n_step[0], 1, Z), V(2, n_step[-1], 1, Z),
                V(32, Z), V(K, Z), V(K, Z), V(K, Z), V(32, Z), V(32, Z), V(32, Z), V(32, Z), V(K, Z),
                pltpu.SemaphoreType.DMA((nsem,)), pltpu.SemaphoreType.DMA((2, nsem)),
                pltpu.SemaphoreType.DMA((4, len(groups))), pltpu.SemaphoreType.DMA((4, len(groups))),
            ],
            compiler_params=pltpu.CompilerParams(collective_id=0, has_side_effects=True),
        )(right_side, start_guess, conductivity, recycled)
        sol, res, hes = pl.pallas_call(
            deliver,
            out_shape=(shape, shape, jax.ShapeDtypeStruct(hes.shape, hes.dtype)),
            in_specs=[vm] * 3,
            out_specs=(vm,) * 3,
        )(sol, res, hes)
        return sol, res, hes.T

    return jax.shard_map(
        body,
        mesh=mesh,
        in_specs=(P(*AXES), P(*AXES), P(*AXES), P(None, *AXES)),
        out_specs=(P(*AXES), P(*AXES), P()),
        check_vma=False,
    )
```

```python
import functools
import itertools

import jax
import jax.numpy as jnp
from jax import lax
from jax.experimental import pallas as pl
from jax.experimental.pallas import tpu as pltpu
from jax.sharding import PartitionSpec as P

STEPS = 8
MESH = pl.DeviceIdType.MESH
AXES = ("px", "py", "pz")
TWO = (("py", "pz"), ("px",))
ONE = (("px", "py", "pz"),)
CHUNK = 8
GF = 4
DEEP = 3
PAIR = 2
VROWS = 24

shift_value = 0.4
SHIFT = 2.8

DIRS = [d for d in itertools.product((-1, 0, 1), repeat=3) if d != (0, 0, 0)]


def sem_counts(sizes):
    dirs = [d for d in DIRS if all(s == 0 or n > 1 for n, s in zip(sizes, d))]
    flat = sum(d[2] == 0 for d in dirs)
    tall = len(dirs) - flat
    return flat, tall // 2 if sizes[2] == 2 else tall


def shell_cells(s):
    return [(i, j) for i in range(1, s + 1) for j in range(1, s + 1) if max(i, j) == s]


def square_cells(d):
    return [(i, j) for i in range(1, d + 1) for j in range(1, d + 1)]


def kernel(
    sizes, groups,
    rhs_hbm, guess_hbm, cond_hbm, rec_hbm,
    sol_out, res_out, hes_out,
    rhs, cond, src, img, awf,
    aface, aedge, ax, ay, ac,
    bface1, bedge1, bx1, by1, bc1,
    bface2, bedge2, bx2, by2, bc2,
    bface3, bedge3, bx3, by3, bc3,
    pack0, pface0, pedge0, zm0, zx0, zy0, zc0,
    pack1, pface1, pedge1, zm1, zx1, zy1, zc1,
    wbuf, wface, wedge, mx, my, mc, zm2, zx2, zy2, zc2,
    fields, kext, dext, temp, zext, zw, pe,
    gred1, gred2, nred1, nred2, sred1, sred2,
    mat, na, gmat, n2mat, hcols, nsq, coefa, coefb, ecoef,
    hsend, hrecv, rsend, rrecv, isem,
):
    nsz = dict(zip(AXES, sizes))
    me = {a: lax.axis_index(a) for a in AXES}
    K, X, Y, Z = rec_hbm.shape
    NF = K + 2
    C0 = K
    XE, YE = X + 2 * DEEP, Y + 8
    NC = (NF + CHUNK - 1) // CHUNK
    f32 = jnp.float32
    lane_p = lax.broadcasted_iota(jnp.int32, (YE, Z), 1)
    lane2 = lax.broadcasted_iota(jnp.int32, (32, Z), 1)
    row2 = lax.broadcasted_iota(jnp.int32, (32, Z), 0)
    row1 = row2[:, :1]
    lane1 = lane2[:1]

    pair = nsz["pz"] == 2

    def exists(d):
        ok = None
        for a, s in zip(AXES, d):
            if s == 0 or (pair and a == "pz"):
                continue
            here = (me[a] < nsz[a] - 1) if s > 0 else (me[a] > 0)
            ok = here if ok is None else jnp.logical_and(ok, here)
        return True if ok is None else ok

    def when(ok, f):
        if ok is True:
            f()
        else:
            pl.when(ok)(f)

    def possible(d):
        return all(s == 0 or nsz[a] > 1 for a, s in zip(AXES, d)) and not (pair and d[2] < 0)

    flat = [d for d in DIRS if possible(d) and d[2] == 0]
    tall = [d for d in DIRS if possible(d) and d[2] != 0]
    dirs = flat + tall
    NFLAT, NTALL = len(flat), len(tall)

    def sem_index(chunk, d):
        if d[2] == 0:
            return NTALL + chunk * NFLAT + flat.index(d)
        return tall.index(d)

    def target(d):
        x, y, z = (me[a] + s for a, s in zip(AXES, d))
        return x, y, 1 - me["pz"] if pair and d[2] else z

    def group_info(group):
        n = 1
        rank = 0
        for a in group:
            n *= nsz[a]
            rank = rank * nsz[a] + me[a]
        return n, rank

    def copies(sends, recvs, batch, chunk, zones):
        out = []
        for dx, dy, dz in dirs:
            if (dz != 0) not in zones:
                continue
            main, xsl, face, edge = sends(dz)
            side = None if dz == 0 else me["pz"] if pair else int(dz < 0)
            rm, rx, ry, rc = recvs(side)
            hx, hy = int(dx > 0), int(dy > 0)
            if dx == 0 and dy == 0:
                s, t = main, rm
            elif dy == 0:
                s, t = main.at[:, xsl[hx]], rx.at[1 - hx]
            elif dx == 0:
                s, t = face.at[hy], ry.at[1 - hy]
            else:
                s, t = edge.at[hx, hy], rc.at[1 - hx, 1 - hy]
            d = (dx, dy, dz)
            out.append((d, pltpu.make_async_remote_copy(
                src_ref=s, dst_ref=t,
                send_sem=hsend.at[sem_index(chunk, d)], recv_sem=hrecv.at[batch * (NTALL + NC * NFLAT) + sem_index(chunk, d)],
                device_id=target(d), device_id_type=MESH,
            )))
        return out

    def start_halo(cs):
        for d, c in cs:
            when(exists(d), c.start)

    def wait_recv(cs):
        for d, c in cs:
            when(exists(tuple(-s for s in d)), c.wait_recv)

    def wait_send(cs):
        for d, c in cs:
            when(exists(d), c.wait_send)

    def ends(d):
        return pl.ds(0, d), pl.ds(X - d, d)

    def batch_copies(b, c):
        f0, f1 = c * CHUNK, min((c + 1) * CHUNK, NF)
        fs, es = pl.ds(f0, f1 - f0), pl.ds(f0, CHUNK)
        depth = DEEP if b else 1
        wholes = (img, bface1, bedge1, bx1, by1, bc1) if b else (src, aface, aedge, ax, ay, ac)
        lanes = (
            (pack1, pface1, pedge1, zm1, zx1, zy1, zc1) if b
            else (pack0, pface0, pedge0, zm0, zx0, zy0, zc0)
        )
        rows = pl.ds(f0 * X, min(CHUNK * X, aface.shape[1] - f0 * X))

        def sends(dz):
            if dz == 0:
                main, face, edge = wholes[:3]
                return main.at[fs], ends(1), face.at[:, rows], edge.at[:, :, es]
            return lanes[0], ends(depth), lanes[1], lanes[2]

        def recvs(h):
            if h is None:
                rx, ry, rc = wholes[3:]
                return None, rx.at[:, fs], ry.at[:, rows], rc.at[:, :, es]
            return tuple(r.at[h] for r in lanes[3:])

        return copies(sends, recvs, b, c % NC, (c == NC,))

    def shell_copies(s):
        face, edge, rx, ry, rc = (
            (bface2, bedge2, bx2, by2, bc2) if s == 2 else (bface3, bedge3, bx3, by3, bc3)
        )
        planes = pl.ds(s - 1, 1), pl.ds(X - s, 1)
        return copies(
            lambda dz: (img, planes, face, edge), lambda h: (None, rx, ry, rc),
            1, NC + s - 2, (False,),
        )

    def pair_copies(par):
        def sends(dz):
            return wbuf.at[par], ends(PAIR), wface.at[par], wedge.at[par]

        def recvs(h):
            if h is None:
                return None, mx.at[par], my.at[par], mc.at[par]
            return zm2.at[par, h], zx2.at[par, h], zy2.at[par, h], zc2.at[par, h]

        return copies(sends, recvs, par, 0, (False, True))

    def pack_edges(row_of, face, edge, frow, erow, depths, cells):
        for n, i in enumerate(depths):
            for x in range(X):
                at = pl.ds(frow + n * X + x, 1)
                face[0, at, :] = row_of(x, i - 1)
                face[1, at, :] = row_of(x, Y - i)
        for n, (i, j) in enumerate(cells):
            for hx, hy in itertools.product((0, 1), repeat=2):
                edge[hx, hy, pl.ds(erow + n, 1), :] = row_of(
                    X - i if hx else i - 1, Y - j if hy else j - 1
                )

    def value_rows(val):
        return lambda x, y: val[x, y : y + 1, :]

    def ref_rows(ref, f):
        return lambda x, y: ref[f, x, y : y + 1, :]

    def place_edges(dst, ry, rc, frow, erow, depths, cells):
        for n, i in enumerate(depths):
            for x in range(X):
                at = pl.ds(frow + n * X + x, 1)
                dst[DEEP + x, Y + i - 1 : Y + i, :] = ry[1, at, :]
                dst[DEEP + x, YE - i : YE - i + 1, :] = ry[0, at, :]
        for n, (i, j) in enumerate(cells):
            for hx, hy in itertools.product((0, 1), repeat=2):
                x = DEEP + X + i - 1 if hx else DEEP - i
                y = Y + j - 1 if hy else YE - j
                dst[x, y : y + 1, :] = rc[hx, hy, pl.ds(erow + n, 1), :]

    def place_shell(dst, rx, ry, rc, f, s):
        cells = shell_cells(s)
        dst[DEEP - s, 0:Y, :] = rx[0, f, 0]
        dst[DEEP + X + s - 1, 0:Y, :] = rx[1, f, 0]
        place_edges(dst, ry, rc, f * X, f * len(cells), (s,), cells)

    def place_all(dst, main, rx, ry, rc, f, depth):
        cells = square_cells(depth)
        dst[DEEP : DEEP + X, 0:Y, :] = main[f]
        dst[DEEP - depth : DEEP, 0:Y, :] = rx[0, f]
        dst[DEEP + X : DEEP + X + depth, 0:Y, :] = rx[1, f]
        place_edges(
            dst, ry, rc, f * X * depth, f * len(cells), tuple(range(1, depth + 1)), cells
        )

    def slots(depth):
        return 2 * depth, lax.rem(lane_p, 2 * depth) < depth

    def zone_plane(f, x, depth):
        return pltpu.roll(zw[x], Z - depth - 2 * depth * f, 1)

    def fill_zone(depth, zm, zx, zy, zc):
        for h in range(2):
            place_all(zext.at[h], zm.at[h], zx.at[h], zy.at[h], zc.at[h], 0, depth)
        low = slots(depth)[1]
        for x in range(DEEP - depth, DEEP + X + depth):
            zw[x] = jnp.where(low, zext[0, x], zext[1, x])

    def pack_lanes(get, count, depth, pack, pface, pedge):
        lane = lax.broadcasted_iota(jnp.int32, (X, Y, Z), 2)
        width = 2 * depth
        v = jnp.zeros((X, Y, Z), f32)
        for f in range(count):
            here = jnp.logical_and(lane >= width * f, lane < width * (f + 1))
            v = jnp.where(here, pltpu.roll(get(f), width * f + depth, 2), v)
        pack[0] = v
        pack_edges(
            value_rows(v), pface, pedge, 0, 0,
            tuple(range(1, depth + 1)), square_cells(depth),
        )

    def sum_zy(e, b):
        left = pltpu.roll(jnp.where(lane_p == Z - 1, b, e), 1, 1)
        right = pltpu.roll(jnp.where(lane_p == 0, b, e), Z - 1, 1)
        t = (left + right) + (e + e)
        return (pltpu.roll(t, 1, 0) + pltpu.roll(t, YE - 1, 0)) + (t + t)

    def apply(get, zones, lo, hi, rows, use):
        planes = {}
        for x in range(lo - 1, hi + 1):
            now = []
            for z in range(2):
                e = get(z, x)
                now += [e, kext[z, x] * e]
            planes[x] = now
            if x > lo:
                sums = [
                    (a + c) + (b + b) for a, b, c in zip(planes[x - 2], planes[x - 1], now)
                ]
                for z in zones:
                    o = 1 - z
                    k0 = kext[z, x - 1, :rows]
                    near = sum_zy(sums[2 * z], sums[2 * o])[:rows]
                    far = sum_zy(sums[2 * z + 1], sums[2 * o + 1])[:rows]
                    e0 = planes[x - 1][2 * z][:rows]
                    use(z, x - 1, dext[z, x - 1, :rows] * e0 - k0 * near - far, k0)

    def make_diag(shift):
        for z in range(2):
            sums = [sum_zy(kext[z, x], kext[1 - z, x]) for x in range(XE)]
            for x in range(1, XE - 1):
                total = (sums[x - 1] + sums[x + 1]) + (sums[x] + sums[x])
                dext[z, x] = (shift_value - shift) + 64.0 * kext[z, x] + total

    lane8 = lane2[:8]
    row8 = row2[:8]

    def fold(v):
        return jnp.sum(v.reshape(X * Y // 8, 8, Z), axis=0)

    def row_sums(parts):
        parts = parts + [None] * (-len(parts) % 8)
        for d in (1, 2, 4):
            here = lax.rem(lax.div(row8, d), 2) == 0
            merged = []
            for a, b in zip(parts[::2], parts[1::2]):
                if a is None:
                    merged.append(None)
                    continue
                b = 0.0 if b is None else b
                merged.append(jnp.where(here, a, b) + pltpu.roll(jnp.where(here, b, a), d, 0))
            parts = merged
        return jnp.concatenate(
            [jnp.zeros((8, Z), f32) if p is None else p for p in parts], axis=0
        )

    def lane_sum(v):
        return jnp.sum(v, axis=1, keepdims=True)

    def col_sum(v):
        return jnp.sum(v, axis=0, keepdims=True)

    def symmetric(n, rows, dots):
        lane = lax.broadcasted_iota(jnp.int32, (rows, Z), 1)
        row = lax.broadcasted_iota(jnp.int32, (rows, Z), 0)
        out = jnp.zeros((rows, Z), f32)
        for a in range(n):
            col = lane_sum(row_sums(dots(a)))
            if col.shape[0] < rows:
                col = jnp.concatenate([col, jnp.zeros((rows - col.shape[0], 1), f32)], axis=0)
            across = col_sum(jnp.where((lane == row) & (row < a), col, 0.0))
            out = jnp.where(lane == a, col, jnp.where(row == a, across, out))
        return out

    spots = {}
    for axis in AXES:
        for o in range(nsz[axis]):
            at = me[axis] + o
            spots[axis, o] = jnp.where(at >= nsz[axis], at - nsz[axis], at) if o else at

    def peers(group):
        ways = list(itertools.product(*(range(nsz[a]) for a in group)))[1:]
        far = lambda w: -sum(min(o, nsz[a] - o) for a, o in zip(group, w))
        return [
            tuple(spots[a, w[group.index(a)]] if a in group else me[a] for a in AXES)
            for w in sorted(ways, key=far)
        ]

    def reduce_start(value, bufs, slot, g):
        group = groups[g]
        rank = group_info(group)[1]
        buf = bufs[g]
        buf[rank] = value
        for peer in peers(group):
            pltpu.make_async_remote_copy(
                src_ref=buf.at[rank], dst_ref=buf.at[rank],
                send_sem=rsend.at[slot, g], recv_sem=rrecv.at[slot, g],
                device_id=peer, device_id_type=MESH,
            ).start()

    def reduce_end(bufs, slot, g):
        group = groups[g]
        n, rank = group_info(group)
        buf = bufs[g]
        others = pltpu.make_async_remote_copy(
            src_ref=buf.at[pl.ds(0, n - 1)], dst_ref=buf.at[pl.ds(0, n - 1)],
            send_sem=rsend.at[slot, g], recv_sem=rrecv.at[slot, g],
            device_id=peers(group)[0], device_id_type=MESH,
        )
        others.wait_recv()
        parts = [buf[r] for r in range(n)]
        while len(parts) > 1:
            parts = [sum(parts[r : r + 2][1:], parts[r]) for r in range(0, len(parts), 2)]
        others.wait_send()
        return parts[0]

    def reduce_rest(bufs, slot):
        total = reduce_end(bufs, slot, 0)
        for g in range(1, len(groups)):
            reduce_start(total, bufs, slot, g)
            total = reduce_end(bufs, slot, g)
        return total

    def clear_all(refs):
        for ref in refs:
            def clear(i, carry, ref=ref):
                ref[i] = jnp.zeros(ref.shape[1:], f32)
                return carry

            lax.fori_loop(0, ref.shape[0], clear, 0)

    loads = [
        pltpu.make_async_copy(a, b, isem.at[n])
        for n, (a, b) in enumerate(
            ((cond_hbm, cond), (guess_hbm, src.at[K]), (rec_hbm, src.at[pl.ds(0, K)]), (rhs_hbm, rhs))
        )
    ]
    for c in loads:
        c.start()
    clear_all((ax, ay, ac, bx1, by1, bc1, bx2, by2, bc2, bx3, by3, bc3))
    clear_all((zm0, zx0, zy0, zc0, zm1, zx1, zy1, zc1, mx, my, mc, zm2, zx2, zy2, zc2))
    barrier = pltpu.get_barrier_semaphore()
    count = jnp.int32(0)
    for group in ONE:
        everyone = peers(group)
        for peer in everyone:
            pl.semaphore_signal(barrier, inc=1, device_id=peer, device_id_type=MESH)
        count = count + len(everyone)

    clear_all((wface, wedge, aface, aedge, bface1, bedge1, bface2, bedge2, bface3, bedge3))
    clear_all((pface0, pedge0, pface1, pedge1))

    near_cells = shell_cells(1)

    for c in loads:
        c.wait()
    src[K + 1] = 0.125 * cond[...]

    def load_field(f, carry):
        pack_edges(ref_rows(src, f), aface, aedge, f * X, f, (1,), near_cells)
        return carry

    lax.fori_loop(0, NF, load_field, 0, unroll=2)
    pack_lanes(lambda f: src[f], NF, 1, pack0, pface0, pedge0)
    pl.semaphore_wait(barrier, count)

    first = [batch_copies(0, c) for c in range(NC + 1)]
    second = [batch_copies(1, c) for c in range(NC + 1)]
    order = [NC - 1] + list(range(NC - 1))
    for c in [NC] + order:
        start_halo(first[c])
    clear_all((fields, kext, dext, zext, zw, pe))
    temp[...] = jnp.zeros(temp.shape, f32)
    img[NF - 1] = src[NF - 1]
    pack_edges(
        ref_rows(src, NF - 1), bface1, bedge1, (NF - 1) * X, NF - 1, (1,), near_cells
    )
    wait_recv(first[NC])
    fill_zone(1, zm0, zx0, zy0, zc0)

    def image(f, carry):
        dst = temp.at[0]
        dst[DEEP : DEEP + X, 0:Y, :] = src[f]
        place_shell(dst, ax, ay, ac, f, 1)
        for x in range(DEEP - 1, DEEP + X + 1):
            temp[1, x] = zone_plane(f, x, 1)

        def use(z, x, v, k):
            img[f, x - DEEP] = v

        apply(lambda z, x: temp[z, x], (0,), DEEP, DEEP + X, Y, use)
        pack_edges(ref_rows(img, f), bface1, bedge1, f * X, f, (1,), near_cells)
        return carry

    for c in order:
        wait_recv(first[c])
        if c == NC - 1:
            kext[0, DEEP : DEEP + X, 0:Y, :] = src[K + 1]
            place_shell(kext.at[0], ax, ay, ac, K + 1, 1)
            for x in range(DEEP - 1, DEEP + X + 1):
                v = zone_plane(K + 1, x, 1)
                kext[1, x] = jnp.where((lane_p < 1) | (lane_p >= Z - 1), v, 0.0)
            make_diag(0.0)
            lax.fori_loop(c * CHUNK, K + 1, image, 0)
            img[K] = rhs[...] - img[K]
            pack_edges(ref_rows(img, K), bface1, bedge1, K * X, K, (1,), near_cells)
        else:
            lax.fori_loop(c * CHUNK, (c + 1) * CHUNK, image, 0, unroll=2)
        wait_send(first[c])
        start_halo(second[c])
    pack_lanes(lambda f: img[f], NF, DEEP, pack1, pface1, pedge1)
    wait_send(first[NC])
    start_halo(second[NC])

    GR = (K + 8) // 8 * 8
    GW = Z // (GR // GF)
    assert K + 1 <= GW and 2 * DEEP * NF <= Z

    def gram_dots(a):
        va = img[a]
        return [fold(img[b] * va) for b in range(a + 1)]

    gram = symmetric(K + 1, GR, gram_dots)
    part = gram[:GF]
    for q in range(1, GR // GF):
        part = part + pltpu.roll(gram[GF * q : GF * q + GF], q * GW, 1)
    reduce_start(part, (gred1, gred2), 2, 0)

    shells = {2: shell_copies(2), 3: shell_copies(3)}
    for s, face, edge in ((2, bface2, bedge2), (3, bface3, bedge3)):
        cells = shell_cells(s)

        def pack_shell(f, carry, s=s, face=face, edge=edge, cells=cells):
            pack_edges(ref_rows(img, f), face, edge, f * X, f * len(cells), (s,), cells)
            return carry

        lax.fori_loop(0, NF, pack_shell, 0, unroll=2)
        start_halo(shells[s])

    for c in second:
        wait_recv(c)
    fill_zone(DEEP, zm1, zx1, zy1, zc1)

    def inner(f, carry):
        fields[f, 0, DEEP : DEEP + X, 0:Y, :] = img[f]
        place_shell(fields.at[f, 0], bx1, by1, bc1, f, 1)
        for x in range(XE):
            fields[f, 1, x] = zone_plane(f, x, DEEP)
        return carry

    lax.fori_loop(0, K + 1, inner, 0, unroll=4)
    for x in range(XE):
        v = zone_plane(K + 1, x, DEEP)
        kext[1, x] = jnp.where((lane_p < DEEP) | (lane_p >= Z - DEEP), v, 0.0)
    make_diag(SHIFT)

    def second_image(f, carry):
        def use(z, x, v, k):
            awf[f, x - DEEP] = v

        apply(lambda z, x: fields[f, z, x], (0,), DEEP, DEEP + X, Y, use)
        return carry

    lax.fori_loop(0, K, second_image, 0, unroll=2)

    def cross_dots(a):
        va = awf[a]
        return [fold(img[b] * va) for b in range(a + 1)]

    def square_dots(a):
        va = awf[a]
        return [fold(awf[b] * va) for b in range(a + 1)]

    cross = jnp.concatenate([symmetric(K, K, cross_dots), symmetric(K, K, square_dots)], axis=0)
    lane_n = lax.broadcasted_iota(jnp.int32, (2 * K, Z), 1)
    NW = Z // (2 * K // GF)
    assert K <= NW
    part = cross[:GF]
    for q in range(1, 2 * K // GF):
        part = part + pltpu.roll(cross[GF * q : GF * q + GF], q * NW, 1)
    reduce_start(part, (nred1, nred2), 3, 0)

    def outer(s, rx, ry, rc):
        wait_recv(shells[s])

        def place(f, carry):
            place_shell(fields.at[f, 0], rx, ry, rc, f, s)
            return carry

        lax.fori_loop(0, K + 1, place, 0, unroll=2)
        place_shell(kext.at[0], rx, ry, rc, K + 1, s)
        make_diag(SHIFT)

    outer(2, bx2, by2, bc2)

    part = reduce_rest((gred1, gred2), 2)
    gram = [part] + [pltpu.roll(part, Z - q * GW, 1) for q in range(1, GR // GF)]
    gram = jnp.concatenate(gram, axis=0)

    lane_k = lax.broadcasted_iota(jnp.int32, (K, Z), 1)
    row_k = lax.broadcasted_iota(jnp.int32, (K, Z), 0)
    a_mat = jnp.where(lane_k < K, gram[:K], 0.0)
    gmat[...] = a_mat
    for k in range(K):
        prow = a_mat[k : k + 1, :]
        pcol = a_mat[:, k : k + 1]
        inv_p = 1.0 / a_mat[k : k + 1, k : k + 1]
        prow_s = jnp.where(lane1 == k, 1.0, prow) * inv_p
        base = jnp.where(lane_k == k, 0.0, a_mat)
        a_mat = jnp.where(row_k == k, jnp.broadcast_to(prow_s, (K, Z)), base - pcol * prow_s)
    mat[...] = jnp.where(
        row2 < VROWS, jnp.where(lane2 == row2, 1.0, 0.0),
        jnp.where(lane2 == row2 + VROWS, 1.0, 0.0),
    )
    mat[0:K, :] = a_mat
    grow = jnp.where(lane1 < K, gram[K : K + 1, :], 0.0)
    ecoef[...] = jnp.broadcast_to(jnp.sum(a_mat * grow, axis=1, keepdims=True), (K, Z))

    def begin(p, carry):
        z, x = lax.rem(p, 2), DEEP - PAIR + lax.div(p, 2)
        v = fields[C0, z, x]
        for a in range(K):
            v = v - ecoef[a : a + 1, :] * fields[a, z, x]
        fields[C0, z, x] = v
        return carry

    lax.fori_loop(0, 2 * (X + 2 * PAIR), begin, 0, unroll=4)
    for c in second:
        wait_send(c)
    hcols[...] = jnp.zeros((32, Z), f32)
    nsq[...] = jnp.ones((32, Z), f32)

    def finish_cross():
        part = reduce_rest((nred1, nred2), 3)
        both = [part] + [pltpu.roll(part, Z - q * NW, 1) for q in range(1, 2 * K // GF)]
        both = jnp.where(lane_n < K, jnp.concatenate(both, axis=0), 0.0)
        na[...] = both[:K]
        n2mat[...] = both[K:]

    def record(j, c1, c2, t1, q1, q2, uu, ww):
        old = hcols[...]
        q_lane = col_sum(jnp.where((lane2 == row2 - K) & (lane2 < j), c1, 0.0))
        c3 = c2 - q1 * c1 - lane_sum(old * q_lane)
        c3 = jnp.where(row1 < VROWS, c3, 0.0)
        e_lane = col_sum(jnp.where((lane2 == row2) & (row2 < K), c3, 0.0))
        ge = lane_sum(gmat[...] * e_lane)
        now = jnp.where(row1 == K + j + 1, 1.0, c1)
        then = jnp.where(row1 == K + j + 1, q2, jnp.where(row1 == K + j + 2, 1.0, c3))
        hcols[...] = jnp.where(lane2 == j, now, jnp.where(lane2 == j + 1, then, old))
        nv = na[...]
        nv = jnp.where(lane_k == K + j, t1[:K], jnp.where(lane_k == K + j + 1, ge, nv))
        na[...] = nv
        new = jnp.where(row2 == K + j, uu, jnp.where(row2 == K + j + 1, ww, nsq[...]))
        nsq[...] = new
        fresh = jnp.logical_and(lane2 == row2, (row2 == K + j) | (row2 == K + j + 1))
        mat[...] = jnp.where(fresh, 1.0 / new, mat[...])

    pending = []
    last_sq = None
    for j in range(0, STEPS, 2):
        last = j == STEPS - 2
        par = (j // 2) % 2
        u = fields.at[C0 + j]
        p1r, p2r = pe.at[0], pe.at[1]

        def use(z, x, v, k):
            p1r[z, x] = jnp.where(k > 0.0, v, 0.0)

        apply(lambda z, x: u[z, x], (0, 1), DEEP - 1, DEEP + X + 1, YE, use)

        def use(z, x, v, k):
            wbuf[par, 1, x - DEEP] = v

        apply(lambda z, x: p1r[z, x], (0,), DEEP, DEEP + X, Y, use)
        p1 = p1r[0, DEEP : DEEP + X, 0:Y, :]
        p2 = wbuf[par, 1]
        wbuf[par, 0] = p1
        if not last:
            for n, v in ((0, p1), (1, p2)):
                cells = square_cells(PAIR)
                pack_edges(
                    value_rows(v), wface.at[par], wedge.at[par], n * X * PAIR,
                    n * len(cells), tuple(range(1, PAIR + 1)), cells,
                )

        rows1, rows2 = [], []
        for f in range(K + j + 1):
            v = fields[f, 0, DEEP : DEEP + X, 0:Y, :]
            rows1.append(fold(v * p1))
            rows2.append(fold(v * p2))
        gap = [None] * (VROWS - K - j - 1)
        uin = u[0, DEEP : DEEP + X, 0:Y, :]
        rows = rows1 + gap + rows2 + gap
        rows += [fold(p1 * p1), fold(p1 * p2), fold(p2 * p2), fold(uin * uin)] + [None] * 4
        if last:
            rows += [fold(awf[a] * p2) for a in range(K)]
        R = 2 * VROWS + 8 + (K if last else 0)
        lane_r = lax.broadcasted_iota(jnp.int32, (R, Z), 1)
        row_r = lax.broadcasted_iota(jnp.int32, (R, Z), 0)
        sums = lane_sum(row_sums(rows))
        part = col_sum(jnp.where(lane_r == row_r, sums, 0.0))
        bufs = (sred1.at[par], sred2.at[par])
        reduce_start(part, bufs, par, 0)
        if not last:
            cs = pair_copies(par)
            if j == 0:
                for s in shells:
                    wait_send(shells[s])
            start_halo(cs)
        if j == 0:
            outer(3, bx3, by3, bc3)
            finish_cross()
        for p in pending:
            record(*p)
        if not last:
            wait_recv(cs)
            for n in range(2):
                place_all(pe.at[n, 0], wbuf.at[par], mx.at[par], my.at[par], mc.at[par], n, PAIR)
                for h in range(2):
                    place_all(
                        zext.at[h], zm2.at[par, h], zx2.at[par, h], zy2.at[par, h],
                        zc2.at[par, h], n, PAIR,
                    )
                for x in range(DEEP - PAIR, DEEP + X + PAIR):
                    pe[n, 1, x] = jnp.where(
                        lane_p >= Z - PAIR, zext[0, x],
                        jnp.where(lane_p < PAIR, zext[1, x], 0.0),
                    )
        else:
            pe[1, 0, DEEP : DEEP + X, 0:Y, :] = p2
        total = reduce_rest(bufs, par)

        m = mat[...]
        c1 = lane_sum(m * total)
        p11, p12, p22, uu = (c1[VROWS + n : VROWS + n + 1] for n in range(4))
        inv_uu = 1.0 / uu
        c1 = jnp.where(row1 == K + j, c1 * inv_uu, jnp.where(row1 < VROWS, c1, 0.0))
        t1 = lane_sum(jnp.where((lane2 == row2) & (row2 < VROWS), total, 0.0))
        t2 = lane_sum(jnp.where((lane2 == row2 + VROWS) & (row2 < K), total, 0.0))
        nv = jnp.where(lane_k == K + j, t1[:K], na[...])
        low = col_sum(nv * c1[:K])
        diff = pltpu.roll(total, Z - VROWS, 1) - low
        c2 = lane_sum(m * diff)
        c2 = jnp.where(row1 == K + j, c2 * inv_uu, jnp.where(row1 < VROWS, c2, 0.0))
        ww = p11 - col_sum(t1 * c1)
        q1 = c1[K + j : K + j + 1]
        a2e = col_sum(t2 * c1)
        q2 = (p12 - col_sum(t1 * c2) - a2e) / ww - q1
        s = q1 + q2
        cc = c2 - s * c1
        coefa[...] = jnp.broadcast_to(c1, (32, Z))
        coefb[...] = jnp.broadcast_to(jnp.where(row1 == VROWS, s, cc), (32, Z))
        pending = [(j, c1, c2, t1, q1, q2, uu, ww)]
        if last:
            a3 = lane_sum(jnp.where(lane2 == row2 + 2 * VROWS + 8, total, 0.0))[:K]
            e1 = c1[:K]
            e_lane = col_sum(jnp.where(lane_k == row_k, e1, 0.0))
            n2e = lane_sum(n2mat[...] * e_lane)
            d_col = lane_sum(jnp.where((lane2 == row2) & (row2 < VROWS), diff, 0.0))
            last_sq = (
                p22 - s * p12 + s * a2e - col_sum(e1 * (2.0 * a3 - n2e)) - col_sum(cc * d_col)
            )

        p_lo, p_n = (DEEP - 1, X + 2) if last else (0, XE)

        def combine(p, carry, j=j, p_lo=p_lo):
            z, x = lax.rem(p, 2), p_lo + lax.div(p, 2)
            t = jnp.zeros((YE, Z), f32)
            g = jnp.zeros((YE, Z), f32)
            for a in range(K):
                w = fields[a, z, x]
                t = t + coefa[a : a + 1, :] * w
                g = g + coefb[a : a + 1, :] * w
            temp[z, x] = t
            v1 = pe[0, z, x]
            g = pe[1, z, x] - coefb[VROWS : VROWS + 1, :] * v1 - g
            v1 = v1 - t
            for a in range(K, K + j + 1):
                w = fields[a, z, x]
                v1 = v1 - coefa[a : a + 1, :] * w
                g = g - coefb[a : a + 1, :] * w
            fields[C0 + j + 1, z, x] = v1
            fields[C0 + j + 2, z, x] = g
            return carry

        lax.fori_loop(0, 2 * p_n, combine, 0, unroll=2)
        w2 = fields.at[C0 + j + 2]
        if last:
            def use(z, x, v, k):
                w2[0, x, 0:Y, :] = w2[0, x, 0:Y, :] - v

            apply(lambda z, x: temp[z, x], (0,), DEEP, DEEP + X, Y, use)
        else:
            def use(z, x, v, k):
                w2[z, x] = w2[z, x] - jnp.where(k > 0.0, v, 0.0)

            apply(lambda z, x: temp[z, x], (0, 1), DEEP - PAIR, DEEP + X + PAIR, YE, use)
            wait_send(cs)

    for p in pending:
        record(*p)

    hc = hcols[...]
    n2_col = nsq[C0 : C0 + STEPS, :]
    n_col = jnp.sqrt(n2_col)
    inv_col = 1.0 / n_col
    inv_row = col_sum(jnp.where(lane8 == row8, inv_col, 0.0))
    last_n = jnp.sqrt(last_sq)
    upper = hc[C0 : C0 + STEPS] * n_col * inv_row
    upper = jnp.where(lane8 < STEPS, upper, 0.0)
    upper = jnp.where(lane8 == row8, upper + SHIFT, upper)
    bottom = jnp.where(lane1 == STEPS - 1, last_n * inv_row, 0.0)
    hes = jnp.concatenate([upper, bottom], axis=0)
    lane_t, row_t = lane2[: STEPS + 1], row2[: STEPS + 1]
    for col in range(STEPS):
        picked = jnp.where(lane_t == row_t, hes[:, col : col + 1], 0.0)
        hes_out[col : col + 1, :] = jnp.sum(picked, axis=0, keepdims=True)[:, : STEPS + 1]

    rows = [hes[i : i + 1] for i in range(STEPS + 1)]
    rows[0] = jnp.where(lane1 == STEPS, n_col[0:1], rows[0])
    for i in range(STEPS):
        top, low = rows[i][:, i : i + 1], rows[i + 1][:, i : i + 1]
        inv_r = 1.0 / jnp.sqrt(top * top + low * low)
        cs_, sn = top * inv_r, low * inv_r
        rows[i], rows[i + 1] = cs_ * rows[i] + sn * rows[i + 1], cs_ * rows[i + 1] - sn * rows[i]
    ysol = jnp.zeros((1, Z), f32)
    for i in range(STEPS - 1, -1, -1):
        known = jnp.sum(jnp.where(lane1 > i, rows[i] * ysol, 0.0), axis=1, keepdims=True)
        yi = (rows[i][:, STEPS : STEPS + 1] - known) / rows[i][:, i : i + 1]
        ysol = jnp.where(lane1 == i, yi, ysol)

    rcoef = ecoef[:, :1] - jnp.sum(hc[:K] * (ysol * inv_row), axis=1, keepdims=True)
    ycol = jnp.sum(jnp.where(lane8 == row8, ysol * inv_row, 0.0), axis=1, keepdims=True)
    hy8 = jnp.sum(upper * ysol, axis=1, keepdims=True) * inv_col[:, :1]
    hy9 = jnp.sum(bottom * ysol, axis=1, keepdims=True) / last_n
    out = src[K]
    for a in range(K):
        out = out + rcoef[a : a + 1, :] * src[a]
    res = fields[C0, 0, DEEP : DEEP + X, 0:Y, :]
    for i in range(STEPS):
        ui = fields[C0 + i, 0, DEEP : DEEP + X, 0:Y, :]
        out = out + ycol[i : i + 1, :] * ui
        res = res - hy8[i : i + 1, :] * ui
    res = res - hy9 * fields[C0 + STEPS, 0, DEEP : DEEP + X, 0:Y, :]
    sol_out[...] = out
    res_out[...] = res


def deliver(sol, res, hes, sol_out, res_out, hes_out):
    sol_out[...] = sol[...]
    res_out[...] = res[...]
    hes_out[...] = hes[...]


def round_up(n, m):
    return (n + m - 1) // m * m


def solution(mesh):
    sizes = tuple(mesh.shape[a] for a in AXES)

    def body(right_side, start_guess, conductivity, recycled):
        K, X, Y, Z = recycled.shape
        NF = K + 2
        FR, ER = round_up(NF * X, 8), round_up(NF, 8)
        assert X >= DEEP and Y % 8 == 0 and K + STEPS <= VROWS

        def count(group):
            n = 1
            for a in group:
                n *= mesh.shape[a]
            return n

        groups = ONE if count(AXES) <= 64 else TWO
        n_step = [count(g) for g in groups]
        nflat, ntall = sem_counts(sizes)
        chunks = (NF + CHUNK - 1) // CHUNK
        nsem = ntall + (chunks + 2) * nflat
        nrecv = 2 * ntall + (2 * chunks + 2) * nflat
        XE, YE = X + 2 * DEEP, Y + 8
        V = lambda *s: pltpu.VMEM(s, jnp.float32)
        vm = pl.BlockSpec(memory_space=pltpu.VMEM)
        shape = jax.ShapeDtypeStruct((X, Y, Z), jnp.float32)

        def halo(s):
            cells = 2 * s - 1
            return [
                V(2, FR, Z), V(2, 2, ER * cells, Z),
                V(2, NF, 1, Y, Z), V(2, FR, Z), V(2, 2, ER * cells, Z),
            ]

        def lanes(d):
            rows, cells = round_up(X * d, 8), d * d
            return [
                V(1, X, Y, Z), V(2, rows, Z), V(2, 2, cells, Z),
                V(2, 1, X, Y, Z), V(2, 2, 1, d, Y, Z), V(2, 2, rows, Z), V(2, 2, 2, cells, Z),
            ]

        prow, pcell = round_up(2 * X * PAIR, 8), 2 * PAIR * PAIR
        sol, res, hes = pl.pallas_call(
            functools.partial(kernel, sizes, groups),
            out_shape=(shape, shape, jax.ShapeDtypeStruct((STEPS, STEPS + 1), jnp.float32)),
            in_specs=[pl.BlockSpec(memory_space=pltpu.HBM)] * 4,
            out_specs=(vm, vm, vm),
            scratch_shapes=[
                V(X, Y, Z), V(X, Y, Z), V(NF, X, Y, Z), V(NF, X, Y, Z), V(K, X, Y, Z),
                *halo(1), *halo(1), *halo(2), *halo(3), *lanes(1), *lanes(DEEP),
                V(2, 2, X, Y, Z), V(2, 2, prow, Z), V(2, 2, 2, pcell, Z),
                V(2, 2, 2, PAIR, Y, Z), V(2, 2, prow, Z), V(2, 2, 2, pcell, Z),
                V(2, 2, 2, X, Y, Z), V(2, 2, 2, 2, PAIR, Y, Z),
                V(2, 2, 2, prow, Z), V(2, 2, 2, 2, pcell, Z),
                V(K + STEPS + 1, 2, XE, YE, Z), V(2, XE, YE, Z), V(2, XE, YE, Z),
                V(2, XE, YE, Z), V(2, XE, YE, Z), V(XE, YE, Z), V(2, 2, XE, YE, Z),
                V(n_step[0], GF, Z), V(n_step[-1], GF, Z), V(n_step[0], GF, Z), V(n_step[-1], GF, Z),
                V(2, n_step[0], 1, Z), V(2, n_step[-1], 1, Z),
                V(32, Z), V(K, Z), V(K, Z), V(K, Z), V(32, Z), V(32, Z), V(32, Z), V(32, Z), V(K, Z),
                pltpu.SemaphoreType.DMA((nsem,)), pltpu.SemaphoreType.DMA((nrecv,)),
                pltpu.SemaphoreType.DMA((4, len(groups))), pltpu.SemaphoreType.DMA((4, len(groups))),
                pltpu.SemaphoreType.DMA((4,)),
            ],
            compiler_params=pltpu.CompilerParams(collective_id=0, has_side_effects=True),
        )(right_side, start_guess, conductivity, recycled)
        sol, res, hes = pl.pallas_call(
            deliver,
            out_shape=(shape, shape, jax.ShapeDtypeStruct(hes.shape, hes.dtype)),
            in_specs=[vm] * 3,
            out_specs=(vm,) * 3,
        )(sol, res, hes)
        return sol, res, hes.T

    return jax.shard_map(
        body,
        mesh=mesh,
        in_specs=(P(*AXES), P(*AXES), P(*AXES), P(None, *AXES)),
        out_specs=(P(*AXES), P(*AXES), P()),
        check_vma=False,
    )
```

```python
import functools
import itertools

import jax
import jax.numpy as jnp
from jax import lax
from jax.experimental import pallas as pl
from jax.experimental.pallas import tpu as pltpu
from jax.sharding import PartitionSpec as P

STEPS = 8
MESH = pl.DeviceIdType.MESH
AXES = ("px", "py", "pz")
TWO = (("py", "pz"), ("px",))
ONE = (("px", "py", "pz"),)
CHUNK = 8
GF = 4
DEEP = 3
PAIR = 2
VROWS = 24
VMEM = 67043328
KEPT = 10310 * 1024

shift_value = 0.4
SHIFT = 2.8

DIRS = [d for d in itertools.product((-1, 0, 1), repeat=3) if d != (0, 0, 0)]


def sem_counts(sizes):
    dirs = [d for d in DIRS if all(s == 0 or n > 1 for n, s in zip(sizes, d))]
    flat = sum(d[2] == 0 for d in dirs)
    tall = len(dirs) - flat
    return flat, tall // 2 if sizes[2] == 2 else tall


def shell_cells(s):
    return [(i, j) for i in range(1, s + 1) for j in range(1, s + 1) if max(i, j) == s]


def square_cells(d):
    return [(i, j) for i in range(1, d + 1) for j in range(1, d + 1)]


def kernel(
    sizes, groups,
    rhs_hbm, guess_hbm, cond_hbm, rec_hbm,
    sol_out, res_out, hes_out,
    rhs, cond, src, img, awf,
    aface, aedge, ax, ay, ac,
    bface1, bedge1, bx1, by1, bc1,
    bface2, bedge2, bx2, by2, bc2,
    bface3, bedge3, bx3, by3, bc3,
    pack0, pface0, pedge0, zm0, zx0, zy0, zc0,
    pack1, pface1, pedge1, zm1, zx1, zy1, zc1,
    wbuf, wface, wedge, wpack, wpface, wpedge, mx, my, mc, zm2, zx2, zy2, zc2,
    fields, kext, dext, temp, zext, zw, pe,
    gred1, gred2, nred1, nred2, sred1, sred2,
    mat, na, gmat, n2mat, hcols, nsq, coefa, coefb, ecoef,
    hsend, hrecv, rsend, rrecv, isem,
):
    nsz = dict(zip(AXES, sizes))
    me = {a: lax.axis_index(a) for a in AXES}
    K, X, Y, Z = rec_hbm.shape
    NF = K + 2
    C0 = K
    XE, YE = X + 2 * DEEP, Y + 8
    NC = (NF + CHUNK - 1) // CHUNK
    f32 = jnp.float32
    lane_p = lax.broadcasted_iota(jnp.int32, (YE, Z), 1)
    lane2 = lax.broadcasted_iota(jnp.int32, (32, Z), 1)
    row2 = lax.broadcasted_iota(jnp.int32, (32, Z), 0)
    row1 = row2[:, :1]
    lane1 = lane2[:1]

    pair = nsz["pz"] == 2

    def exists(d):
        ok = None
        for a, s in zip(AXES, d):
            if s == 0 or (pair and a == "pz"):
                continue
            here = (me[a] < nsz[a] - 1) if s > 0 else (me[a] > 0)
            ok = here if ok is None else jnp.logical_and(ok, here)
        return True if ok is None else ok

    def when(ok, f):
        if ok is True:
            f()
        else:
            pl.when(ok)(f)

    def possible(d):
        return all(s == 0 or nsz[a] > 1 for a, s in zip(AXES, d)) and not (pair and d[2] < 0)

    flat = [d for d in DIRS if possible(d) and d[2] == 0]
    tall = [d for d in DIRS if possible(d) and d[2] != 0]
    dirs = flat + tall
    NFLAT, NTALL = len(flat), len(tall)

    def sem_index(chunk, d):
        if d[2] == 0:
            return NTALL + chunk * NFLAT + flat.index(d)
        return tall.index(d)

    def target(d):
        x, y, z = (me[a] + s for a, s in zip(AXES, d))
        return x, y, 1 - me["pz"] if pair and d[2] else z

    def group_info(group):
        n = 1
        rank = 0
        for a in group:
            n *= nsz[a]
            rank = rank * nsz[a] + me[a]
        return n, rank

    def copies(sends, recvs, batch, chunk, zones):
        out = []
        for dx, dy, dz in dirs:
            if (dz != 0) not in zones:
                continue
            main, xsl, face, edge = sends(dz)
            side = None if dz == 0 else me["pz"] if pair else int(dz < 0)
            rm, rx, ry, rc = recvs(side)
            hx, hy = int(dx > 0), int(dy > 0)
            if dx == 0 and dy == 0:
                s, t = main, rm
            elif dy == 0:
                s, t = main.at[:, xsl[hx]], rx.at[1 - hx]
            elif dx == 0:
                s, t = face.at[hy], ry.at[1 - hy]
            else:
                s, t = edge.at[hx, hy], rc.at[1 - hx, 1 - hy]
            d = (dx, dy, dz)
            out.append((d, pltpu.make_async_remote_copy(
                src_ref=s, dst_ref=t,
                send_sem=hsend.at[sem_index(chunk, d)], recv_sem=hrecv.at[batch * (NTALL + NC * NFLAT) + sem_index(chunk, d)],
                device_id=target(d), device_id_type=MESH,
            )))
        return out

    def start_halo(cs):
        for d, c in cs:
            when(exists(d), c.start)

    def wait_recv(cs):
        for d, c in cs:
            when(exists(tuple(-s for s in d)), c.wait_recv)

    def wait_send(cs):
        for d, c in cs:
            when(exists(d), c.wait_send)

    def ends(d):
        return pl.ds(0, d), pl.ds(X - d, d)

    def batch_copies(b, c):
        f0, f1 = c * CHUNK, min((c + 1) * CHUNK, NF)
        fs, es = pl.ds(f0, f1 - f0), pl.ds(f0, CHUNK)
        depth = DEEP if b else 1
        wholes = (img, bface1, bedge1, bx1, by1, bc1) if b else (src, aface, aedge, ax, ay, ac)
        lanes = (
            (pack1, pface1, pedge1, zm1, zx1, zy1, zc1) if b
            else (pack0, pface0, pedge0, zm0, zx0, zy0, zc0)
        )
        rows = pl.ds(f0 * X, min(CHUNK * X, aface.shape[1] - f0 * X))

        def sends(dz):
            if dz == 0:
                main, face, edge = wholes[:3]
                return main.at[fs], ends(1), face.at[:, rows], edge.at[:, :, es]
            return lanes[0], ends(depth), lanes[1], lanes[2]

        def recvs(h):
            if h is None:
                rx, ry, rc = wholes[3:]
                return None, rx.at[:, fs], ry.at[:, rows], rc.at[:, :, es]
            return tuple(r.at[h] for r in lanes[3:])

        return copies(sends, recvs, b, c % NC, (c == NC,))

    def shell_copies(s):
        face, edge, rx, ry, rc = (
            (bface2, bedge2, bx2, by2, bc2) if s == 2 else (bface3, bedge3, bx3, by3, bc3)
        )
        planes = pl.ds(s - 1, 1), pl.ds(X - s, 1)
        return copies(
            lambda dz: (img, planes, face, edge), lambda h: (None, rx, ry, rc),
            1, NC + s - 2, (False,),
        )

    def pair_copies(par):
        def sends(dz):
            if dz == 0:
                return wbuf.at[par], ends(PAIR), wface.at[par], wedge.at[par]
            return wpack.at[par], ends(PAIR), wpface.at[par], wpedge.at[par]

        def recvs(h):
            if h is None:
                return None, mx.at[par], my.at[par], mc.at[par]
            return zm2.at[par, h], zx2.at[par, h], zy2.at[par, h], zc2.at[par, h]

        return copies(sends, recvs, par, 0, (False, True))

    def pack_edges(row_of, face, edge, frow, erow, depths, cells):
        for n, i in enumerate(depths):
            for x in range(X):
                at = pl.ds(frow + n * X + x, 1)
                face[0, at, :] = row_of(x, i - 1)
                face[1, at, :] = row_of(x, Y - i)
        for n, (i, j) in enumerate(cells):
            for hx, hy in itertools.product((0, 1), repeat=2):
                edge[hx, hy, pl.ds(erow + n, 1), :] = row_of(
                    X - i if hx else i - 1, Y - j if hy else j - 1
                )

    def value_rows(val):
        return lambda x, y: val[x, y : y + 1, :]

    def ref_rows(ref, f):
        return lambda x, y: ref[f, x, y : y + 1, :]

    def place_edges(dst, ry, rc, frow, erow, depths, cells):
        for n, i in enumerate(depths):
            for x in range(X):
                at = pl.ds(frow + n * X + x, 1)
                dst[DEEP + x, Y + i - 1 : Y + i, :] = ry[1, at, :]
                dst[DEEP + x, YE - i : YE - i + 1, :] = ry[0, at, :]
        for n, (i, j) in enumerate(cells):
            for hx, hy in itertools.product((0, 1), repeat=2):
                x = DEEP + X + i - 1 if hx else DEEP - i
                y = Y + j - 1 if hy else YE - j
                dst[x, y : y + 1, :] = rc[hx, hy, pl.ds(erow + n, 1), :]

    def place_shell(dst, rx, ry, rc, f, s):
        cells = shell_cells(s)
        dst[DEEP - s, 0:Y, :] = rx[0, f, 0]
        dst[DEEP + X + s - 1, 0:Y, :] = rx[1, f, 0]
        place_edges(dst, ry, rc, f * X, f * len(cells), (s,), cells)

    def place_all(dst, main, rx, ry, rc, f, depth):
        cells = square_cells(depth)
        dst[DEEP : DEEP + X, 0:Y, :] = main[f]
        dst[DEEP - depth : DEEP, 0:Y, :] = rx[0, f]
        dst[DEEP + X : DEEP + X + depth, 0:Y, :] = rx[1, f]
        place_edges(
            dst, ry, rc, f * X * depth, f * len(cells), tuple(range(1, depth + 1)), cells
        )

    def slots(depth):
        return 2 * depth, lax.rem(lane_p, 2 * depth) < depth

    def zone_plane(f, x, depth):
        return pltpu.roll(zw[x], Z - depth - 2 * depth * f, 1)

    def fill_zone(depth, zm, zx, zy, zc):
        for h in range(2):
            place_all(zext.at[h], zm.at[h], zx.at[h], zy.at[h], zc.at[h], 0, depth)
        low = slots(depth)[1]
        return {
            x: jnp.where(low, zext[0, x], zext[1, x])
            for x in range(DEEP - depth, DEEP + X + depth)
        }

    def keep_zone(planes):
        for x, v in planes.items():
            zw[x] = v

    def pack_lanes(get, count, depth, pack, pface, pedge):
        lane = lax.broadcasted_iota(jnp.int32, (X, Y, Z), 2)
        width = 2 * depth
        v = jnp.zeros((X, Y, Z), f32)
        for f in range(count):
            here = jnp.logical_and(lane >= width * f, lane < width * (f + 1))
            v = jnp.where(here, pltpu.roll(get(f), width * f + depth, 2), v)
        pack[0] = v
        pack_edges(
            value_rows(v), pface, pedge, 0, 0,
            tuple(range(1, depth + 1)), square_cells(depth),
        )

    def sum_zy(e, b):
        left = pltpu.roll(jnp.where(lane_p == Z - 1, b, e), 1, 1)
        right = pltpu.roll(jnp.where(lane_p == 0, b, e), Z - 1, 1)
        t = (left + right) + (e + e)
        return (pltpu.roll(t, 1, 0) + pltpu.roll(t, YE - 1, 0)) + (t + t)

    def apply(get, zones, lo, hi, rows, use):
        planes = {}
        for x in range(lo - 1, hi + 1):
            now = []
            for z in range(2):
                e = get(z, x)
                now += [e, kext[z, x] * e]
            planes[x] = now
            if x > lo:
                sums = [
                    (a + c) + (b + b) for a, b, c in zip(planes[x - 2], planes[x - 1], now)
                ]
                for z in zones:
                    o = 1 - z
                    k0 = kext[z, x - 1, :rows]
                    near = sum_zy(sums[2 * z], sums[2 * o])[:rows]
                    far = sum_zy(sums[2 * z + 1], sums[2 * o + 1])[:rows]
                    e0 = planes[x - 1][2 * z][:rows]
                    use(z, x - 1, dext[z, x - 1, :rows] * e0 - k0 * near - far, k0)

    def make_diag(shift):
        for z in range(2):
            sums = [sum_zy(kext[z, x], kext[1 - z, x]) for x in range(XE)]
            for x in range(1, XE - 1):
                total = (sums[x - 1] + sums[x + 1]) + (sums[x] + sums[x])
                dext[z, x] = (shift_value - shift) + 64.0 * kext[z, x] + total

    lane8 = lane2[:8]
    row8 = row2[:8]

    def fold(v):
        return jnp.sum(v.reshape(X * Y // 8, 8, Z), axis=0)

    def row_sums(parts):
        parts = parts + [None] * (-len(parts) % 8)
        for d in (1, 2, 4):
            here = lax.rem(lax.div(row8, d), 2) == 0
            merged = []
            for a, b in zip(parts[::2], parts[1::2]):
                if a is None:
                    merged.append(None)
                    continue
                b = 0.0 if b is None else b
                merged.append(jnp.where(here, a, b) + pltpu.roll(jnp.where(here, b, a), d, 0))
            parts = merged
        return jnp.concatenate(
            [jnp.zeros((8, Z), f32) if p is None else p for p in parts], axis=0
        )

    def lane_sum(v):
        return jnp.sum(v, axis=1, keepdims=True)

    def col_sum(v):
        return jnp.sum(v, axis=0, keepdims=True)

    def symmetric(n, rows, dots):
        lane = lax.broadcasted_iota(jnp.int32, (rows, Z), 1)
        row = lax.broadcasted_iota(jnp.int32, (rows, Z), 0)
        out = jnp.zeros((rows, Z), f32)
        for a in range(n):
            col = lane_sum(row_sums(dots(a)))
            if col.shape[0] < rows:
                col = jnp.concatenate([col, jnp.zeros((rows - col.shape[0], 1), f32)], axis=0)
            across = col_sum(jnp.where((lane == row) & (row < a), col, 0.0))
            out = jnp.where(lane == a, col, jnp.where(row == a, across, out))
        return out

    spots = {}
    for axis in AXES:
        for o in range(nsz[axis]):
            at = me[axis] + o
            spots[axis, o] = jnp.where(at >= nsz[axis], at - nsz[axis], at) if o else at

    def peers(group):
        ways = list(itertools.product(*(range(nsz[a]) for a in group)))[1:]
        far = lambda w: -sum(min(o, nsz[a] - o) for a, o in zip(group, w))
        return [
            tuple(spots[a, w[group.index(a)]] if a in group else me[a] for a in AXES)
            for w in sorted(ways, key=far)
        ]

    def reduce_start(value, bufs, slot, g):
        group = groups[g]
        rank = group_info(group)[1]
        buf = bufs[g]
        buf[rank] = value
        for peer in peers(group):
            pltpu.make_async_remote_copy(
                src_ref=buf.at[rank], dst_ref=buf.at[rank],
                send_sem=rsend.at[slot, g], recv_sem=rrecv.at[slot, g],
                device_id=peer, device_id_type=MESH,
            ).start()

    def reduce_end(bufs, slot, g):
        group = groups[g]
        n, rank = group_info(group)
        buf = bufs[g]
        others = pltpu.make_async_remote_copy(
            src_ref=buf.at[pl.ds(0, n - 1)], dst_ref=buf.at[pl.ds(0, n - 1)],
            send_sem=rsend.at[slot, g], recv_sem=rrecv.at[slot, g],
            device_id=peers(group)[0], device_id_type=MESH,
        )
        others.wait_recv()
        parts = [buf[r] for r in range(n)]
        while len(parts) > 1:
            parts = [sum(parts[r : r + 2][1:], parts[r]) for r in range(0, len(parts), 2)]
        others.wait_send()
        return parts[0]

    def reduce_rest(bufs, slot):
        total = reduce_end(bufs, slot, 0)
        for g in range(1, len(groups)):
            reduce_start(total, bufs, slot, g)
            total = reduce_end(bufs, slot, g)
        return total

    def clear_all(refs):
        for ref in refs:
            def clear(i, carry, ref=ref):
                ref[i] = jnp.zeros(ref.shape[1:], f32)
                return carry

            lax.fori_loop(0, ref.shape[0], clear, 0)

    loads = [
        pltpu.make_async_copy(a, b, isem.at[n])
        for n, (a, b) in enumerate(
            ((cond_hbm, cond), (guess_hbm, src.at[K]), (rec_hbm, src.at[pl.ds(0, K)]), (rhs_hbm, rhs))
        )
    ]
    for c in loads:
        c.start()
    clear_all((ax, ay, ac, bx1, by1, bc1, bx2, by2, bc2, bx3, by3, bc3))
    clear_all((zm0, zx0, zy0, zc0, zm1, zx1, zy1, zc1, mx, my, mc, zm2, zx2, zy2, zc2))
    barrier = pltpu.get_barrier_semaphore()
    count = jnp.int32(0)
    for group in ONE:
        everyone = peers(group)
        for peer in everyone:
            pl.semaphore_signal(barrier, inc=1, device_id=peer, device_id_type=MESH)
        count = count + len(everyone)

    clear_all((wface, wedge, wpface, wpedge, aface, aedge, bface1, bedge1, bface2, bedge2, bface3, bedge3))
    clear_all((pface0, pedge0, pface1, pedge1))

    near_cells = shell_cells(1)

    for c in loads:
        c.wait()
    src[K + 1] = 0.125 * cond[...]

    def load_field(f, carry):
        pack_edges(ref_rows(src, f), aface, aedge, f * X, f, (1,), near_cells)
        return carry

    lax.fori_loop(0, NF, load_field, 0, unroll=2)
    pack_lanes(lambda f: src[f], NF, 1, pack0, pface0, pedge0)
    pl.semaphore_wait(barrier, count)

    first = [batch_copies(0, c) for c in range(NC + 1)]
    second = [batch_copies(1, c) for c in range(NC + 1)]
    order = [NC - 1] + list(range(NC - 1))
    for c in [NC] + order:
        start_halo(first[c])
    clear_all((fields, kext, dext, zext, zw, pe))
    temp[...] = jnp.zeros(temp.shape, f32)
    img[NF - 1] = src[NF - 1]
    pack_edges(
        ref_rows(src, NF - 1), bface1, bedge1, (NF - 1) * X, NF - 1, (1,), near_cells
    )
    wait_recv(first[NC])
    keep_zone(fill_zone(1, zm0, zx0, zy0, zc0))

    def image(f, carry):
        dst = temp.at[0]
        dst[DEEP : DEEP + X, 0:Y, :] = src[f]
        place_shell(dst, ax, ay, ac, f, 1)
        for x in range(DEEP - 1, DEEP + X + 1):
            temp[1, x] = zone_plane(f, x, 1)

        def use(z, x, v, k):
            img[f, x - DEEP] = v

        apply(lambda z, x: temp[z, x], (0,), DEEP, DEEP + X, Y, use)
        pack_edges(ref_rows(img, f), bface1, bedge1, f * X, f, (1,), near_cells)
        return carry

    for c in order:
        wait_recv(first[c])
        if c == NC - 1:
            kext[0, DEEP : DEEP + X, 0:Y, :] = src[K + 1]
            place_shell(kext.at[0], ax, ay, ac, K + 1, 1)
            for x in range(DEEP - 1, DEEP + X + 1):
                v = zone_plane(K + 1, x, 1)
                kext[1, x] = jnp.where((lane_p < 1) | (lane_p >= Z - 1), v, 0.0)
            make_diag(0.0)
            lax.fori_loop(c * CHUNK, K + 1, image, 0)
            img[K] = rhs[...] - img[K]
            pack_edges(ref_rows(img, K), bface1, bedge1, K * X, K, (1,), near_cells)
        else:
            lax.fori_loop(c * CHUNK, (c + 1) * CHUNK, image, 0, unroll=2)
        wait_send(first[c])
        start_halo(second[c])
    pack_lanes(lambda f: img[f], NF, DEEP, pack1, pface1, pedge1)
    wait_send(first[NC])
    start_halo(second[NC])

    GR = (K + 8) // 8 * 8
    GW = Z // (GR // GF)
    assert K + 1 <= GW and 2 * DEEP * NF <= Z

    def gram_dots(a):
        va = img[a]
        return [fold(img[b] * va) for b in range(a + 1)]

    gram = symmetric(K + 1, GR, gram_dots)
    part = gram[:GF]
    for q in range(1, GR // GF):
        part = part + pltpu.roll(gram[GF * q : GF * q + GF], q * GW, 1)
    reduce_start(part, (gred1, gred2), 2, 0)

    shells = {2: shell_copies(2), 3: shell_copies(3)}
    for s, face, edge in ((2, bface2, bedge2), (3, bface3, bedge3)):
        cells = shell_cells(s)

        def pack_shell(f, carry, s=s, face=face, edge=edge, cells=cells):
            pack_edges(ref_rows(img, f), face, edge, f * X, f * len(cells), (s,), cells)
            return carry

        start_halo([c for c in shells[s] if c[0][1] == 0])
        lax.fori_loop(0, NF, pack_shell, 0, unroll=2)
        start_halo([c for c in shells[s] if c[0][1] != 0])

    for c in second:
        wait_recv(c)
    keep_zone(fill_zone(DEEP, zm1, zx1, zy1, zc1))

    def inner(f, carry):
        fields[f, 0, DEEP : DEEP + X, 0:Y, :] = img[f]
        place_shell(fields.at[f, 0], bx1, by1, bc1, f, 1)
        for x in range(XE):
            fields[f, 1, x] = zone_plane(f, x, DEEP)
        return carry

    lax.fori_loop(0, K + 1, inner, 0, unroll=4)
    for x in range(XE):
        v = zone_plane(K + 1, x, DEEP)
        kext[1, x] = jnp.where((lane_p < DEEP) | (lane_p >= Z - DEEP), v, 0.0)
    make_diag(SHIFT)

    def second_image(f, carry):
        def use(z, x, v, k):
            awf[f, x - DEEP] = v

        apply(lambda z, x: fields[f, z, x], (0,), DEEP, DEEP + X, Y, use)
        return carry

    lax.fori_loop(0, K, second_image, 0, unroll=2)

    def cross_dots(a):
        va = awf[a]
        return [fold(img[b] * va) for b in range(a + 1)]

    def square_dots(a):
        va = awf[a]
        return [fold(awf[b] * va) for b in range(a + 1)]

    NG = 2
    NW = Z // (K // NG)
    assert K <= NW

    def squeeze(m):
        part = m[:NG]
        for q in range(1, K // NG):
            part = part + pltpu.roll(m[NG * q : NG * q + NG], q * NW, 1)
        return part

    def unsqueeze(part):
        both = [part] + [pltpu.roll(part, Z - q * NW, 1) for q in range(1, K // NG)]
        lane = lax.broadcasted_iota(jnp.int32, (K, Z), 1)
        return jnp.where(lane < K, jnp.concatenate(both, axis=0), 0.0)

    reduce_start(squeeze(symmetric(K, K, cross_dots)), (nred1, nred2), 3, 0)

    def outer(s, rx, ry, rc):
        wait_recv(shells[s])

        def place(f, carry):
            place_shell(fields.at[f, 0], rx, ry, rc, f, s)
            return carry

        lax.fori_loop(0, K + 1, place, 0, unroll=2)
        place_shell(kext.at[0], rx, ry, rc, K + 1, s)
        make_diag(SHIFT)

    outer(2, bx2, by2, bc2)

    part = reduce_rest((gred1, gred2), 2)
    gram = [part] + [pltpu.roll(part, Z - q * GW, 1) for q in range(1, GR // GF)]
    gram = jnp.concatenate(gram, axis=0)

    lane_k = lax.broadcasted_iota(jnp.int32, (K, Z), 1)
    row_k = lax.broadcasted_iota(jnp.int32, (K, Z), 0)
    a_mat = jnp.where(lane_k < K, gram[:K], 0.0)
    gmat[...] = a_mat
    for k in range(K):
        prow = a_mat[k : k + 1, :]
        pcol = a_mat[:, k : k + 1]
        inv_p = 1.0 / a_mat[k : k + 1, k : k + 1]
        prow_s = jnp.where(lane1 == k, 1.0, prow) * inv_p
        base = jnp.where(lane_k == k, 0.0, a_mat)
        a_mat = jnp.where(row_k == k, jnp.broadcast_to(prow_s, (K, Z)), base - pcol * prow_s)
    mat[...] = jnp.where(
        row2 < VROWS, jnp.where(lane2 == row2, 1.0, 0.0),
        jnp.where(lane2 == row2 + VROWS, 1.0, 0.0),
    )
    mat[0:K, :] = a_mat
    grow = jnp.where(lane1 < K, gram[K : K + 1, :], 0.0)
    ecoef[...] = jnp.broadcast_to(jnp.sum(a_mat * grow, axis=1, keepdims=True), (K, Z))

    def begin(p, carry):
        z, x = lax.rem(p, 2), DEEP - PAIR + lax.div(p, 2)
        v = fields[C0, z, x]
        for a in range(K):
            v = v - ecoef[a : a + 1, :] * fields[a, z, x]
        fields[C0, z, x] = v
        return carry

    lax.fori_loop(0, 2 * (X + 2 * PAIR), begin, 0, unroll=4)
    for c in second:
        wait_send(c)
    hcols[...] = jnp.zeros((32, Z), f32)
    nsq[...] = jnp.ones((32, Z), f32)

    def record(j, c1, c2, t1, q1, q2, uu, ww):
        old = hcols[...]
        q_lane = col_sum(jnp.where((lane2 == row2 - K) & (lane2 < j), c1, 0.0))
        c3 = c2 - q1 * c1 - lane_sum(old * q_lane)
        c3 = jnp.where(row1 < VROWS, c3, 0.0)
        e_lane = col_sum(jnp.where((lane2 == row2) & (row2 < K), c3, 0.0))
        ge = lane_sum(gmat[...] * e_lane)
        now = jnp.where(row1 == K + j + 1, 1.0, c1)
        then = jnp.where(row1 == K + j + 1, q2, jnp.where(row1 == K + j + 2, 1.0, c3))
        hcols[...] = jnp.where(lane2 == j, now, jnp.where(lane2 == j + 1, then, old))
        nv = na[...]
        nv = jnp.where(lane_k == K + j, t1[:K], jnp.where(lane_k == K + j + 1, ge, nv))
        na[...] = nv
        new = jnp.where(row2 == K + j, uu, jnp.where(row2 == K + j + 1, ww, nsq[...]))
        nsq[...] = new
        fresh = jnp.logical_and(lane2 == row2, (row2 == K + j) | (row2 == K + j + 1))
        mat[...] = jnp.where(fresh, 1.0 / new, mat[...])

    pending = []
    last_sq = None
    for j in range(0, STEPS, 2):
        last = j == STEPS - 2
        par = (j // 2) % 2
        u = fields.at[C0 + j]
        p1r, p2r = pe.at[0], pe.at[1]

        def use(z, x, v, k):
            p1r[z, x] = jnp.where(k > 0.0, v, 0.0)

        apply(lambda z, x: u[z, x], (0, 1), DEEP - 1, DEEP + X + 1, YE, use)

        def use(z, x, v, k):
            wbuf[par, 1, x - DEEP] = v

        apply(lambda z, x: p1r[z, x], (0,), DEEP, DEEP + X, Y, use)
        p1 = p1r[0, DEEP : DEEP + X, 0:Y, :]
        p2 = wbuf[par, 1]
        wbuf[par, 0] = p1
        if not last:
            for n, v in ((0, p1), (1, p2)):
                cells = square_cells(PAIR)
                pack_edges(
                    value_rows(v), wface.at[par], wedge.at[par], n * X * PAIR,
                    n * len(cells), tuple(range(1, PAIR + 1)), cells,
                )

        rows1, rows2 = [], []
        for f in range(K + j + 1):
            v = fields[f, 0, DEEP : DEEP + X, 0:Y, :]
            rows1.append(fold(v * p1))
            rows2.append(fold(v * p2))
        gap = [None] * (VROWS - K - j - 1)
        uin = u[0, DEEP : DEEP + X, 0:Y, :]
        rows = rows1 + gap + rows2 + gap
        rows += [fold(p1 * p1), fold(p1 * p2), fold(p2 * p2), fold(uin * uin)] + [None] * 4
        if last:
            rows += [fold(awf[a] * p2) for a in range(K)]
        R = 2 * VROWS + 8 + (K if last else 0)
        lane_r = lax.broadcasted_iota(jnp.int32, (R, Z), 1)
        row_r = lax.broadcasted_iota(jnp.int32, (R, Z), 0)
        sums = lane_sum(row_sums(rows))
        part = col_sum(jnp.where(lane_r == row_r, sums, 0.0))
        bufs = (sred1.at[par], sred2.at[par])
        reduce_start(part, bufs, par, 0)
        if not last:
            pack_lanes(
                lambda n: p2 if n else p1, 2, PAIR,
                wpack.at[par], wpface.at[par], wpedge.at[par],
            )
            cs = pair_copies(par)
            if j == 0:
                for s in shells:
                    wait_send(shells[s])
            start_halo(cs)
        if j == 0:
            outer(3, bx3, by3, bc3)
            na[...] = unsqueeze(reduce_rest((nred1, nred2), 3))
            n2mat[...] = symmetric(K, K, square_dots)
        if j == STEPS - 4:
            reduce_start(squeeze(n2mat[...]), (nred1, nred2), 3, 0)
        if last:
            n2mat[...] = unsqueeze(reduce_rest((nred1, nred2), 3))
        for p in pending:
            record(*p)
        if not last:
            wait_recv(cs)
            for n in range(2):
                place_all(pe.at[n, 0], wbuf.at[par], mx.at[par], my.at[par], mc.at[par], n, PAIR)
            for x, v in fill_zone(
                PAIR, zm2.at[par], zx2.at[par], zy2.at[par], zc2.at[par]
            ).items():
                for n in range(2):
                    pe[n, 1, x] = pltpu.roll(v, Z - PAIR - 2 * PAIR * n, 1)
        else:
            pe[1, 0, DEEP : DEEP + X, 0:Y, :] = p2
        total = reduce_rest(bufs, par)

        m = mat[...]
        c1 = lane_sum(m * total)
        p11, p12, p22, uu = (c1[VROWS + n : VROWS + n + 1] for n in range(4))
        inv_uu = 1.0 / uu
        c1 = jnp.where(row1 == K + j, c1 * inv_uu, jnp.where(row1 < VROWS, c1, 0.0))
        t1 = lane_sum(jnp.where((lane2 == row2) & (row2 < VROWS), total, 0.0))
        t2 = lane_sum(jnp.where((lane2 == row2 + VROWS) & (row2 < K), total, 0.0))
        nv = jnp.where(lane_k == K + j, t1[:K], na[...])
        low = col_sum(nv * c1[:K])
        diff = pltpu.roll(total, Z - VROWS, 1) - low
        c2 = lane_sum(m * diff)
        c2 = jnp.where(row1 == K + j, c2 * inv_uu, jnp.where(row1 < VROWS, c2, 0.0))
        ww = p11 - col_sum(t1 * c1)
        q1 = c1[K + j : K + j + 1]
        a2e = col_sum(t2 * c1)
        q2 = (p12 - col_sum(t1 * c2) - a2e) / ww - q1
        s = q1 + q2
        cc = c2 - s * c1
        coefa[...] = jnp.broadcast_to(c1, (32, Z))
        coefb[...] = jnp.broadcast_to(jnp.where(row1 == VROWS, s, cc), (32, Z))
        pending = [(j, c1, c2, t1, q1, q2, uu, ww)]
        if last:
            a3 = lane_sum(jnp.where(lane2 == row2 + 2 * VROWS + 8, total, 0.0))[:K]
            e1 = c1[:K]
            e_lane = col_sum(jnp.where(lane_k == row_k, e1, 0.0))
            n2e = lane_sum(n2mat[...] * e_lane)
            d_col = lane_sum(jnp.where((lane2 == row2) & (row2 < VROWS), diff, 0.0))
            last_sq = (
                p22 - s * p12 + s * a2e - col_sum(e1 * (2.0 * a3 - n2e)) - col_sum(cc * d_col)
            )

        p_lo, p_n = (DEEP - 1, X + 2) if last else (DEEP - PAIR, X + 2 * PAIR)

        def combine(p, carry, j=j, p_lo=p_lo):
            z, x = lax.rem(p, 2), p_lo + lax.div(p, 2)
            t = jnp.zeros((YE, Z), f32)
            g = jnp.zeros((YE, Z), f32)
            for a in range(K):
                w = fields[a, z, x]
                t = t + coefa[a : a + 1, :] * w
                g = g + coefb[a : a + 1, :] * w
            temp[z, x] = t
            v1 = pe[0, z, x]
            g = pe[1, z, x] - coefb[VROWS : VROWS + 1, :] * v1 - g
            v1 = v1 - t
            for a in range(K, K + j + 1):
                w = fields[a, z, x]
                v1 = v1 - coefa[a : a + 1, :] * w
                g = g - coefb[a : a + 1, :] * w
            fields[C0 + j + 1, z, x] = v1
            fields[C0 + j + 2, z, x] = g
            return carry

        def images_only(p, carry):
            z, x = lax.rem(p, 2), lax.div(p, 2) * (XE - 1)
            t = jnp.zeros((YE, Z), f32)
            for a in range(K):
                t = t + coefa[a : a + 1, :] * fields[a, z, x]
            temp[z, x] = t
            return carry

        if not last:
            lax.fori_loop(0, 4, images_only, 0, unroll=2)
        lax.fori_loop(0, 2 * p_n, combine, 0, unroll=2)
        w2 = fields.at[C0 + j + 2]
        if last:
            def use(z, x, v, k):
                w2[0, x, 0:Y, :] = w2[0, x, 0:Y, :] - v

            apply(lambda z, x: temp[z, x], (0,), DEEP, DEEP + X, Y, use)
        else:
            def use(z, x, v, k):
                w2[z, x] = w2[z, x] - jnp.where(k > 0.0, v, 0.0)

            apply(lambda z, x: temp[z, x], (0, 1), DEEP - PAIR, DEEP + X + PAIR, YE, use)
            wait_send(cs)

    for p in pending:
        record(*p)

    hc = hcols[...]
    n2_col = nsq[C0 : C0 + STEPS, :]
    n_col = jnp.sqrt(n2_col)
    inv_col = 1.0 / n_col
    inv_row = col_sum(jnp.where(lane8 == row8, inv_col, 0.0))
    last_n = jnp.sqrt(last_sq)
    upper = hc[C0 : C0 + STEPS] * n_col * inv_row
    upper = jnp.where(lane8 < STEPS, upper, 0.0)
    upper = jnp.where(lane8 == row8, upper + SHIFT, upper)
    bottom = jnp.where(lane1 == STEPS - 1, last_n * inv_row, 0.0)
    hes = jnp.concatenate([upper, bottom], axis=0)
    lane_t, row_t = lane2[: STEPS + 1], row2[: STEPS + 1]
    for col in range(STEPS):
        picked = jnp.where(lane_t == row_t, hes[:, col : col + 1], 0.0)
        hes_out[col : col + 1, :] = jnp.sum(picked, axis=0, keepdims=True)[:, : STEPS + 1]

    rows = [hes[i : i + 1] for i in range(STEPS + 1)]
    rows[0] = jnp.where(lane1 == STEPS, n_col[0:1], rows[0])
    for i in range(STEPS):
        top, low = rows[i][:, i : i + 1], rows[i + 1][:, i : i + 1]
        inv_r = 1.0 / jnp.sqrt(top * top + low * low)
        cs_, sn = top * inv_r, low * inv_r
        rows[i], rows[i + 1] = cs_ * rows[i] + sn * rows[i + 1], cs_ * rows[i + 1] - sn * rows[i]
    ysol = jnp.zeros((1, Z), f32)
    for i in range(STEPS - 1, -1, -1):
        known = jnp.sum(jnp.where(lane1 > i, rows[i] * ysol, 0.0), axis=1, keepdims=True)
        yi = (rows[i][:, STEPS : STEPS + 1] - known) / rows[i][:, i : i + 1]
        ysol = jnp.where(lane1 == i, yi, ysol)

    rcoef = ecoef[:, :1] - jnp.sum(hc[:K] * (ysol * inv_row), axis=1, keepdims=True)
    ycol = jnp.sum(jnp.where(lane8 == row8, ysol * inv_row, 0.0), axis=1, keepdims=True)
    hy8 = jnp.sum(upper * ysol, axis=1, keepdims=True) * inv_col[:, :1]
    hy9 = jnp.sum(bottom * ysol, axis=1, keepdims=True) / last_n
    out = src[K]
    for a in range(K):
        out = out + rcoef[a : a + 1, :] * src[a]
    res = fields[C0, 0, DEEP : DEEP + X, 0:Y, :]
    for i in range(STEPS):
        ui = fields[C0 + i, 0, DEEP : DEEP + X, 0:Y, :]
        out = out + ycol[i : i + 1, :] * ui
        res = res - hy8[i : i + 1, :] * ui
    res = res - hy9 * fields[C0 + STEPS, 0, DEEP : DEEP + X, 0:Y, :]
    sol_out[...] = out
    res_out[...] = res


def deliver(sol, res, hes, sol_out, res_out, hes_out):
    sol_out[...] = sol[...]
    res_out[...] = res[...]
    hes_out[...] = hes[...]


def round_up(n, m):
    return (n + m - 1) // m * m


def solution(mesh):
    sizes = tuple(mesh.shape[a] for a in AXES)

    def body(right_side, start_guess, conductivity, recycled):
        K, X, Y, Z = recycled.shape
        NF = K + 2
        FR, ER = round_up(NF * X, 8), round_up(NF, 8)
        assert X >= DEEP and Y % 8 == 0 and K + STEPS <= VROWS

        def count(group):
            n = 1
            for a in group:
                n *= mesh.shape[a]
            return n

        groups = ONE if count(AXES) <= 64 else TWO
        n_step = [count(g) for g in groups]
        nflat, ntall = sem_counts(sizes)
        chunks = (NF + CHUNK - 1) // CHUNK
        nsem = ntall + (chunks + 2) * nflat
        nrecv = 2 * ntall + (2 * chunks + 2) * nflat
        XE, YE = X + 2 * DEEP, Y + 8
        V = lambda *s: pltpu.VMEM(s, jnp.float32)
        vm = pl.BlockSpec(memory_space=pltpu.VMEM)
        shape = jax.ShapeDtypeStruct((X, Y, Z), jnp.float32)

        def halo(s):
            cells = 2 * s - 1
            return [
                V(2, FR, Z), V(2, 2, ER * cells, Z),
                V(2, NF, 1, Y, Z), V(2, FR, Z), V(2, 2, ER * cells, Z),
            ]

        def lanes(d):
            rows, cells = round_up(X * d, 8), d * d
            return [
                V(1, X, Y, Z), V(2, rows, Z), V(2, 2, cells, Z),
                V(2, 1, X, Y, Z), V(2, 2, 1, d, Y, Z), V(2, 2, rows, Z), V(2, 2, 2, cells, Z),
            ]

        prow, pcell = round_up(2 * X * PAIR, 8), 2 * PAIR * PAIR
        lrow, lcell = round_up(X * PAIR, 8), PAIR * PAIR
        sol, res, hes = pl.pallas_call(
            functools.partial(kernel, sizes, groups),
            out_shape=(shape, shape, jax.ShapeDtypeStruct((STEPS, STEPS + 1), jnp.float32)),
            in_specs=[pl.BlockSpec(memory_space=pltpu.HBM)] * 4,
            out_specs=(vm, vm, vm),
            scratch_shapes=[
                V(X, Y, Z), V(X, Y, Z), V(NF, X, Y, Z), V(NF, X, Y, Z), V(K, X, Y, Z),
                *halo(1), *halo(1), *halo(2), *halo(3), *lanes(1), *lanes(DEEP),
                V(2, 2, X, Y, Z), V(2, 2, prow, Z), V(2, 2, 2, pcell, Z),
                V(2, 1, X, Y, Z), V(2, 2, lrow, Z), V(2, 2, 2, lcell, Z),
                V(2, 2, 2, PAIR, Y, Z), V(2, 2, prow, Z), V(2, 2, 2, pcell, Z),
                V(2, 2, 1, X, Y, Z), V(2, 2, 2, 1, PAIR, Y, Z),
                V(2, 2, 2, lrow, Z), V(2, 2, 2, 2, lcell, Z),
                V(K + STEPS + 1, 2, XE, YE, Z), V(2, XE, YE, Z), V(2, XE, YE, Z),
                V(2, XE, YE, Z), V(2, XE, YE, Z), V(XE, YE, Z), V(2, 2, XE, YE, Z),
                V(n_step[0], GF, Z), V(n_step[-1], GF, Z), V(n_step[0], 2, Z), V(n_step[-1], 2, Z),
                V(2, n_step[0], 1, Z), V(2, n_step[-1], 1, Z),
                V(32, Z), V(K, Z), V(K, Z), V(K, Z), V(32, Z), V(32, Z), V(32, Z), V(32, Z), V(K, Z),
                pltpu.SemaphoreType.DMA((nsem,)), pltpu.SemaphoreType.DMA((nrecv,)),
                pltpu.SemaphoreType.DMA((4, len(groups))), pltpu.SemaphoreType.DMA((4, len(groups))),
                pltpu.SemaphoreType.DMA((4,)),
            ],
            compiler_params=pltpu.CompilerParams(collective_id=0, has_side_effects=True, vmem_limit_bytes=VMEM - KEPT),
        )(right_side, start_guess, conductivity, recycled)
        sol, res, hes = pl.pallas_call(
            deliver,
            out_shape=(shape, shape, jax.ShapeDtypeStruct(hes.shape, hes.dtype)),
            in_specs=[vm] * 3,
            out_specs=(vm,) * 3,
            compiler_params=pltpu.CompilerParams(vmem_limit_bytes=8 * 2**20),
        )(sol, res, hes)
        return sol, res, hes.T

    return jax.shard_map(
        body,
        mesh=mesh,
        in_specs=(P(*AXES), P(*AXES), P(*AXES), P(None, *AXES)),
        out_specs=(P(*AXES), P(*AXES), P()),
        check_vma=False,
    )
```

```python
import functools
import itertools

import jax
import jax.numpy as jnp
from jax import lax
from jax.experimental import pallas as pl
from jax.experimental.pallas import tpu as pltpu
from jax.sharding import PartitionSpec as P

STEPS = 8
MESH = pl.DeviceIdType.MESH
AXES = ("px", "py", "pz")
TWO = (("py", "pz"), ("px",))
ONE = (("px", "py", "pz"),)
CHUNK = 8
GF = 4
DEEP = 3
PAIR = 2
VROWS = 24
VMEM = 67043328
KEPT = 10310 * 1024

shift_value = 0.4
SHIFT = 2.8

DIRS = [d for d in itertools.product((-1, 0, 1), repeat=3) if d != (0, 0, 0)]


def sem_counts(sizes):
    dirs = [d for d in DIRS if all(s == 0 or n > 1 for n, s in zip(sizes, d))]
    flat = sum(d[2] == 0 for d in dirs)
    tall = len(dirs) - flat
    return flat, tall // 2 if sizes[2] == 2 else tall


def shell_cells(s):
    return [(i, j) for i in range(1, s + 1) for j in range(1, s + 1) if max(i, j) == s]


def square_cells(d):
    return [(i, j) for i in range(1, d + 1) for j in range(1, d + 1)]


def kernel(
    sizes, groups,
    rhs_hbm, guess_hbm, cond_hbm, rec_hbm,
    sol_out, res_out, hes_out,
    rhs, cond, src, img, awf,
    aface, aedge, ax, ay, ac,
    bface1, bedge1, bx1, by1, bc1,
    bface2, bedge2, bx2, by2, bc2,
    bface3, bedge3, bx3, by3, bc3,
    pack0, pface0, pedge0, zm0, zx0, zy0, zc0,
    pack1, pface1, pedge1, zm1, zx1, zy1, zc1,
    wbuf, wface, wedge, wpack, wpface, wpedge, mx, my, mc, zm2, zx2, zy2, zc2,
    fields, kext, dext, temp, zext, zw, pe,
    gred1, gred2, nred1, nred2, sred1, sred2,
    mat, na, gmat, n2mat, hcols, nsq, coefa, coefb, ecoef,
    hsend, hrecv, rsend, rrecv, isem,
):
    nsz = dict(zip(AXES, sizes))
    me = {a: lax.axis_index(a) for a in AXES}
    K, X, Y, Z = rec_hbm.shape
    NF = K + 2
    C0 = K
    XE, YE = X + 2 * DEEP, Y + 8
    NC = (NF + CHUNK - 1) // CHUNK
    f32 = jnp.float32
    lane_p = lax.broadcasted_iota(jnp.int32, (YE, Z), 1)
    lane2 = lax.broadcasted_iota(jnp.int32, (32, Z), 1)
    row2 = lax.broadcasted_iota(jnp.int32, (32, Z), 0)
    row1 = row2[:, :1]
    lane1 = lane2[:1]

    pair = nsz["pz"] == 2

    def exists(d):
        ok = None
        for a, s in zip(AXES, d):
            if s == 0 or (pair and a == "pz"):
                continue
            here = (me[a] < nsz[a] - 1) if s > 0 else (me[a] > 0)
            ok = here if ok is None else jnp.logical_and(ok, here)
        return True if ok is None else ok

    def when(ok, f):
        if ok is True:
            f()
        else:
            pl.when(ok)(f)

    def possible(d):
        return all(s == 0 or nsz[a] > 1 for a, s in zip(AXES, d)) and not (pair and d[2] < 0)

    flat = [d for d in DIRS if possible(d) and d[2] == 0]
    tall = [d for d in DIRS if possible(d) and d[2] != 0]
    dirs = flat + tall
    NFLAT, NTALL = len(flat), len(tall)

    def sem_index(chunk, d):
        if d[2] == 0:
            return NTALL + chunk * NFLAT + flat.index(d)
        return tall.index(d)

    def target(d):
        x, y, z = (me[a] + s for a, s in zip(AXES, d))
        return x, y, 1 - me["pz"] if pair and d[2] else z

    def group_info(group):
        n = 1
        rank = 0
        for a in group:
            n *= nsz[a]
            rank = rank * nsz[a] + me[a]
        return n, rank

    def copies(sends, recvs, batch, chunk, zones):
        out = []
        for dx, dy, dz in dirs:
            if (dz != 0) not in zones:
                continue
            main, xsl, face, edge = sends(dz)
            side = None if dz == 0 else me["pz"] if pair else int(dz < 0)
            rm, rx, ry, rc = recvs(side)
            hx, hy = int(dx > 0), int(dy > 0)
            if dx == 0 and dy == 0:
                s, t = main, rm
            elif dy == 0:
                s, t = main.at[:, xsl[hx]], rx.at[1 - hx]
            elif dx == 0:
                s, t = face.at[hy], ry.at[1 - hy]
            else:
                s, t = edge.at[hx, hy], rc.at[1 - hx, 1 - hy]
            d = (dx, dy, dz)
            out.append((d, pltpu.make_async_remote_copy(
                src_ref=s, dst_ref=t,
                send_sem=hsend.at[sem_index(chunk, d)], recv_sem=hrecv.at[batch * (NTALL + NC * NFLAT) + sem_index(chunk, d)],
                device_id=target(d), device_id_type=MESH,
            )))
        return out

    def start_halo(cs):
        for d, c in cs:
            when(exists(d), c.start)

    def wait_recv(cs):
        for d, c in cs:
            when(exists(tuple(-s for s in d)), c.wait_recv)

    def wait_send(cs):
        for d, c in cs:
            when(exists(d), c.wait_send)

    def ends(d):
        return pl.ds(0, d), pl.ds(X - d, d)

    def batch_copies(b, c):
        f0, f1 = c * CHUNK, min((c + 1) * CHUNK, NF)
        fs, es = pl.ds(f0, f1 - f0), pl.ds(f0, CHUNK)
        depth = DEEP if b else 1
        wholes = (img, bface1, bedge1, bx1, by1, bc1) if b else (src, aface, aedge, ax, ay, ac)
        lanes = (
            (pack1, pface1, pedge1, zm1, zx1, zy1, zc1) if b
            else (pack0, pface0, pedge0, zm0, zx0, zy0, zc0)
        )
        rows = pl.ds(f0 * X, min(CHUNK * X, aface.shape[1] - f0 * X))

        def sends(dz):
            if dz == 0:
                main, face, edge = wholes[:3]
                return main.at[fs], ends(1), face.at[:, rows], edge.at[:, :, es]
            return lanes[0], ends(depth), lanes[1], lanes[2]

        def recvs(h):
            if h is None:
                rx, ry, rc = wholes[3:]
                return None, rx.at[:, fs], ry.at[:, rows], rc.at[:, :, es]
            return tuple(r.at[h] for r in lanes[3:])

        return copies(sends, recvs, b, c % NC, (c == NC,))

    def shell_copies(s):
        face, edge, rx, ry, rc = (
            (bface2, bedge2, bx2, by2, bc2) if s == 2 else (bface3, bedge3, bx3, by3, bc3)
        )
        planes = pl.ds(s - 1, 1), pl.ds(X - s, 1)
        return copies(
            lambda dz: (img, planes, face, edge), lambda h: (None, rx, ry, rc),
            1, NC + s - 2, (False,),
        )

    def pair_copies(par):
        def sends(dz):
            if dz == 0:
                return wbuf.at[par], ends(PAIR), wface.at[par], wedge.at[par]
            return wpack.at[par], ends(PAIR), wpface.at[par], wpedge.at[par]

        def recvs(h):
            if h is None:
                return None, mx.at[par], my.at[par], mc.at[par]
            return zm2.at[par, h], zx2.at[par, h], zy2.at[par, h], zc2.at[par, h]

        return copies(sends, recvs, par, 0, (False, True))

    def pack_edges(row_of, face, edge, frow, erow, depths, cells):
        for n, i in enumerate(depths):
            for x in range(X):
                at = pl.ds(frow + n * X + x, 1)
                face[0, at, :] = row_of(x, i - 1)
                face[1, at, :] = row_of(x, Y - i)
        for n, (i, j) in enumerate(cells):
            for hx, hy in itertools.product((0, 1), repeat=2):
                edge[hx, hy, pl.ds(erow + n, 1), :] = row_of(
                    X - i if hx else i - 1, Y - j if hy else j - 1
                )

    def value_rows(val):
        return lambda x, y: val[x, y : y + 1, :]

    def ref_rows(ref, f):
        return lambda x, y: ref[f, x, y : y + 1, :]

    def place_edges(dst, ry, rc, frow, erow, depths, cells):
        for n, i in enumerate(depths):
            for x in range(X):
                at = pl.ds(frow + n * X + x, 1)
                dst[DEEP + x, Y + i - 1 : Y + i, :] = ry[1, at, :]
                dst[DEEP + x, YE - i : YE - i + 1, :] = ry[0, at, :]
        for n, (i, j) in enumerate(cells):
            for hx, hy in itertools.product((0, 1), repeat=2):
                x = DEEP + X + i - 1 if hx else DEEP - i
                y = Y + j - 1 if hy else YE - j
                dst[x, y : y + 1, :] = rc[hx, hy, pl.ds(erow + n, 1), :]

    def place_shell(dst, rx, ry, rc, f, s):
        cells = shell_cells(s)
        dst[DEEP - s, 0:Y, :] = rx[0, f, 0]
        dst[DEEP + X + s - 1, 0:Y, :] = rx[1, f, 0]
        place_edges(dst, ry, rc, f * X, f * len(cells), (s,), cells)

    def place_all(dst, main, rx, ry, rc, f, depth):
        cells = square_cells(depth)
        dst[DEEP : DEEP + X, 0:Y, :] = main[f]
        dst[DEEP - depth : DEEP, 0:Y, :] = rx[0, f]
        dst[DEEP + X : DEEP + X + depth, 0:Y, :] = rx[1, f]
        place_edges(
            dst, ry, rc, f * X * depth, f * len(cells), tuple(range(1, depth + 1)), cells
        )

    def slots(depth):
        return 2 * depth, lax.rem(lane_p, 2 * depth) < depth

    def zone_plane(f, x, depth):
        return pltpu.roll(zw[x], Z - depth - 2 * depth * f, 1)

    def fill_zone(depth, zm, zx, zy, zc):
        for h in range(2):
            place_all(zext.at[h], zm.at[h], zx.at[h], zy.at[h], zc.at[h], 0, depth)
        low = slots(depth)[1]
        return {
            x: jnp.where(low, zext[0, x], zext[1, x])
            for x in range(DEEP - depth, DEEP + X + depth)
        }

    def keep_zone(planes):
        for x, v in planes.items():
            zw[x] = v

    def pack_lanes(get, count, depth, pack, pface, pedge):
        lane = lax.broadcasted_iota(jnp.int32, (X, Y, Z), 2)
        width = 2 * depth
        v = jnp.zeros((X, Y, Z), f32)
        for f in range(count):
            here = jnp.logical_and(lane >= width * f, lane < width * (f + 1))
            v = jnp.where(here, pltpu.roll(get(f), width * f + depth, 2), v)
        pack[0] = v
        pack_edges(
            value_rows(v), pface, pedge, 0, 0,
            tuple(range(1, depth + 1)), square_cells(depth),
        )

    def sum_zy(e, b):
        left = pltpu.roll(jnp.where(lane_p == Z - 1, b, e), 1, 1)
        right = pltpu.roll(jnp.where(lane_p == 0, b, e), Z - 1, 1)
        t = (left + right) + (e + e)
        return (pltpu.roll(t, 1, 0) + pltpu.roll(t, YE - 1, 0)) + (t + t)

    def apply(get, zones, lo, hi, rows, use):
        planes = {}
        for x in range(lo - 1, hi + 1):
            now = []
            for z in range(2):
                e = get(z, x)
                now += [e, kext[z, x] * e]
            planes[x] = now
            if x > lo:
                sums = [
                    (a + c) + (b + b) for a, b, c in zip(planes[x - 2], planes[x - 1], now)
                ]
                for z in zones:
                    o = 1 - z
                    k0 = kext[z, x - 1, :rows]
                    near = sum_zy(sums[2 * z], sums[2 * o])[:rows]
                    far = sum_zy(sums[2 * z + 1], sums[2 * o + 1])[:rows]
                    e0 = planes[x - 1][2 * z][:rows]
                    use(z, x - 1, dext[z, x - 1, :rows] * e0 - k0 * near - far, k0)

    def make_diag(shift):
        for z in range(2):
            sums = [sum_zy(kext[z, x], kext[1 - z, x]) for x in range(XE)]
            for x in range(1, XE - 1):
                total = (sums[x - 1] + sums[x + 1]) + (sums[x] + sums[x])
                dext[z, x] = (shift_value - shift) + 64.0 * kext[z, x] + total

    lane8 = lane2[:8]
    row8 = row2[:8]

    def fold(v):
        return jnp.sum(v.reshape(X * Y // 8, 8, Z), axis=0)

    def row_sums(parts):
        parts = parts + [None] * (-len(parts) % 8)
        for d in (1, 2, 4):
            here = lax.rem(lax.div(row8, d), 2) == 0
            merged = []
            for a, b in zip(parts[::2], parts[1::2]):
                if a is None:
                    merged.append(None)
                    continue
                b = 0.0 if b is None else b
                merged.append(jnp.where(here, a, b) + pltpu.roll(jnp.where(here, b, a), d, 0))
            parts = merged
        return jnp.concatenate(
            [jnp.zeros((8, Z), f32) if p is None else p for p in parts], axis=0
        )

    def lane_sum(v):
        return jnp.sum(v, axis=1, keepdims=True)

    def col_sum(v):
        return jnp.sum(v, axis=0, keepdims=True)

    def symmetric(n, rows, dots):
        lane = lax.broadcasted_iota(jnp.int32, (rows, Z), 1)
        row = lax.broadcasted_iota(jnp.int32, (rows, Z), 0)
        out = jnp.zeros((rows, Z), f32)
        for a in range(n):
            col = lane_sum(row_sums(dots(a)))
            if col.shape[0] < rows:
                col = jnp.concatenate([col, jnp.zeros((rows - col.shape[0], 1), f32)], axis=0)
            across = col_sum(jnp.where((lane == row) & (row < a), col, 0.0))
            out = jnp.where(lane == a, col, jnp.where(row == a, across, out))
        return out

    spots = {}
    for axis in AXES:
        for o in range(nsz[axis]):
            at = me[axis] + o
            spots[axis, o] = jnp.where(at >= nsz[axis], at - nsz[axis], at) if o else at

    def peers(group):
        ways = list(itertools.product(*(range(nsz[a]) for a in group)))[1:]
        far = lambda w: -sum(min(o, nsz[a] - o) for a, o in zip(group, w))
        return [
            tuple(spots[a, w[group.index(a)]] if a in group else me[a] for a in AXES)
            for w in sorted(ways, key=far)
        ]

    def reduce_start(value, bufs, slot, g):
        group = groups[g]
        rank = group_info(group)[1]
        buf = bufs[g]
        buf[rank] = value
        for peer in peers(group):
            pltpu.make_async_remote_copy(
                src_ref=buf.at[rank], dst_ref=buf.at[rank],
                send_sem=rsend.at[slot, g], recv_sem=rrecv.at[slot, g],
                device_id=peer, device_id_type=MESH,
            ).start()

    def reduce_end(bufs, slot, g):
        group = groups[g]
        n, rank = group_info(group)
        buf = bufs[g]
        others = pltpu.make_async_remote_copy(
            src_ref=buf.at[pl.ds(0, n - 1)], dst_ref=buf.at[pl.ds(0, n - 1)],
            send_sem=rsend.at[slot, g], recv_sem=rrecv.at[slot, g],
            device_id=peers(group)[0], device_id_type=MESH,
        )
        others.wait_recv()
        parts = [buf[r] for r in range(n)]
        while len(parts) > 1:
            parts = [sum(parts[r : r + 2][1:], parts[r]) for r in range(0, len(parts), 2)]
        others.wait_send()
        return parts[0]

    def reduce_rest(bufs, slot):
        total = reduce_end(bufs, slot, 0)
        for g in range(1, len(groups)):
            reduce_start(total, bufs, slot, g)
            total = reduce_end(bufs, slot, g)
        return total

    def clear_all(refs):
        for ref in refs:
            def clear(i, carry, ref=ref):
                ref[i] = jnp.zeros(ref.shape[1:], f32)
                return carry

            lax.fori_loop(0, ref.shape[0], clear, 0)

    loads = [
        pltpu.make_async_copy(a, b, isem.at[n])
        for n, (a, b) in enumerate(
            ((cond_hbm, cond), (guess_hbm, src.at[K]), (rec_hbm, src.at[pl.ds(0, K)]), (rhs_hbm, rhs))
        )
    ]
    for c in loads:
        c.start()
    clear_all((ax, ay, ac, bx1, by1, bc1, bx2, by2, bc2, bx3, by3, bc3))
    clear_all((zm0, zx0, zy0, zc0, zm1, zx1, zy1, zc1, mx, my, mc, zm2, zx2, zy2, zc2))
    barrier = pltpu.get_barrier_semaphore()
    count = jnp.int32(0)
    for group in ONE:
        everyone = peers(group)
        for peer in everyone:
            pl.semaphore_signal(barrier, inc=1, device_id=peer, device_id_type=MESH)
        count = count + len(everyone)

    clear_all((wface, wedge, wpface, wpedge, aface, aedge, bface1, bedge1, bface2, bedge2, bface3, bedge3))
    clear_all((pface0, pedge0, pface1, pedge1))

    near_cells = shell_cells(1)

    for c in loads:
        c.wait()
    src[K + 1] = 0.125 * cond[...]

    def load_field(f, carry):
        pack_edges(ref_rows(src, f), aface, aedge, f * X, f, (1,), near_cells)
        return carry

    lax.fori_loop(0, NF, load_field, 0, unroll=2)
    pack_lanes(lambda f: src[f], NF, 1, pack0, pface0, pedge0)
    pl.semaphore_wait(barrier, count)

    first = [batch_copies(0, c) for c in range(NC + 1)]
    second = [batch_copies(1, c) for c in range(NC + 1)]
    order = [NC - 1] + list(range(NC - 1))
    for c in [NC] + order:
        start_halo(first[c])
    clear_all((fields, kext, dext, zext, zw, pe))
    temp[...] = jnp.zeros(temp.shape, f32)
    img[NF - 1] = src[NF - 1]
    pack_edges(
        ref_rows(src, NF - 1), bface1, bedge1, (NF - 1) * X, NF - 1, (1,), near_cells
    )
    wait_recv(first[NC])
    keep_zone(fill_zone(1, zm0, zx0, zy0, zc0))

    def image(f, carry):
        dst = temp.at[0]
        dst[DEEP : DEEP + X, 0:Y, :] = src[f]
        place_shell(dst, ax, ay, ac, f, 1)
        for x in range(DEEP - 1, DEEP + X + 1):
            temp[1, x] = zone_plane(f, x, 1)

        def use(z, x, v, k):
            img[f, x - DEEP] = v

        apply(lambda z, x: temp[z, x], (0,), DEEP, DEEP + X, Y, use)
        pack_edges(ref_rows(img, f), bface1, bedge1, f * X, f, (1,), near_cells)
        return carry

    for c in order:
        wait_recv(first[c])
        if c == NC - 1:
            kext[0, DEEP : DEEP + X, 0:Y, :] = src[K + 1]
            place_shell(kext.at[0], ax, ay, ac, K + 1, 1)
            for x in range(DEEP - 1, DEEP + X + 1):
                v = zone_plane(K + 1, x, 1)
                kext[1, x] = jnp.where((lane_p < 1) | (lane_p >= Z - 1), v, 0.0)
            make_diag(0.0)
            lax.fori_loop(c * CHUNK, K + 1, image, 0)
            img[K] = rhs[...] - img[K]
            pack_edges(ref_rows(img, K), bface1, bedge1, K * X, K, (1,), near_cells)
        else:
            lax.fori_loop(c * CHUNK, (c + 1) * CHUNK, image, 0, unroll=2)
        wait_send(first[c])
        start_halo(second[c])
    pack_lanes(lambda f: img[f], NF, DEEP, pack1, pface1, pedge1)
    wait_send(first[NC])
    start_halo(second[NC])

    GR = (K + 8) // 8 * 8
    GW = Z // (GR // GF)
    assert K + 1 <= GW and 2 * DEEP * NF <= Z

    def gram_dots(a):
        va = img[a]
        return [fold(img[b] * va) for b in range(a + 1)]

    gram = symmetric(K + 1, GR, gram_dots)
    part = gram[:GF]
    for q in range(1, GR // GF):
        part = part + pltpu.roll(gram[GF * q : GF * q + GF], q * GW, 1)
    reduce_start(part, (gred1, gred2), 2, 0)

    shells = {2: shell_copies(2), 3: shell_copies(3)}
    for s, face, edge in ((2, bface2, bedge2), (3, bface3, bedge3)):
        cells = shell_cells(s)

        def pack_shell(f, carry, s=s, face=face, edge=edge, cells=cells):
            pack_edges(ref_rows(img, f), face, edge, f * X, f * len(cells), (s,), cells)
            return carry

        start_halo([c for c in shells[s] if c[0][1] == 0])
        lax.fori_loop(0, NF, pack_shell, 0, unroll=2)
        start_halo([c for c in shells[s] if c[0][1] != 0])

    for c in second:
        wait_recv(c)
    keep_zone(fill_zone(DEEP, zm1, zx1, zy1, zc1))

    def inner(f, carry):
        fields[f, 0, DEEP : DEEP + X, 0:Y, :] = img[f]
        place_shell(fields.at[f, 0], bx1, by1, bc1, f, 1)
        for x in range(XE):
            fields[f, 1, x] = zone_plane(f, x, DEEP)
        return carry

    lax.fori_loop(0, K + 1, inner, 0, unroll=4)
    for x in range(XE):
        v = zone_plane(K + 1, x, DEEP)
        kext[1, x] = jnp.where((lane_p < DEEP) | (lane_p >= Z - DEEP), v, 0.0)
    make_diag(SHIFT)

    def second_image(f, carry):
        def use(z, x, v, k):
            awf[f, x - DEEP] = v

        apply(lambda z, x: fields[f, z, x], (0,), DEEP, DEEP + X, Y, use)
        return carry

    lax.fori_loop(0, K, second_image, 0, unroll=2)

    def cross_dots(a):
        va = awf[a]
        return [fold(img[b] * va) for b in range(a + 1)]

    def square_dots(a):
        va = awf[a]
        return [fold(awf[b] * va) for b in range(a + 1)]

    NG = 2
    NW = Z // (K // NG)
    assert K <= NW

    def squeeze(m):
        part = m[:NG]
        for q in range(1, K // NG):
            part = part + pltpu.roll(m[NG * q : NG * q + NG], q * NW, 1)
        return part

    def unsqueeze(part):
        both = [part] + [pltpu.roll(part, Z - q * NW, 1) for q in range(1, K // NG)]
        lane = lax.broadcasted_iota(jnp.int32, (K, Z), 1)
        return jnp.where(lane < K, jnp.concatenate(both, axis=0), 0.0)

    reduce_start(squeeze(symmetric(K, K, cross_dots)), (nred1, nred2), 3, 0)

    def outer(s, rx, ry, rc):
        wait_recv(shells[s])

        def place(f, carry):
            place_shell(fields.at[f, 0], rx, ry, rc, f, s)
            return carry

        lax.fori_loop(0, K + 1, place, 0, unroll=2)
        place_shell(kext.at[0], rx, ry, rc, K + 1, s)
        make_diag(SHIFT)

    outer(2, bx2, by2, bc2)

    part = reduce_rest((gred1, gred2), 2)
    gram = [part] + [pltpu.roll(part, Z - q * GW, 1) for q in range(1, GR // GF)]
    gram = jnp.concatenate(gram, axis=0)

    lane_k = lax.broadcasted_iota(jnp.int32, (K, Z), 1)
    row_k = lax.broadcasted_iota(jnp.int32, (K, Z), 0)
    a_mat = jnp.where(lane_k < K, gram[:K], 0.0)
    gmat[...] = a_mat
    for k in range(K):
        prow = a_mat[k : k + 1, :]
        pcol = a_mat[:, k : k + 1]
        inv_p = 1.0 / a_mat[k : k + 1, k : k + 1]
        prow_s = jnp.where(lane1 == k, 1.0, prow) * inv_p
        base = jnp.where(lane_k == k, 0.0, a_mat)
        a_mat = jnp.where(row_k == k, jnp.broadcast_to(prow_s, (K, Z)), base - pcol * prow_s)
    mat[...] = jnp.where(
        row2 < VROWS, jnp.where(lane2 == row2, 1.0, 0.0),
        jnp.where(lane2 == row2 + VROWS, 1.0, 0.0),
    )
    mat[0:K, :] = a_mat
    grow = jnp.where(lane1 < K, gram[K : K + 1, :], 0.0)
    ecoef[...] = jnp.broadcast_to(jnp.sum(a_mat * grow, axis=1, keepdims=True), (K, Z))

    def begin(p, carry):
        z, x = lax.rem(p, 2), DEEP - PAIR + lax.div(p, 2)
        v = fields[C0, z, x]
        for a in range(K):
            v = v - ecoef[a : a + 1, :] * fields[a, z, x]
        fields[C0, z, x] = v
        return carry

    lax.fori_loop(0, 2 * (X + 2 * PAIR), begin, 0, unroll=4)
    for c in second:
        wait_send(c)
    hcols[...] = jnp.zeros((32, Z), f32)
    nsq[...] = jnp.ones((32, Z), f32)

    def record(j, c1, c2, t1, q1, q2, uu, ww):
        old = hcols[...]
        q_lane = col_sum(jnp.where((lane2 == row2 - K) & (lane2 < j), c1, 0.0))
        c3 = c2 - q1 * c1 - lane_sum(old * q_lane)
        c3 = jnp.where(row1 < VROWS, c3, 0.0)
        e_lane = col_sum(jnp.where((lane2 == row2) & (row2 < K), c3, 0.0))
        ge = lane_sum(gmat[...] * e_lane)
        now = jnp.where(row1 == K + j + 1, 1.0, c1)
        then = jnp.where(row1 == K + j + 1, q2, jnp.where(row1 == K + j + 2, 1.0, c3))
        hcols[...] = jnp.where(lane2 == j, now, jnp.where(lane2 == j + 1, then, old))
        nv = na[...]
        nv = jnp.where(lane_k == K + j, t1[:K], jnp.where(lane_k == K + j + 1, ge, nv))
        na[...] = nv
        new = jnp.where(row2 == K + j, uu, jnp.where(row2 == K + j + 1, ww, nsq[...]))
        nsq[...] = new
        fresh = jnp.logical_and(lane2 == row2, (row2 == K + j) | (row2 == K + j + 1))
        mat[...] = jnp.where(fresh, 1.0 / new, mat[...])

    pending = []
    last_sq = None
    for j in range(0, STEPS, 2):
        last = j == STEPS - 2
        par = (j // 2) % 2
        u = fields.at[C0 + j]
        p1r, p2r = pe.at[0], pe.at[1]

        def use(z, x, v, k):
            p1r[z, x] = jnp.where(k > 0.0, v, 0.0)

        apply(lambda z, x: u[z, x], (0, 1), DEEP - 1, DEEP + X + 1, YE, use)

        def use(z, x, v, k):
            wbuf[par, 1, x - DEEP] = v

        apply(lambda z, x: p1r[z, x], (0,), DEEP, DEEP + X, Y, use)
        p1 = p1r[0, DEEP : DEEP + X, 0:Y, :]
        p2 = wbuf[par, 1]
        wbuf[par, 0] = p1
        if not last:
            for n, v in ((0, p1), (1, p2)):
                cells = square_cells(PAIR)
                pack_edges(
                    value_rows(v), wface.at[par], wedge.at[par], n * X * PAIR,
                    n * len(cells), tuple(range(1, PAIR + 1)), cells,
                )

        rows1, rows2 = [], []
        for f in range(K + j + 1):
            v = fields[f, 0, DEEP : DEEP + X, 0:Y, :]
            rows1.append(fold(v * p1))
            rows2.append(fold(v * p2))
        gap = [None] * (VROWS - K - j - 1)
        uin = u[0, DEEP : DEEP + X, 0:Y, :]
        rows = rows1 + gap + rows2 + gap
        rows += [fold(p1 * p1), fold(p1 * p2), fold(p2 * p2), fold(uin * uin)] + [None] * 4
        if last:
            rows += [fold(awf[a] * p2) for a in range(K)]
        R = 2 * VROWS + 8 + (K if last else 0)
        lane_r = lax.broadcasted_iota(jnp.int32, (R, Z), 1)
        row_r = lax.broadcasted_iota(jnp.int32, (R, Z), 0)
        sums = lane_sum(row_sums(rows))
        part = col_sum(jnp.where(lane_r == row_r, sums, 0.0))
        bufs = (sred1.at[par], sred2.at[par])
        reduce_start(part, bufs, par, 0)
        if not last:
            pack_lanes(
                lambda n: p2 if n else p1, 2, PAIR,
                wpack.at[par], wpface.at[par], wpedge.at[par],
            )
            cs = pair_copies(par)
            if j == 0:
                for s in shells:
                    wait_send(shells[s])
            start_halo(cs)
        if j == 0:
            outer(3, bx3, by3, bc3)
            na[...] = unsqueeze(reduce_rest((nred1, nred2), 3))
            n2mat[...] = symmetric(K, K, square_dots)
        if j == STEPS - 4:
            reduce_start(squeeze(n2mat[...]), (nred1, nred2), 3, 0)
        if last:
            n2mat[...] = unsqueeze(reduce_rest((nred1, nred2), 3))
        for p in pending:
            record(*p)
        if not last:
            wait_recv(cs)
            for n in range(2):
                place_all(pe.at[n, 0], wbuf.at[par], mx.at[par], my.at[par], mc.at[par], n, PAIR)
            for x, v in fill_zone(
                PAIR, zm2.at[par], zx2.at[par], zy2.at[par], zc2.at[par]
            ).items():
                for n in range(2):
                    pe[n, 1, x] = pltpu.roll(v, Z - PAIR - 2 * PAIR * n, 1)
        else:
            pe[1, 0, DEEP : DEEP + X, 0:Y, :] = p2
        total = reduce_rest(bufs, par)

        m = mat[...]
        c1 = lane_sum(m * total)
        p11, p12, p22, uu = (c1[VROWS + n : VROWS + n + 1] for n in range(4))
        inv_uu = 1.0 / uu
        c1 = jnp.where(row1 == K + j, c1 * inv_uu, jnp.where(row1 < VROWS, c1, 0.0))
        t1 = lane_sum(jnp.where((lane2 == row2) & (row2 < VROWS), total, 0.0))
        t2 = lane_sum(jnp.where((lane2 == row2 + VROWS) & (row2 < K), total, 0.0))
        nv = jnp.where(lane_k == K + j, t1[:K], na[...])
        low = col_sum(nv * c1[:K])
        diff = pltpu.roll(total, Z - VROWS, 1) - low
        c2 = lane_sum(m * diff)
        c2 = jnp.where(row1 == K + j, c2 * inv_uu, jnp.where(row1 < VROWS, c2, 0.0))
        ww = p11 - col_sum(t1 * c1)
        q1 = c1[K + j : K + j + 1]
        a2e = col_sum(t2 * c1)
        q2 = (p12 - col_sum(t1 * c2) - a2e) / ww - q1
        s = q1 + q2
        cc = c2 - s * c1
        coefa[...] = jnp.broadcast_to(c1, (32, Z))
        coefb[...] = jnp.broadcast_to(jnp.where(row1 == VROWS, s, cc), (32, Z))
        pending = [(j, c1, c2, t1, q1, q2, uu, ww)]
        if last:
            a3 = lane_sum(jnp.where(lane2 == row2 + 2 * VROWS + 8, total, 0.0))[:K]
            e1 = c1[:K]
            e_lane = col_sum(jnp.where(lane_k == row_k, e1, 0.0))
            n2e = lane_sum(n2mat[...] * e_lane)
            d_col = lane_sum(jnp.where((lane2 == row2) & (row2 < VROWS), diff, 0.0))
            last_sq = (
                p22 - s * p12 + s * a2e - col_sum(e1 * (2.0 * a3 - n2e)) - col_sum(cc * d_col)
            )

        p_lo, p_n = (DEEP - 1, X + 2) if last else (DEEP - PAIR, X + 2 * PAIR)

        def combine(p, carry, j=j, p_lo=p_lo):
            z, x = lax.rem(p, 2), p_lo + lax.div(p, 2)
            t = jnp.zeros((YE, Z), f32)
            g = jnp.zeros((YE, Z), f32)
            for a in range(K):
                w = fields[a, z, x]
                t = t + coefa[a : a + 1, :] * w
                g = g + coefb[a : a + 1, :] * w
            temp[z, x] = t
            v1 = pe[0, z, x]
            g = pe[1, z, x] - coefb[VROWS : VROWS + 1, :] * v1 - g
            v1 = v1 - t
            for a in range(K, K + j + 1):
                w = fields[a, z, x]
                v1 = v1 - coefa[a : a + 1, :] * w
                g = g - coefb[a : a + 1, :] * w
            fields[C0 + j + 1, z, x] = v1
            fields[C0 + j + 2, z, x] = g
            return carry

        def images_only(p, carry):
            z, x = lax.rem(p, 2), lax.div(p, 2) * (XE - 1)
            t = jnp.zeros((YE, Z), f32)
            for a in range(K):
                t = t + coefa[a : a + 1, :] * fields[a, z, x]
            temp[z, x] = t
            return carry

        if not last:
            lax.fori_loop(0, 4, images_only, 0, unroll=2)
        lax.fori_loop(0, 2 * p_n, combine, 0, unroll=2)
        w2 = fields.at[C0 + j + 2]
        if last:
            def use(z, x, v, k):
                w2[0, x, 0:Y, :] = w2[0, x, 0:Y, :] - v

            apply(lambda z, x: temp[z, x], (0,), DEEP, DEEP + X, Y, use)
        else:
            def use(z, x, v, k):
                w2[z, x] = w2[z, x] - jnp.where(k > 0.0, v, 0.0)

            apply(lambda z, x: temp[z, x], (0, 1), DEEP - PAIR, DEEP + X + PAIR, YE, use)
            wait_send(cs)

    for p in pending:
        record(*p)

    hc = hcols[...]
    n2_col = nsq[C0 : C0 + STEPS, :]
    n_col = jnp.sqrt(n2_col)
    inv_col = 1.0 / n_col
    inv_row = col_sum(jnp.where(lane8 == row8, inv_col, 0.0))
    last_n = jnp.sqrt(last_sq)
    upper = hc[C0 : C0 + STEPS] * n_col * inv_row
    upper = jnp.where(lane8 < STEPS, upper, 0.0)
    upper = jnp.where(lane8 == row8, upper + SHIFT, upper)
    bottom = jnp.where(lane1 == STEPS - 1, last_n * inv_row, 0.0)
    hes = jnp.concatenate([upper, bottom], axis=0)
    lane_t, row_t = lane2[: STEPS + 1], row2[: STEPS + 1]
    for col in range(STEPS):
        picked = jnp.where(lane_t == row_t, hes[:, col : col + 1], 0.0)
        hes_out[col : col + 1, :] = jnp.sum(picked, axis=0, keepdims=True)[:, : STEPS + 1]

    h = {
        (r, c): jnp.broadcast_to(hes[r : r + 1, c : c + 1], (1, Z))
        for c in range(STEPS) for r in range(c + 2)
    }
    goal = [n_col[0:1]] + [jnp.zeros((1, Z), f32)] * STEPS
    for i in range(STEPS):
        top, low = h[i, i], h[i + 1, i]
        inv_r = 1.0 / jnp.sqrt(top * top + low * low)
        cs_, sn = top * inv_r, low * inv_r
        for c in range(i, STEPS):
            up, down = h[i, c], h[i + 1, c]
            h[i, c], h[i + 1, c] = cs_ * up + sn * down, cs_ * down - sn * up
        goal[i], goal[i + 1] = cs_ * goal[i] + sn * goal[i + 1], cs_ * goal[i + 1] - sn * goal[i]
    found = {}
    ysol = jnp.zeros((1, Z), f32)
    for i in range(STEPS - 1, -1, -1):
        rest = goal[i]
        for c in range(STEPS - 1, i, -1):
            rest = rest - h[i, c] * found[c]
        found[i] = rest * (1.0 / h[i, i])
        ysol = jnp.where(lane1 == i, found[i], ysol)

    rcoef = ecoef[:, :1] - jnp.sum(hc[:K] * (ysol * inv_row), axis=1, keepdims=True)
    ycol = jnp.sum(jnp.where(lane8 == row8, ysol * inv_row, 0.0), axis=1, keepdims=True)
    hy8 = jnp.sum(upper * ysol, axis=1, keepdims=True) * inv_col[:, :1]
    hy9 = jnp.sum(bottom * ysol, axis=1, keepdims=True) / last_n
    out = src[K]
    for a in range(K):
        out = out + rcoef[a : a + 1, :] * src[a]
    res = fields[C0, 0, DEEP : DEEP + X, 0:Y, :]
    for i in range(STEPS):
        ui = fields[C0 + i, 0, DEEP : DEEP + X, 0:Y, :]
        out = out + ycol[i : i + 1, :] * ui
        res = res - hy8[i : i + 1, :] * ui
    res = res - hy9 * fields[C0 + STEPS, 0, DEEP : DEEP + X, 0:Y, :]
    sol_out[...] = out
    res_out[...] = res


def deliver(sol, res, hes, sol_out, res_out, hes_out):
    sol_out[...] = sol[...]
    res_out[...] = res[...]
    hes_out[...] = hes[...]


def round_up(n, m):
    return (n + m - 1) // m * m


def solution(mesh):
    sizes = tuple(mesh.shape[a] for a in AXES)

    def body(right_side, start_guess, conductivity, recycled):
        K, X, Y, Z = recycled.shape
        NF = K + 2
        FR, ER = round_up(NF * X, 8), round_up(NF, 8)
        assert X >= DEEP and Y % 8 == 0 and K + STEPS <= VROWS

        def count(group):
            n = 1
            for a in group:
                n *= mesh.shape[a]
            return n

        groups = ONE if count(AXES) <= 64 else TWO
        n_step = [count(g) for g in groups]
        nflat, ntall = sem_counts(sizes)
        chunks = (NF + CHUNK - 1) // CHUNK
        nsem = ntall + (chunks + 2) * nflat
        nrecv = 2 * ntall + (2 * chunks + 2) * nflat
        XE, YE = X + 2 * DEEP, Y + 8
        V = lambda *s: pltpu.VMEM(s, jnp.float32)
        vm = pl.BlockSpec(memory_space=pltpu.VMEM)
        shape = jax.ShapeDtypeStruct((X, Y, Z), jnp.float32)

        def halo(s):
            cells = 2 * s - 1
            return [
                V(2, FR, Z), V(2, 2, ER * cells, Z),
                V(2, NF, 1, Y, Z), V(2, FR, Z), V(2, 2, ER * cells, Z),
            ]

        def lanes(d):
            rows, cells = round_up(X * d, 8), d * d
            return [
                V(1, X, Y, Z), V(2, rows, Z), V(2, 2, cells, Z),
                V(2, 1, X, Y, Z), V(2, 2, 1, d, Y, Z), V(2, 2, rows, Z), V(2, 2, 2, cells, Z),
            ]

        prow, pcell = round_up(2 * X * PAIR, 8), 2 * PAIR * PAIR
        lrow, lcell = round_up(X * PAIR, 8), PAIR * PAIR
        sol, res, hes = pl.pallas_call(
            functools.partial(kernel, sizes, groups),
            out_shape=(shape, shape, jax.ShapeDtypeStruct((STEPS, STEPS + 1), jnp.float32)),
            in_specs=[pl.BlockSpec(memory_space=pltpu.HBM)] * 4,
            out_specs=(vm, vm, vm),
            scratch_shapes=[
                V(X, Y, Z), V(X, Y, Z), V(NF, X, Y, Z), V(NF, X, Y, Z), V(K, X, Y, Z),
                *halo(1), *halo(1), *halo(2), *halo(3), *lanes(1), *lanes(DEEP),
                V(2, 2, X, Y, Z), V(2, 2, prow, Z), V(2, 2, 2, pcell, Z),
                V(2, 1, X, Y, Z), V(2, 2, lrow, Z), V(2, 2, 2, lcell, Z),
                V(2, 2, 2, PAIR, Y, Z), V(2, 2, prow, Z), V(2, 2, 2, pcell, Z),
                V(2, 2, 1, X, Y, Z), V(2, 2, 2, 1, PAIR, Y, Z),
                V(2, 2, 2, lrow, Z), V(2, 2, 2, 2, lcell, Z),
                V(K + STEPS + 1, 2, XE, YE, Z), V(2, XE, YE, Z), V(2, XE, YE, Z),
                V(2, XE, YE, Z), V(2, XE, YE, Z), V(XE, YE, Z), V(2, 2, XE, YE, Z),
                V(n_step[0], GF, Z), V(n_step[-1], GF, Z), V(n_step[0], 2, Z), V(n_step[-1], 2, Z),
                V(2, n_step[0], 1, Z), V(2, n_step[-1], 1, Z),
                V(32, Z), V(K, Z), V(K, Z), V(K, Z), V(32, Z), V(32, Z), V(32, Z), V(32, Z), V(K, Z),
                pltpu.SemaphoreType.DMA((nsem,)), pltpu.SemaphoreType.DMA((nrecv,)),
                pltpu.SemaphoreType.DMA((4, len(groups))), pltpu.SemaphoreType.DMA((4, len(groups))),
                pltpu.SemaphoreType.DMA((4,)),
            ],
            compiler_params=pltpu.CompilerParams(collective_id=0, has_side_effects=True, vmem_limit_bytes=VMEM - KEPT),
        )(right_side, start_guess, conductivity, recycled)
        sol, res, hes = pl.pallas_call(
            deliver,
            out_shape=(shape, shape, jax.ShapeDtypeStruct(hes.shape, hes.dtype)),
            in_specs=[vm] * 3,
            out_specs=(vm,) * 3,
            compiler_params=pltpu.CompilerParams(vmem_limit_bytes=8 * 2**20),
        )(sol, res, hes)
        return sol, res, hes.T

    return jax.shard_map(
        body,
        mesh=mesh,
        in_specs=(P(*AXES), P(*AXES), P(*AXES), P(None, *AXES)),
        out_specs=(P(*AXES), P(*AXES), P()),
        check_vma=False,
    )
```

```python
import functools
import itertools

import jax
import jax.numpy as jnp
from jax import lax
from jax.experimental import pallas as pl
from jax.experimental.pallas import tpu as pltpu
from jax.sharding import PartitionSpec as P

STEPS = 8
MESH = pl.DeviceIdType.MESH
AXES = ("px", "py", "pz")
TWO = (("py", "pz"), ("px",))
ONE = (("px", "py", "pz"),)
CHUNK = 8
GF = 4
DEEP = 3
PAIR = 2
VROWS = 24
VMEM = 67043328
KEPT = 10310 * 1024

shift_value = 0.4
SHIFT = 2.8

DIRS = [d for d in itertools.product((-1, 0, 1), repeat=3) if d != (0, 0, 0)]


def sem_counts(sizes):
    dirs = [d for d in DIRS if all(s == 0 or n > 1 for n, s in zip(sizes, d))]
    flat = sum(d[2] == 0 for d in dirs)
    tall = len(dirs) - flat
    return flat, tall // 2 if sizes[2] == 2 else tall


def shell_cells(s):
    return [(i, j) for i in range(1, s + 1) for j in range(1, s + 1) if max(i, j) == s]


def square_cells(d):
    return [(i, j) for i in range(1, d + 1) for j in range(1, d + 1)]


def kernel(
    sizes, groups,
    rhs_hbm, guess_hbm, cond_hbm, rec_hbm,
    sol_out, res_out, hes_out,
    rhs, cond, src, img, awf,
    aface, aedge, ax, ay, ac,
    bface1, bedge1, bx1, by1, bc1,
    bface2, bedge2, bx2, by2, bc2,
    bface3, bedge3, bx3, by3, bc3,
    pack0, pface0, pedge0, zm0, zx0, zy0, zc0,
    pack1, pface1, pedge1, zm1, zx1, zy1, zc1,
    wbuf, wface, wedge, wpack, wpface, wpedge, mx, my, mc, zm2, zx2, zy2, zc2,
    fields, kext, dext, temp, zext, zw, pe,
    gred1, gred2, nred1, nred2, sred1, sred2,
    mat, na, gmat, n2mat, hcols, nsq, coefa, coefb, ecoef,
    hsend, hrecv, rsend, rrecv, isem,
):
    nsz = dict(zip(AXES, sizes))
    me = {a: lax.axis_index(a) for a in AXES}
    K, X, Y, Z = rec_hbm.shape
    NF = K + 2
    C0 = K
    XE, YE = X + 2 * DEEP, Y + 8
    NC = (NF + CHUNK - 1) // CHUNK
    f32 = jnp.float32
    lane_p = lax.broadcasted_iota(jnp.int32, (YE, Z), 1)
    lane2 = lax.broadcasted_iota(jnp.int32, (32, Z), 1)
    row2 = lax.broadcasted_iota(jnp.int32, (32, Z), 0)
    row1 = row2[:, :1]
    lane1 = lane2[:1]

    pair = nsz["pz"] == 2

    def exists(d):
        ok = None
        for a, s in zip(AXES, d):
            if s == 0 or (pair and a == "pz"):
                continue
            here = (me[a] < nsz[a] - 1) if s > 0 else (me[a] > 0)
            ok = here if ok is None else jnp.logical_and(ok, here)
        return True if ok is None else ok

    def when(ok, f):
        if ok is True:
            f()
        else:
            pl.when(ok)(f)

    def possible(d):
        return all(s == 0 or nsz[a] > 1 for a, s in zip(AXES, d)) and not (pair and d[2] < 0)

    flat = [d for d in DIRS if possible(d) and d[2] == 0]
    tall = [d for d in DIRS if possible(d) and d[2] != 0]
    dirs = flat + tall
    NFLAT, NTALL = len(flat), len(tall)

    def sem_index(chunk, d):
        if d[2] == 0:
            return NTALL + chunk * NFLAT + flat.index(d)
        return tall.index(d)

    def target(d):
        x, y, z = (me[a] + s for a, s in zip(AXES, d))
        return x, y, 1 - me["pz"] if pair and d[2] else z

    def group_info(group):
        n = 1
        rank = 0
        for a in group:
            n *= nsz[a]
            rank = rank * nsz[a] + me[a]
        return n, rank

    def copies(sends, recvs, batch, chunk, zones):
        out = []
        for dx, dy, dz in dirs:
            if (dz != 0) not in zones:
                continue
            main, xsl, face, edge = sends(dz)
            side = None if dz == 0 else me["pz"] if pair else int(dz < 0)
            rm, rx, ry, rc = recvs(side)
            hx, hy = int(dx > 0), int(dy > 0)
            if dx == 0 and dy == 0:
                s, t = main, rm
            elif dy == 0:
                s, t = main.at[:, xsl[hx]], rx.at[1 - hx]
            elif dx == 0:
                s, t = face.at[hy], ry.at[1 - hy]
            else:
                s, t = edge.at[hx, hy], rc.at[1 - hx, 1 - hy]
            d = (dx, dy, dz)
            out.append((d, pltpu.make_async_remote_copy(
                src_ref=s, dst_ref=t,
                send_sem=hsend.at[sem_index(chunk, d)], recv_sem=hrecv.at[batch * (NTALL + NC * NFLAT) + sem_index(chunk, d)],
                device_id=target(d), device_id_type=MESH,
            )))
        return out

    def start_halo(cs):
        for d, c in cs:
            when(exists(d), c.start)

    def wait_recv(cs):
        for d, c in cs:
            when(exists(tuple(-s for s in d)), c.wait_recv)

    def wait_send(cs):
        for d, c in cs:
            when(exists(d), c.wait_send)

    def ends(d):
        return pl.ds(0, d), pl.ds(X - d, d)

    def batch_copies(b, c):
        f0, f1 = c * CHUNK, min((c + 1) * CHUNK, NF)
        fs, es = pl.ds(f0, f1 - f0), pl.ds(f0, CHUNK)
        depth = DEEP if b else 1
        wholes = (img, bface1, bedge1, bx1, by1, bc1) if b else (src, aface, aedge, ax, ay, ac)
        lanes = (
            (pack1, pface1, pedge1, zm1, zx1, zy1, zc1) if b
            else (pack0, pface0, pedge0, zm0, zx0, zy0, zc0)
        )
        rows = pl.ds(f0 * X, min(CHUNK * X, aface.shape[1] - f0 * X))

        def sends(dz):
            if dz == 0:
                main, face, edge = wholes[:3]
                return main.at[fs], ends(1), face.at[:, rows], edge.at[:, :, es]
            return lanes[0], ends(depth), lanes[1], lanes[2]

        def recvs(h):
            if h is None:
                rx, ry, rc = wholes[3:]
                return None, rx.at[:, fs], ry.at[:, rows], rc.at[:, :, es]
            return tuple(r.at[h] for r in lanes[3:])

        return copies(sends, recvs, b, c % NC, (c == NC,))

    def shell_copies(s):
        face, edge, rx, ry, rc = (
            (bface2, bedge2, bx2, by2, bc2) if s == 2 else (bface3, bedge3, bx3, by3, bc3)
        )
        planes = pl.ds(s - 1, 1), pl.ds(X - s, 1)
        return copies(
            lambda dz: (img, planes, face, edge), lambda h: (None, rx, ry, rc),
            1, NC + s - 2, (False,),
        )

    def pair_copies(par):
        def sends(dz):
            if dz == 0:
                return wbuf.at[par], ends(PAIR), wface.at[par], wedge.at[par]
            return wpack.at[par], ends(PAIR), wpface.at[par], wpedge.at[par]

        def recvs(h):
            if h is None:
                return None, mx.at[par], my.at[par], mc.at[par]
            return zm2.at[par, h], zx2.at[par, h], zy2.at[par, h], zc2.at[par, h]

        return copies(sends, recvs, par, 0, (False, True))

    def pack_edges(row_of, face, edge, frow, erow, depths, cells):
        for n, i in enumerate(depths):
            for x in range(X):
                at = pl.ds(frow + n * X + x, 1)
                face[0, at, :] = row_of(x, i - 1)
                face[1, at, :] = row_of(x, Y - i)
        for n, (i, j) in enumerate(cells):
            for hx, hy in itertools.product((0, 1), repeat=2):
                edge[hx, hy, pl.ds(erow + n, 1), :] = row_of(
                    X - i if hx else i - 1, Y - j if hy else j - 1
                )

    def value_rows(val):
        return lambda x, y: val[x, y : y + 1, :]

    def ref_rows(ref, f):
        return lambda x, y: ref[f, x, y : y + 1, :]

    def place_edges(dst, ry, rc, frow, erow, depths, cells):
        for n, i in enumerate(depths):
            for x in range(X):
                at = pl.ds(frow + n * X + x, 1)
                dst[DEEP + x, Y + i - 1 : Y + i, :] = ry[1, at, :]
                dst[DEEP + x, YE - i : YE - i + 1, :] = ry[0, at, :]
        for n, (i, j) in enumerate(cells):
            for hx, hy in itertools.product((0, 1), repeat=2):
                x = DEEP + X + i - 1 if hx else DEEP - i
                y = Y + j - 1 if hy else YE - j
                dst[x, y : y + 1, :] = rc[hx, hy, pl.ds(erow + n, 1), :]

    def place_shell(dst, rx, ry, rc, f, s):
        cells = shell_cells(s)
        dst[DEEP - s, 0:Y, :] = rx[0, f, 0]
        dst[DEEP + X + s - 1, 0:Y, :] = rx[1, f, 0]
        place_edges(dst, ry, rc, f * X, f * len(cells), (s,), cells)

    def place_all(dst, main, rx, ry, rc, f, depth):
        cells = square_cells(depth)
        dst[DEEP : DEEP + X, 0:Y, :] = main[f]
        dst[DEEP - depth : DEEP, 0:Y, :] = rx[0, f]
        dst[DEEP + X : DEEP + X + depth, 0:Y, :] = rx[1, f]
        place_edges(
            dst, ry, rc, f * X * depth, f * len(cells), tuple(range(1, depth + 1)), cells
        )

    def slots(depth):
        return 2 * depth, lax.rem(lane_p, 2 * depth) < depth

    def zone_plane(f, x, depth):
        return pltpu.roll(zw[x], Z - depth - 2 * depth * f, 1)

    def fill_zone(depth, zm, zx, zy, zc):
        for h in range(2):
            place_all(zext.at[h], zm.at[h], zx.at[h], zy.at[h], zc.at[h], 0, depth)
        low = slots(depth)[1]
        return {
            x: jnp.where(low, zext[0, x], zext[1, x])
            for x in range(DEEP - depth, DEEP + X + depth)
        }

    def keep_zone(planes):
        for x, v in planes.items():
            zw[x] = v

    def pack_lanes(get, count, depth, pack, pface, pedge):
        lane = lax.broadcasted_iota(jnp.int32, (X, Y, Z), 2)
        width = 2 * depth
        v = jnp.zeros((X, Y, Z), f32)
        for f in range(count):
            here = jnp.logical_and(lane >= width * f, lane < width * (f + 1))
            v = jnp.where(here, pltpu.roll(get(f), width * f + depth, 2), v)
        pack[0] = v
        pack_edges(
            value_rows(v), pface, pedge, 0, 0,
            tuple(range(1, depth + 1)), square_cells(depth),
        )

    def sum_zy(e, b):
        left = pltpu.roll(jnp.where(lane_p == Z - 1, b, e), 1, 1)
        right = pltpu.roll(jnp.where(lane_p == 0, b, e), Z - 1, 1)
        t = (left + right) + (e + e)
        return (pltpu.roll(t, 1, 0) + pltpu.roll(t, YE - 1, 0)) + (t + t)

    def apply(get, zones, lo, hi, rows, use):
        planes = {}
        for x in range(lo - 1, hi + 1):
            now = []
            for z in range(2):
                e = get(z, x)
                now += [e, kext[z, x] * e]
            planes[x] = now
            if x > lo:
                sums = [
                    (a + c) + (b + b) for a, b, c in zip(planes[x - 2], planes[x - 1], now)
                ]
                for z in zones:
                    o = 1 - z
                    k0 = kext[z, x - 1, :rows]
                    near = sum_zy(sums[2 * z], sums[2 * o])[:rows]
                    far = sum_zy(sums[2 * z + 1], sums[2 * o + 1])[:rows]
                    e0 = planes[x - 1][2 * z][:rows]
                    use(z, x - 1, dext[z, x - 1, :rows] * e0 - k0 * near - far, k0)

    def make_diag(shift):
        for z in range(2):
            sums = [sum_zy(kext[z, x], kext[1 - z, x]) for x in range(XE)]
            for x in range(1, XE - 1):
                total = (sums[x - 1] + sums[x + 1]) + (sums[x] + sums[x])
                dext[z, x] = (shift_value - shift) + 64.0 * kext[z, x] + total

    lane8 = lane2[:8]
    row8 = row2[:8]

    def fold(v):
        return jnp.sum(v.reshape(X * Y // 8, 8, Z), axis=0)

    def row_sums(parts):
        parts = parts + [None] * (-len(parts) % 8)
        for d in (1, 2, 4):
            here = lax.rem(lax.div(row8, d), 2) == 0
            merged = []
            for a, b in zip(parts[::2], parts[1::2]):
                if a is None:
                    merged.append(None)
                    continue
                b = 0.0 if b is None else b
                merged.append(jnp.where(here, a, b) + pltpu.roll(jnp.where(here, b, a), d, 0))
            parts = merged
        return jnp.concatenate(
            [jnp.zeros((8, Z), f32) if p is None else p for p in parts], axis=0
        )

    def lane_sum(v):
        return jnp.sum(v, axis=1, keepdims=True)

    def col_sum(v):
        return jnp.sum(v, axis=0, keepdims=True)

    def symmetric(n, rows, dots):
        lane = lax.broadcasted_iota(jnp.int32, (rows, Z), 1)
        row = lax.broadcasted_iota(jnp.int32, (rows, Z), 0)
        out = jnp.zeros((rows, Z), f32)
        for a in range(n):
            col = lane_sum(row_sums(dots(a)))
            if col.shape[0] < rows:
                col = jnp.concatenate([col, jnp.zeros((rows - col.shape[0], 1), f32)], axis=0)
            across = col_sum(jnp.where((lane == row) & (row < a), col, 0.0))
            out = jnp.where(lane == a, col, jnp.where(row == a, across, out))
        return out

    spots = {}
    for axis in AXES:
        for o in range(nsz[axis]):
            at = me[axis] + o
            spots[axis, o] = jnp.where(at >= nsz[axis], at - nsz[axis], at) if o else at

    def peers(group):
        ways = list(itertools.product(*(range(nsz[a]) for a in group)))[1:]
        far = lambda w: -sum(min(o, nsz[a] - o) for a, o in zip(group, w))
        return [
            tuple(spots[a, w[group.index(a)]] if a in group else me[a] for a in AXES)
            for w in sorted(ways, key=far)
        ]

    def reduce_start(value, bufs, slot, g):
        group = groups[g]
        rank = group_info(group)[1]
        buf = bufs[g]
        buf[rank] = value
        for peer in peers(group):
            pltpu.make_async_remote_copy(
                src_ref=buf.at[rank], dst_ref=buf.at[rank],
                send_sem=rsend.at[slot, g], recv_sem=rrecv.at[slot, g],
                device_id=peer, device_id_type=MESH,
            ).start()

    def reduce_end(bufs, slot, g):
        group = groups[g]
        n, rank = group_info(group)
        buf = bufs[g]
        others = pltpu.make_async_remote_copy(
            src_ref=buf.at[pl.ds(0, n - 1)], dst_ref=buf.at[pl.ds(0, n - 1)],
            send_sem=rsend.at[slot, g], recv_sem=rrecv.at[slot, g],
            device_id=peers(group)[0], device_id_type=MESH,
        )
        others.wait_recv()
        parts = [buf[r] for r in range(n)]
        while len(parts) > 1:
            parts = [sum(parts[r : r + 2][1:], parts[r]) for r in range(0, len(parts), 2)]
        others.wait_send()
        return parts[0]

    def reduce_rest(bufs, slot):
        total = reduce_end(bufs, slot, 0)
        for g in range(1, len(groups)):
            reduce_start(total, bufs, slot, g)
            total = reduce_end(bufs, slot, g)
        return total

    def clear_all(refs):
        for ref in refs:
            def clear(i, carry, ref=ref):
                ref[i] = jnp.zeros(ref.shape[1:], f32)
                return carry

            lax.fori_loop(0, ref.shape[0], clear, 0)

    loads = [
        pltpu.make_async_copy(a, b, isem.at[n])
        for n, (a, b) in enumerate(
            ((cond_hbm, cond), (guess_hbm, src.at[K]), (rec_hbm, src.at[pl.ds(0, K)]), (rhs_hbm, rhs))
        )
    ]
    for c in loads:
        c.start()
    clear_all((ax, ay, ac, bx1, by1, bc1, bx2, by2, bc2, bx3, by3, bc3))
    clear_all((zm0, zx0, zy0, zc0, zm1, zx1, zy1, zc1, mx, my, mc, zm2, zx2, zy2, zc2))
    barrier = pltpu.get_barrier_semaphore()
    count = jnp.int32(0)
    for group in ONE:
        everyone = peers(group)
        for peer in everyone:
            pl.semaphore_signal(barrier, inc=1, device_id=peer, device_id_type=MESH)
        count = count + len(everyone)

    clear_all((wface, wedge, wpface, wpedge, aface, aedge, bface1, bedge1, bface2, bedge2, bface3, bedge3))
    clear_all((pface0, pedge0, pface1, pedge1))

    near_cells = shell_cells(1)

    for c in loads:
        c.wait()
    src[K + 1] = 0.125 * cond[...]

    def load_field(f, carry):
        pack_edges(ref_rows(src, f), aface, aedge, f * X, f, (1,), near_cells)
        return carry

    lax.fori_loop(0, NF, load_field, 0, unroll=2)
    pack_lanes(lambda f: src[f], NF, 1, pack0, pface0, pedge0)
    pl.semaphore_wait(barrier, count)

    first = [batch_copies(0, c) for c in range(NC + 1)]
    second = [batch_copies(1, c) for c in range(NC + 1)]
    order = [NC - 1] + list(range(NC - 1))
    for c in [NC] + order:
        start_halo(first[c])
    clear_all((fields, kext, dext, zext, zw, pe))
    temp[...] = jnp.zeros(temp.shape, f32)
    img[NF - 1] = src[NF - 1]
    pack_edges(
        ref_rows(src, NF - 1), bface1, bedge1, (NF - 1) * X, NF - 1, (1,), near_cells
    )
    wait_recv(first[NC])
    keep_zone(fill_zone(1, zm0, zx0, zy0, zc0))

    def image(f, carry):
        dst = temp.at[0]
        dst[DEEP : DEEP + X, 0:Y, :] = src[f]
        place_shell(dst, ax, ay, ac, f, 1)
        for x in range(DEEP - 1, DEEP + X + 1):
            temp[1, x] = zone_plane(f, x, 1)

        def use(z, x, v, k):
            img[f, x - DEEP] = v

        apply(lambda z, x: temp[z, x], (0,), DEEP, DEEP + X, Y, use)
        pack_edges(ref_rows(img, f), bface1, bedge1, f * X, f, (1,), near_cells)
        return carry

    for c in order:
        wait_recv(first[c])
        if c == NC - 1:
            kext[0, DEEP : DEEP + X, 0:Y, :] = src[K + 1]
            place_shell(kext.at[0], ax, ay, ac, K + 1, 1)
            for x in range(DEEP - 1, DEEP + X + 1):
                v = zone_plane(K + 1, x, 1)
                kext[1, x] = jnp.where((lane_p < 1) | (lane_p >= Z - 1), v, 0.0)
            make_diag(0.0)
            lax.fori_loop(c * CHUNK, K + 1, image, 0)
            img[K] = rhs[...] - img[K]
            pack_edges(ref_rows(img, K), bface1, bedge1, K * X, K, (1,), near_cells)
        else:
            lax.fori_loop(c * CHUNK, (c + 1) * CHUNK, image, 0, unroll=2)
        wait_send(first[c])
        start_halo(second[c])
    pack_lanes(lambda f: img[f], NF, DEEP, pack1, pface1, pedge1)
    wait_send(first[NC])
    start_halo(second[NC])

    GR = (K + 8) // 8 * 8
    GW = Z // (GR // GF)
    assert K + 1 <= GW and 2 * DEEP * NF <= Z

    def gram_dots(a):
        va = img[a]
        return [fold(img[b] * va) for b in range(a + 1)]

    gram = symmetric(K + 1, GR, gram_dots)
    part = gram[:GF]
    for q in range(1, GR // GF):
        part = part + pltpu.roll(gram[GF * q : GF * q + GF], q * GW, 1)
    reduce_start(part, (gred1, gred2), 2, 0)

    shells = {2: shell_copies(2), 3: shell_copies(3)}
    for s, face, edge in ((2, bface2, bedge2), (3, bface3, bedge3)):
        cells = shell_cells(s)

        def pack_shell(f, carry, s=s, face=face, edge=edge, cells=cells):
            pack_edges(ref_rows(img, f), face, edge, f * X, f * len(cells), (s,), cells)
            return carry

        start_halo([c for c in shells[s] if c[0][1] == 0])
        lax.fori_loop(0, NF, pack_shell, 0, unroll=2)
        start_halo([c for c in shells[s] if c[0][1] != 0])

    for c in second:
        wait_recv(c)
    keep_zone(fill_zone(DEEP, zm1, zx1, zy1, zc1))

    def inner(f, carry):
        fields[f, 0, DEEP : DEEP + X, 0:Y, :] = img[f]
        place_shell(fields.at[f, 0], bx1, by1, bc1, f, 1)
        for x in range(XE):
            fields[f, 1, x] = zone_plane(f, x, DEEP)
        return carry

    lax.fori_loop(0, K + 1, inner, 0, unroll=4)
    for x in range(XE):
        v = zone_plane(K + 1, x, DEEP)
        kext[1, x] = jnp.where((lane_p < DEEP) | (lane_p >= Z - DEEP), v, 0.0)
    make_diag(SHIFT)

    def second_image(f, carry):
        def use(z, x, v, k):
            awf[f, x - DEEP] = v

        apply(lambda z, x: fields[f, z, x], (0,), DEEP, DEEP + X, Y, use)
        return carry

    lax.fori_loop(0, K, second_image, 0, unroll=2)

    def cross_dots(a):
        va = awf[a]
        return [fold(img[b] * va) for b in range(a + 1)]

    def square_dots(a):
        va = awf[a]
        return [fold(awf[b] * va) for b in range(a + 1)]

    NG = 2
    NW = Z // (K // NG)
    assert K <= NW

    def squeeze(m):
        part = m[:NG]
        for q in range(1, K // NG):
            part = part + pltpu.roll(m[NG * q : NG * q + NG], q * NW, 1)
        return part

    def unsqueeze(part):
        both = [part] + [pltpu.roll(part, Z - q * NW, 1) for q in range(1, K // NG)]
        lane = lax.broadcasted_iota(jnp.int32, (K, Z), 1)
        return jnp.where(lane < K, jnp.concatenate(both, axis=0), 0.0)

    reduce_start(squeeze(symmetric(K, K, cross_dots)), (nred1, nred2), 3, 0)

    def outer(s, rx, ry, rc):
        wait_recv(shells[s])

        def place(f, carry):
            place_shell(fields.at[f, 0], rx, ry, rc, f, s)
            return carry

        lax.fori_loop(0, K + 1, place, 0, unroll=2)
        place_shell(kext.at[0], rx, ry, rc, K + 1, s)
        make_diag(SHIFT)

    outer(2, bx2, by2, bc2)

    part = reduce_rest((gred1, gred2), 2)
    gram = [part] + [pltpu.roll(part, Z - q * GW, 1) for q in range(1, GR // GF)]
    gram = jnp.concatenate(gram, axis=0)

    lane_k = lax.broadcasted_iota(jnp.int32, (K, Z), 1)
    row_k = lax.broadcasted_iota(jnp.int32, (K, Z), 0)
    a_mat = jnp.where(lane_k < K, gram[:K], 0.0)
    gmat[...] = a_mat
    for k in range(K):
        prow = a_mat[k : k + 1, :]
        pcol = a_mat[:, k : k + 1]
        inv_p = 1.0 / a_mat[k : k + 1, k : k + 1]
        prow_s = jnp.where(lane1 == k, 1.0, prow) * inv_p
        base = jnp.where(lane_k == k, 0.0, a_mat)
        a_mat = jnp.where(row_k == k, jnp.broadcast_to(prow_s, (K, Z)), base - pcol * prow_s)
    mat[...] = jnp.where(
        row2 < VROWS, jnp.where(lane2 == row2, 1.0, 0.0),
        jnp.where(lane2 == row2 + VROWS, 1.0, 0.0),
    )
    mat[0:K, :] = a_mat
    grow = jnp.where(lane1 < K, gram[K : K + 1, :], 0.0)
    ecoef[...] = jnp.broadcast_to(jnp.sum(a_mat * grow, axis=1, keepdims=True), (K, Z))

    def begin(p, carry):
        z, x = lax.rem(p, 2), DEEP - PAIR + lax.div(p, 2)
        v = fields[C0, z, x]
        for a in range(K):
            v = v - ecoef[a : a + 1, :] * fields[a, z, x]
        fields[C0, z, x] = v
        return carry

    lax.fori_loop(0, 2 * (X + 2 * PAIR), begin, 0, unroll=4)
    for c in second:
        wait_send(c)
    hcols[...] = jnp.zeros((32, Z), f32)
    nsq[...] = jnp.ones((32, Z), f32)

    def record(j, c1, c2, t1, q1, q2, uu, ww):
        old = hcols[...]
        q_lane = col_sum(jnp.where((lane2 == row2 - K) & (lane2 < j), c1, 0.0))
        c3 = c2 - q1 * c1 - lane_sum(old * q_lane)
        c3 = jnp.where(row1 < VROWS, c3, 0.0)
        e_lane = col_sum(jnp.where((lane2 == row2) & (row2 < K), c3, 0.0))
        ge = lane_sum(gmat[...] * e_lane)
        now = jnp.where(row1 == K + j + 1, 1.0, c1)
        then = jnp.where(row1 == K + j + 1, q2, jnp.where(row1 == K + j + 2, 1.0, c3))
        hcols[...] = jnp.where(lane2 == j, now, jnp.where(lane2 == j + 1, then, old))
        nv = na[...]
        nv = jnp.where(lane_k == K + j, t1[:K], jnp.where(lane_k == K + j + 1, ge, nv))
        na[...] = nv
        new = jnp.where(row2 == K + j, uu, jnp.where(row2 == K + j + 1, ww, nsq[...]))
        nsq[...] = new
        fresh = jnp.logical_and(lane2 == row2, (row2 == K + j) | (row2 == K + j + 1))
        mat[...] = jnp.where(fresh, 1.0 / new, mat[...])

    pending = []
    last_sq = None
    for j in range(0, STEPS, 2):
        last = j == STEPS - 2
        par = (j // 2) % 2
        u = fields.at[C0 + j]
        p1r, p2r = pe.at[0], pe.at[1]

        def use(z, x, v, k):
            p1r[z, x] = jnp.where(k > 0.0, v, 0.0)

        apply(lambda z, x: u[z, x], (0, 1), DEEP - 1, DEEP + X + 1, YE, use)

        def use(z, x, v, k):
            wbuf[par, 1, x - DEEP] = v

        apply(lambda z, x: p1r[z, x], (0,), DEEP, DEEP + X, Y, use)
        p1 = p1r[0, DEEP : DEEP + X, 0:Y, :]
        p2 = wbuf[par, 1]
        wbuf[par, 0] = p1
        rows1, rows2 = [], []
        for f in range(K + j + 1):
            v = fields[f, 0, DEEP : DEEP + X, 0:Y, :]
            rows1.append(fold(v * p1))
            rows2.append(fold(v * p2))
        gap = [None] * (VROWS - K - j - 1)
        uin = u[0, DEEP : DEEP + X, 0:Y, :]
        rows = rows1 + gap + rows2 + gap
        rows += [fold(p1 * p1), fold(p1 * p2), fold(p2 * p2), fold(uin * uin)] + [None] * 4
        if last:
            rows += [fold(awf[a] * p2) for a in range(K)]
        R = 2 * VROWS + 8 + (K if last else 0)
        lane_r = lax.broadcasted_iota(jnp.int32, (R, Z), 1)
        row_r = lax.broadcasted_iota(jnp.int32, (R, Z), 0)
        sums = lane_sum(row_sums(rows))
        part = col_sum(jnp.where(lane_r == row_r, sums, 0.0))
        bufs = (sred1.at[par], sred2.at[par])
        reduce_start(part, bufs, par, 0)
        if not last:
            for n, v in ((0, p1), (1, p2)):
                cells = square_cells(PAIR)
                pack_edges(
                    value_rows(v), wface.at[par], wedge.at[par], n * X * PAIR,
                    n * len(cells), tuple(range(1, PAIR + 1)), cells,
                )
            pack_lanes(
                lambda n: p2 if n else p1, 2, PAIR,
                wpack.at[par], wpface.at[par], wpedge.at[par],
            )
            cs = pair_copies(par)
            if j == 0:
                for s in shells:
                    wait_send(shells[s])
            start_halo(cs)
        if j == 0:
            outer(3, bx3, by3, bc3)
            na[...] = unsqueeze(reduce_rest((nred1, nred2), 3))
            n2mat[...] = symmetric(K, K, square_dots)
        if j == STEPS - 4:
            reduce_start(squeeze(n2mat[...]), (nred1, nred2), 3, 0)
        if last:
            n2mat[...] = unsqueeze(reduce_rest((nred1, nred2), 3))
        for p in pending:
            record(*p)
        if not last:
            wait_recv(cs)
            for n in range(2):
                place_all(pe.at[n, 0], wbuf.at[par], mx.at[par], my.at[par], mc.at[par], n, PAIR)
            for x, v in fill_zone(
                PAIR, zm2.at[par], zx2.at[par], zy2.at[par], zc2.at[par]
            ).items():
                for n in range(2):
                    pe[n, 1, x] = pltpu.roll(v, Z - PAIR - 2 * PAIR * n, 1)
        else:
            pe[1, 0, DEEP : DEEP + X, 0:Y, :] = p2
        total = reduce_rest(bufs, par)

        m = mat[...]
        c1 = lane_sum(m * total)
        p11, p12, p22, uu = (c1[VROWS + n : VROWS + n + 1] for n in range(4))
        inv_uu = 1.0 / uu
        c1 = jnp.where(row1 == K + j, c1 * inv_uu, jnp.where(row1 < VROWS, c1, 0.0))
        t1 = lane_sum(jnp.where((lane2 == row2) & (row2 < VROWS), total, 0.0))
        t2 = lane_sum(jnp.where((lane2 == row2 + VROWS) & (row2 < K), total, 0.0))
        nv = jnp.where(lane_k == K + j, t1[:K], na[...])
        low = col_sum(nv * c1[:K])
        diff = pltpu.roll(total, Z - VROWS, 1) - low
        c2 = lane_sum(m * diff)
        c2 = jnp.where(row1 == K + j, c2 * inv_uu, jnp.where(row1 < VROWS, c2, 0.0))
        ww = p11 - col_sum(t1 * c1)
        q1 = c1[K + j : K + j + 1]
        a2e = col_sum(t2 * c1)
        q2 = (p12 - col_sum(t1 * c2) - a2e) / ww - q1
        s = q1 + q2
        cc = c2 - s * c1
        coefa[...] = jnp.broadcast_to(c1, (32, Z))
        coefb[...] = jnp.broadcast_to(jnp.where(row1 == VROWS, s, cc), (32, Z))
        pending = [(j, c1, c2, t1, q1, q2, uu, ww)]
        if last:
            a3 = lane_sum(jnp.where(lane2 == row2 + 2 * VROWS + 8, total, 0.0))[:K]
            e1 = c1[:K]
            e_lane = col_sum(jnp.where(lane_k == row_k, e1, 0.0))
            n2e = lane_sum(n2mat[...] * e_lane)
            d_col = lane_sum(jnp.where((lane2 == row2) & (row2 < VROWS), diff, 0.0))
            last_sq = (
                p22 - s * p12 + s * a2e - col_sum(e1 * (2.0 * a3 - n2e)) - col_sum(cc * d_col)
            )

        p_lo, p_n = (DEEP - 1, X + 2) if last else (DEEP - PAIR, X + 2 * PAIR)

        def combine(p, carry, j=j, p_lo=p_lo):
            z, x = lax.rem(p, 2), p_lo + lax.div(p, 2)
            t = jnp.zeros((YE, Z), f32)
            g = jnp.zeros((YE, Z), f32)
            for a in range(K):
                w = fields[a, z, x]
                t = t + coefa[a : a + 1, :] * w
                g = g + coefb[a : a + 1, :] * w
            temp[z, x] = t
            v1 = pe[0, z, x]
            g = pe[1, z, x] - coefb[VROWS : VROWS + 1, :] * v1 - g
            v1 = v1 - t
            for a in range(K, K + j + 1):
                w = fields[a, z, x]
                v1 = v1 - coefa[a : a + 1, :] * w
                g = g - coefb[a : a + 1, :] * w
            fields[C0 + j + 1, z, x] = v1
            fields[C0 + j + 2, z, x] = g
            return carry

        def images_only(p, carry):
            z, x = lax.rem(p, 2), lax.div(p, 2) * (XE - 1)
            t = jnp.zeros((YE, Z), f32)
            for a in range(K):
                t = t + coefa[a : a + 1, :] * fields[a, z, x]
            temp[z, x] = t
            return carry

        if not last:
            lax.fori_loop(0, 4, images_only, 0, unroll=2)
        lax.fori_loop(0, 2 * p_n, combine, 0, unroll=2)
        w2 = fields.at[C0 + j + 2]
        if last:
            def use(z, x, v, k):
                w2[0, x, 0:Y, :] = w2[0, x, 0:Y, :] - v

            apply(lambda z, x: temp[z, x], (0,), DEEP, DEEP + X, Y, use)
        else:
            def use(z, x, v, k):
                w2[z, x] = w2[z, x] - jnp.where(k > 0.0, v, 0.0)

            apply(lambda z, x: temp[z, x], (0, 1), DEEP - PAIR, DEEP + X + PAIR, YE, use)
            wait_send(cs)

    for p in pending:
        record(*p)

    hc = hcols[...]
    n2_col = nsq[C0 : C0 + STEPS, :]
    n_col = jnp.sqrt(n2_col)
    inv_col = 1.0 / n_col
    inv_row = col_sum(jnp.where(lane8 == row8, inv_col, 0.0))
    last_n = jnp.sqrt(last_sq)
    upper = hc[C0 : C0 + STEPS] * n_col * inv_row
    upper = jnp.where(lane8 < STEPS, upper, 0.0)
    upper = jnp.where(lane8 == row8, upper + SHIFT, upper)
    bottom = jnp.where(lane1 == STEPS - 1, last_n * inv_row, 0.0)
    hes = jnp.concatenate([upper, bottom], axis=0)
    lane_t, row_t = lane2[: STEPS + 1], row2[: STEPS + 1]
    for col in range(STEPS):
        picked = jnp.where(lane_t == row_t, hes[:, col : col + 1], 0.0)
        hes_out[col : col + 1, :] = jnp.sum(picked, axis=0, keepdims=True)[:, : STEPS + 1]

    h = {
        (r, c): jnp.broadcast_to(hes[r : r + 1, c : c + 1], (1, Z))
        for c in range(STEPS) for r in range(c + 2)
    }
    goal = [n_col[0:1]] + [jnp.zeros((1, Z), f32)] * STEPS
    for i in range(STEPS):
        top, low = h[i, i], h[i + 1, i]
        inv_r = 1.0 / jnp.sqrt(top * top + low * low)
        cs_, sn = top * inv_r, low * inv_r
        for c in range(i, STEPS):
            up, down = h[i, c], h[i + 1, c]
            h[i, c], h[i + 1, c] = cs_ * up + sn * down, cs_ * down - sn * up
        goal[i], goal[i + 1] = cs_ * goal[i] + sn * goal[i + 1], cs_ * goal[i + 1] - sn * goal[i]
    found = {}
    ysol = jnp.zeros((1, Z), f32)
    for i in range(STEPS - 1, -1, -1):
        rest = goal[i]
        for c in range(STEPS - 1, i, -1):
            rest = rest - h[i, c] * found[c]
        found[i] = rest * (1.0 / h[i, i])
        ysol = jnp.where(lane1 == i, found[i], ysol)

    rcoef = ecoef[:, :1] - jnp.sum(hc[:K] * (ysol * inv_row), axis=1, keepdims=True)
    ycol = jnp.sum(jnp.where(lane8 == row8, ysol * inv_row, 0.0), axis=1, keepdims=True)
    hy8 = jnp.sum(upper * ysol, axis=1, keepdims=True) * inv_col[:, :1]
    hy9 = jnp.sum(bottom * ysol, axis=1, keepdims=True) / last_n
    out = src[K]
    for a in range(K):
        out = out + rcoef[a : a + 1, :] * src[a]
    res = fields[C0, 0, DEEP : DEEP + X, 0:Y, :]
    for i in range(STEPS):
        ui = fields[C0 + i, 0, DEEP : DEEP + X, 0:Y, :]
        out = out + ycol[i : i + 1, :] * ui
        res = res - hy8[i : i + 1, :] * ui
    res = res - hy9 * fields[C0 + STEPS, 0, DEEP : DEEP + X, 0:Y, :]
    sol_out[...] = out
    res_out[...] = res


def deliver(sol, res, hes, sol_out, res_out, hes_out):
    sol_out[...] = sol[...]
    res_out[...] = res[...]
    hes_out[...] = hes[...]


def round_up(n, m):
    return (n + m - 1) // m * m


def solution(mesh):
    sizes = tuple(mesh.shape[a] for a in AXES)

    def body(right_side, start_guess, conductivity, recycled):
        K, X, Y, Z = recycled.shape
        NF = K + 2
        FR, ER = round_up(NF * X, 8), round_up(NF, 8)
        assert X >= DEEP and Y % 8 == 0 and K + STEPS <= VROWS

        def count(group):
            n = 1
            for a in group:
                n *= mesh.shape[a]
            return n

        groups = ONE if count(AXES) <= 64 else TWO
        n_step = [count(g) for g in groups]
        nflat, ntall = sem_counts(sizes)
        chunks = (NF + CHUNK - 1) // CHUNK
        nsem = ntall + (chunks + 2) * nflat
        nrecv = 2 * ntall + (2 * chunks + 2) * nflat
        XE, YE = X + 2 * DEEP, Y + 8
        V = lambda *s: pltpu.VMEM(s, jnp.float32)
        vm = pl.BlockSpec(memory_space=pltpu.VMEM)
        shape = jax.ShapeDtypeStruct((X, Y, Z), jnp.float32)

        def halo(s):
            cells = 2 * s - 1
            return [
                V(2, FR, Z), V(2, 2, ER * cells, Z),
                V(2, NF, 1, Y, Z), V(2, FR, Z), V(2, 2, ER * cells, Z),
            ]

        def lanes(d):
            rows, cells = round_up(X * d, 8), d * d
            return [
                V(1, X, Y, Z), V(2, rows, Z), V(2, 2, cells, Z),
                V(2, 1, X, Y, Z), V(2, 2, 1, d, Y, Z), V(2, 2, rows, Z), V(2, 2, 2, cells, Z),
            ]

        prow, pcell = round_up(2 * X * PAIR, 8), 2 * PAIR * PAIR
        lrow, lcell = round_up(X * PAIR, 8), PAIR * PAIR
        sol, res, hes = pl.pallas_call(
            functools.partial(kernel, sizes, groups),
            out_shape=(shape, shape, jax.ShapeDtypeStruct((STEPS, STEPS + 1), jnp.float32)),
            in_specs=[pl.BlockSpec(memory_space=pltpu.HBM)] * 4,
            out_specs=(vm, vm, vm),
            scratch_shapes=[
                V(X, Y, Z), V(X, Y, Z), V(NF, X, Y, Z), V(NF, X, Y, Z), V(K, X, Y, Z),
                *halo(1), *halo(1), *halo(2), *halo(3), *lanes(1), *lanes(DEEP),
                V(2, 2, X, Y, Z), V(2, 2, prow, Z), V(2, 2, 2, pcell, Z),
                V(2, 1, X, Y, Z), V(2, 2, lrow, Z), V(2, 2, 2, lcell, Z),
                V(2, 2, 2, PAIR, Y, Z), V(2, 2, prow, Z), V(2, 2, 2, pcell, Z),
                V(2, 2, 1, X, Y, Z), V(2, 2, 2, 1, PAIR, Y, Z),
                V(2, 2, 2, lrow, Z), V(2, 2, 2, 2, lcell, Z),
                V(K + STEPS + 1, 2, XE, YE, Z), V(2, XE, YE, Z), V(2, XE, YE, Z),
                V(2, XE, YE, Z), V(2, XE, YE, Z), V(XE, YE, Z), V(2, 2, XE, YE, Z),
                V(n_step[0], GF, Z), V(n_step[-1], GF, Z), V(n_step[0], 2, Z), V(n_step[-1], 2, Z),
                V(2, n_step[0], 1, Z), V(2, n_step[-1], 1, Z),
                V(32, Z), V(K, Z), V(K, Z), V(K, Z), V(32, Z), V(32, Z), V(32, Z), V(32, Z), V(K, Z),
                pltpu.SemaphoreType.DMA((nsem,)), pltpu.SemaphoreType.DMA((nrecv,)),
                pltpu.SemaphoreType.DMA((4, len(groups))), pltpu.SemaphoreType.DMA((4, len(groups))),
                pltpu.SemaphoreType.DMA((4,)),
            ],
            compiler_params=pltpu.CompilerParams(collective_id=0, has_side_effects=True, vmem_limit_bytes=VMEM - KEPT),
        )(right_side, start_guess, conductivity, recycled)
        sol, res, hes = pl.pallas_call(
            deliver,
            out_shape=(shape, shape, jax.ShapeDtypeStruct(hes.shape, hes.dtype)),
            in_specs=[vm] * 3,
            out_specs=(vm,) * 3,
            compiler_params=pltpu.CompilerParams(vmem_limit_bytes=8 * 2**20),
        )(sol, res, hes)
        return sol, res, hes.T

    return jax.shard_map(
        body,
        mesh=mesh,
        in_specs=(P(*AXES), P(*AXES), P(*AXES), P(None, *AXES)),
        out_specs=(P(*AXES), P(*AXES), P()),
        check_vma=False,
    )
```
